32 devices in a mesh: rows: 4 (over x, core), heads: 8 (over z, y).
Axes of the slice: x: 2, y: 2, z: 4, core: 2. Of those that a mesh axis runs over, the one named last changes fastest.
Arguments:
- hidden_in: bfloat16 [16, 2048, 1024], P('rows', 'heads'), may hold values from -6 to 6
- doc_ids: int32 [16, 2048], P('rows'), may hold values from 0 to 8, as said below
- cotangent: bfloat16 [16, 2048, 1024], P('rows', 'heads'), may hold values from -6 to 6
- attn_gain: float32 [1024], replicated, may hold values from 0.1 to 1.9
- query_weight: bfloat16 [1024, 1024], replicated, may hold values from -0.1875 to 0.1875
- latent_weight: bfloat16 [1024, 512], replicated, may hold values from -0.1875 to 0.1875
- key_lift_weight: bfloat16 [2, 256, 512], replicated, may hold values from -0.375 to 0.375
- value_lift_weight: bfloat16 [2, 256, 512], replicated, may hold values from -0.375 to 0.375
- output_weight: bfloat16 [1024, 1024], replicated, may hold values from -1.5 to 1.5
- ffn_gain: float32 [1024], replicated, may hold values from 0.1 to 1.9
- gate_weight: bfloat16 [1024, 2816], replicated, may hold values from -0.1875 to 0.1875
- up_weight: bfloat16 [1024, 2816], replicated, may hold values from -0.1875 to 0.1875
- down_weight: bfloat16 [2816, 1024], replicated, may hold values from -0.109375 to 0.109375
Outputs:
- hidden_out: bfloat16 [16, 2048, 1024], P('rows', 'heads')
- hidden_grad: float32 [16, 2048, 1024], P('rows', 'heads')
- attn_gain_grad: float32 [1024], P('heads')
- query_grad: float32 [1024, 1024], P('heads')
- latent_grad: float32 [1024, 512], P('heads')
- key_up_grad: float32 [2, 256, 512], P(None, 'heads')
- value_up_grad: float32 [2, 256, 512], P(None, 'heads')
- output_grad: float32 [1024, 1024], P('heads')
- ffn_gain_grad: float32 [1024], P('heads')
- gate_grad: float32 [1024, 2816], P(None, 'heads')
- up_grad: float32 [1024, 2816], P(None, 'heads')
- down_grad: float32 [2816, 1024], P('heads')
The draws below stay inside these ranges and needn't reach their ends.
Inputs may be any that keep to these rules, and one draw needn't show every extreme that they name: `doc_ids`: in each row, ids start at 1 and rise by one at each document boundary along the row; 0 marks padding, which, where a row has any, fills its tail. A row holds at most 8 documents.
All inputs are finite; a program needn't handle non-finite values.
Results may differ from the reference program's by a relative error of at most 0.02.
Values may be sent and summed in bfloat16 or wider, within the bound.
A program may use at most 192 MiB of HBM per device.

```python
import math
import jax
import jax.numpy as jnp
from jax import lax

D = 1024
QUERY_HEADS = 16
HEAD_WIDTH = 64
GROUPS = 2
LATENT = 256
FF = 2816
SEQ = 2048
ROWS = 16
GROUP_HEADS = 8


def draw_doc_ids(key, part):
    cut_key, count_key, pad_key = jax.random.split(key, 3)
    row_keys = jax.random.split(cut_key, ROWS)
    shuffled = jax.vmap(lambda row_key: jax.random.permutation(row_key, SEQ - 1))(row_keys)
    cuts = shuffled[:, :7] + 1
    counts = jax.random.randint(count_key, (ROWS,), 0, 8)
    counts = jnp.where(jnp.arange(ROWS) == 0, 7, counts)
    active = jnp.arange(7)[None, :] < counts[:, None]
    positions = jnp.arange(SEQ)
    passed = (cuts[:, None, :] <= positions[None, :, None]) & active[:, None, :]
    ids = 1 + jnp.sum(passed.astype(jnp.int32), axis=-1)
    padding = jax.random.randint(pad_key, (ROWS,), 1, max(2, SEQ // 4))
    padding = jnp.where(jnp.arange(ROWS) == 0, 0, padding)
    return jnp.where(positions[None, :] >= SEQ - padding[:, None], 0, ids).astype(jnp.int32)


def shard_levels(key, dims, cuts, smallest, largest):
    def one(position, blocks):
        steps = jax.random.uniform(jax.random.fold_in(jax.random.fold_in(key, 6), position), (blocks,), jnp.float32, smallest / len(cuts), largest / len(cuts))
        return jnp.repeat(jnp.exp(steps), dims[position] // blocks).reshape((-1,) + (1,) * (len(dims) - position - 1))

    level = one(*cuts[0])
    for cut in cuts[1:]:
        level = level * one(*cut)
    return level


def scatter_about(own_key, shape, scale, most, cuts=(), kind=jnp.bfloat16):
    drawn = jax.random.normal(own_key, shape, jnp.float32) * scale
    if len(cuts) > 0:
        drawn = shard_levels(own_key, shape, cuts, -0.22, 0.18) * drawn
    return jnp.clip(drawn, min=-most, max=most).astype(kind)


def setup_inputs(seed: int = 0) -> dict:
    splits = jax.random.split(jax.random.key(seed), 14)
    hidden_in = scatter_about(splits[0], (ROWS, SEQ, D), 1.0, 6.0, ((0, 4), (1, 8)))
    doc_ids = draw_doc_ids(jax.random.fold_in(splits[13], 71), 0)
    cotangent = scatter_about(splits[2], (ROWS, SEQ, D), 1.0, 6.0, ((0, 4), (1, 8)))
    attn_gain = jnp.clip(1.0 + 0.18 * jax.random.normal(splits[3], (D,), jnp.float32), 0.1, 1.9)
    query_weight = scatter_about(splits[4], (D, QUERY_HEADS * HEAD_WIDTH), D ** -0.5, 0.1875)
    latent_weight = scatter_about(splits[5], (D, GROUPS * LATENT), D ** -0.5, 0.1875)
    key_lift_weight = scatter_about(splits[6], (GROUPS, LATENT, GROUP_HEADS * HEAD_WIDTH), LATENT ** -0.5, 0.375)
    value_lift_weight = scatter_about(splits[7], (GROUPS, LATENT, GROUP_HEADS * HEAD_WIDTH), LATENT ** -0.5, 0.375)
    output_weight = scatter_about(splits[8], (QUERY_HEADS * HEAD_WIDTH, D), (QUERY_HEADS * HEAD_WIDTH // 64) ** -0.5, 1.5)
    ffn_gain = jnp.clip(1.0 + 0.18 * jax.random.normal(splits[9], (D,), jnp.float32), 0.1, 1.9)
    gate_weight = scatter_about(splits[10], (D, FF), D ** -0.5, 0.1875)
    up_weight = scatter_about(splits[11], (D, FF), D ** -0.5, 0.1875)
    down_weight = scatter_about(splits[12], (FF, D), FF ** -0.5, 0.109375)
    return {"hidden_in": hidden_in, "doc_ids": doc_ids, "cotangent": cotangent, "attn_gain": attn_gain, "query_weight": query_weight, "latent_weight": latent_weight, "key_lift_weight": key_lift_weight, "value_lift_weight": value_lift_weight, "output_weight": output_weight, "ffn_gain": ffn_gain, "gate_weight": gate_weight, "up_weight": up_weight, "down_weight": down_weight}


@jax.custom_vjp
def reduced_precision(v):
    return lax.optimization_barrier(v.astype(jnp.bfloat16)).astype(jnp.float32)

@jax.custom_vjp
def reduced_precision_back(v):
    return v

def low_keep(v):
    return (reduced_precision(v), None)

def low_pass(kept, grad):
    return (grad,)

def back_keep(v):
    return (v, None)

def back_low(kept, grad):
    return (reduced_precision(grad),)
reduced_precision.defvjp(low_keep, low_pass)
reduced_precision_back.defvjp(back_keep, back_low)
exact_precision = lax.Precision.HIGHEST
epsilon = 1e-05

def product(left, right):
    return jnp.dot(left, right, precision=exact_precision)

def normalize(value_matrix, gain):
    return value_matrix * lax.rsqrt(lax.optimization_barrier(jnp.mean(value_matrix * value_matrix, axis=-1, keepdims=True)) + epsilon) * gain

def attend(queries, key_matrix, value_matrix, docs):
    document_pairs, token_length = (queries.shape[0], queries.shape[1])
    block = min(512, token_length)
    scale = HEAD_WIDTH ** (-0.5)
    positions = jnp.arange(token_length, dtype=jnp.int32)

    def one_block(index):
        start = (index * block).astype(jnp.int32)
        query_tile = lax.dynamic_slice_in_dim(queries, start, block, 1)
        query_doc = lax.dynamic_slice_in_dim(docs, start, block, 1)
        query_pos = start + jnp.arange(block, dtype=jnp.int32)
        scores = reduced_precision_back(scale * jnp.einsum('pqhd,pkhd->phqk', query_tile, key_matrix, precision=exact_precision))
        allow = (query_doc[:, :, None] == docs[:, None, :]) & (positions[None, None, :] <= query_pos[None, :, None])
        probs = jax.nn.softmax(jnp.where(allow[:, None], scores, -jnp.inf), axis=-1)
        return jnp.einsum('phqk,pkhd->pqhd', reduced_precision(probs), value_matrix, precision=exact_precision)
    tiles = lax.map(jax.checkpoint(one_block), jnp.arange(token_length // block, dtype=jnp.int32))
    return jnp.moveaxis(tiles, 0, 1).reshape(document_pairs, token_length, QUERY_HEADS, HEAD_WIDTH)

def layer(inputs, docs, attn_gain, query_weight, latent_weight, key_lift_weight, value_lift_weight, output_weight, ffn_gain, gate_weight, up_weight, down_weight):
    document_pairs, token_length = (inputs.shape[0], inputs.shape[1])
    normed_one = reduced_precision(normalize(inputs, attn_gain))
    queries = reduced_precision(reduced_precision_back(product(normed_one, query_weight))).reshape(document_pairs, token_length, QUERY_HEADS, HEAD_WIDTH)
    latent_rows = reduced_precision(reduced_precision_back(product(normed_one, latent_weight))).reshape(document_pairs, token_length, GROUPS, LATENT)
    key_matrix = reduced_precision(reduced_precision_back(jnp.einsum('kmdt,dtr->kmdr', latent_rows, key_lift_weight, precision=exact_precision))).reshape(document_pairs, token_length, QUERY_HEADS, HEAD_WIDTH)
    value_matrix = reduced_precision(reduced_precision_back(jnp.einsum('kmdt,dtr->kmdr', latent_rows, value_lift_weight, precision=exact_precision))).reshape(document_pairs, token_length, QUERY_HEADS, HEAD_WIDTH)
    mixed = reduced_precision(reduced_precision_back(attend(queries, key_matrix, value_matrix, docs))).reshape(document_pairs, token_length, QUERY_HEADS * HEAD_WIDTH)
    resid = inputs + reduced_precision_back(product(mixed, output_weight))
    normed_two = reduced_precision(normalize(resid, ffn_gain))
    gate = reduced_precision_back(product(normed_two, gate_weight))
    up_value = reduced_precision_back(product(normed_two, up_weight))
    hidden = reduced_precision(jax.nn.silu(gate) * up_value)
    return resid + reduced_precision_back(product(hidden, down_weight))

def reference(hidden_in, doc_ids, cotangent, attn_gain, query_weight, latent_weight, key_lift_weight, value_lift_weight, output_weight, ffn_gain, gate_weight, up_weight, down_weight):
    weights = (attn_gain.astype(jnp.float32), query_weight.astype(jnp.float32), latent_weight.astype(jnp.float32), key_lift_weight.astype(jnp.float32), value_lift_weight.astype(jnp.float32), output_weight.astype(jnp.float32), ffn_gain.astype(jnp.float32), gate_weight.astype(jnp.float32), up_weight.astype(jnp.float32), down_weight.astype(jnp.float32))
    rows, token_length = doc_ids.shape
    pair = math.gcd(rows, max(1, 4096 // token_length))
    count = rows // pair
    inputs = hidden_in.astype(jnp.float32).reshape(count, pair, token_length, D)
    keep = (doc_ids != 0).astype(jnp.float32)
    cotangents = (cotangent.astype(jnp.float32) * keep[:, :, None]).reshape(count, pair, token_length, D)
    docs = doc_ids.reshape(count, pair, token_length)

    def advance(totals, items):
        block_in, block_docs, block_cot = items

        def forward(block_x, params):
            return layer(block_x, block_docs, *params)
        output, pull = jax.vjp(forward, block_in, weights)
        grad_in, grad_weights = pull(block_cot)
        totals = tuple((total + grad for total, grad in zip(totals, grad_weights)))
        return (totals, (output.astype(jnp.bfloat16), grad_in))
    initial = tuple((jnp.zeros(weight.shape, jnp.float32) for weight in weights))
    totals, (outputs, grads) = lax.scan(advance, initial, (inputs, docs, cotangents))
    return (outputs.reshape(rows, token_length, D), grads.reshape(rows, token_length, D), totals[0], totals[1], totals[2], totals[3], totals[4], totals[5], totals[6], totals[7], totals[8], totals[9])
```

```python
import functools
import math

import jax
import jax.numpy as jnp
from jax import lax
from jax.experimental import pallas as pl
from jax.experimental.pallas import tpu as pltpu
from jax.sharding import PartitionSpec as P

HEAD_WIDTH = 64
epsilon = 1e-05
blocked = -1e30
LOG2E = math.log2(math.e)
LN2 = math.log(2.0)
QUAD = 4
f32 = jnp.float32
bf16 = jnp.bfloat16


def matmul(left, right):
    return jnp.dot(left, right, preferred_element_type=f32)


def matmul_nt(left, right):
    return lax.dot_general(
        left, right, (((left.ndim - 1,), (right.ndim - 1,)), ((), ())), preferred_element_type=f32
    )


def matmul_tn(left, right):
    return lax.dot_general(left, right, (((0,), (0,)), ((), ())), preferred_element_type=f32)


def rms_inverse(value_matrix):
    return lax.rsqrt(jnp.mean(value_matrix * value_matrix, axis=-1, keepdims=True) + epsilon)


def norm_back(grad_normed, unit, inverse, gain):
    scaled = grad_normed * gain
    grad_in = inverse * (scaled - unit * jnp.mean(scaled * unit, axis=-1, keepdims=True))
    return (grad_in, jnp.sum(grad_normed * unit, axis=0))


def expand_heads(source, weights, factor, out_ref):
    quads, wide, deep = weights.shape
    latent = wide // QUAD
    for quad in range(quads):
        product = matmul_nt(weights[quad], source[:, quad * deep : (quad + 1) * deep])
        if factor != 1.0:
            product = product * factor
        product = product.astype(bf16)
        for h in range(QUAD):
            out_ref[quad * QUAD + h] = product[h * latent : (h + 1) * latent]


def seg_mask(diagonal, base, start):
    keys = start.shape[-1]
    key_at = lax.broadcasted_iota(jnp.int32, (keys, keys), 0)
    allow = key_at >= (start - base)
    if diagonal:
        allow = allow & (key_at <= lax.broadcasted_iota(jnp.int32, (keys, keys), 1))
    return allow


def attend_kernel(count, first, last, diagonal_at, lo, bases, *refs):
    refs = list(refs)
    take = lambda k: [refs.pop(0) for _ in range(k)]
    query_ref, start_ref, key_lift_ref = take(3)
    segs = take(count)
    if not first:
        top_in, total_in, mix_in = take(3)
    if last:
        (value_lift_ref,) = take(1)
        out_ref, lse_ref, mix_ref = take(3)
    else:
        top_out, total_out, mix_out = take(3)
    expanded, top, total, mix = take(4)
    heads = expanded.shape[0]
    tokens = query_ref.shape[1]
    row = pl.program_id(0)
    scale = HEAD_WIDTH ** (-0.5) * LOG2E
    expand_heads(query_ref[0], key_lift_ref, scale, expanded)
    if first:
        top[...] = jnp.full_like(top, blocked)
        total[...] = jnp.zeros_like(total)
        mix[...] = jnp.zeros_like(mix)
    else:
        top[...] = top_in[0]
        total[...] = total_in[0]
        mix[...] = mix_in[0]
    start = start_ref[0]
    for i in range(count):

        @pl.when((bases[i] >= 0) & (bases[i] + tokens - 1 >= lo[row]))
        def _():
            latent = segs[i][0]
            latent_t = latent.T
            allow = seg_mask(i == diagonal_at, bases[i], start)
            for h in range(heads):
                score = jnp.where(allow, matmul(latent, expanded[h]), blocked)
                old = top[h : h + 1]
                new = jnp.maximum(old, jnp.max(score, axis=0, keepdims=True))
                probs = jnp.exp2(score - new)
                fade = jnp.exp2(old - new)
                top[h : h + 1] = new
                total[h : h + 1] = total[h : h + 1] * fade + jnp.sum(probs, axis=0, keepdims=True)
                mix[h] = mix[h] * fade + matmul(latent_t, probs.astype(bf16))

    if not last:
        top_out[0] = top[...]
        total_out[0] = total[...]
        mix_out[0] = mix[...]
        return
    lse_ref[0] = top[...] + jnp.log2(total[...])
    inverse = 1.0 / total[...]
    quads, deep, wide = value_lift_ref.shape
    for h in range(heads):
        mix_ref[0, h] = (mix[h] * inverse[h : h + 1]).astype(bf16)
    for quad in range(quads):
        part = mix_ref[0, quad * QUAD : (quad + 1) * QUAD].reshape(wide, tokens)
        lifted = matmul(value_lift_ref[quad], part)
        out_ref[0, :, quad * deep : (quad + 1) * deep] = lifted.T.astype(bf16)


def whole(array):
    return pl.BlockSpec(array.shape, lambda *_: (0,) * array.ndim)


def by_row(shape):
    return pl.BlockSpec((1,) + tuple(shape[1:]), lambda r, *_: (r,) + (0,) * (len(shape) - 1))


def attend_part(queries, start, key_lift, value_lift, lo, segs, bases, diagonal_at, state, last):
    rows, tokens, width = queries.shape
    heads = width // HEAD_WIDTH
    latent = segs[0].shape[-1]
    state_shapes = [(rows, heads, tokens), (rows, heads, tokens), (rows, heads, latent, tokens)]
    args = [queries, start, key_lift, *segs]
    specs = [by_row(queries.shape), by_row(start.shape), whole(key_lift)]
    specs += [by_row(s.shape) for s in segs]
    if state is not None:
        args += list(state)
        specs += [by_row(s) for s in state_shapes]
    if last:
        args.append(value_lift)
        specs.append(whole(value_lift))
        outs = [
            jax.ShapeDtypeStruct(queries.shape, bf16),
            jax.ShapeDtypeStruct(state_shapes[0], f32),
            jax.ShapeDtypeStruct(state_shapes[2], bf16),
        ]
    else:
        outs = [jax.ShapeDtypeStruct(s, f32) for s in state_shapes]
    blocks = rows * heads * len(segs)
    return pl.pallas_call(
        functools.partial(attend_kernel, len(segs), state is None, last, diagonal_at),
        out_shape=outs,
        grid_spec=pltpu.PrefetchScalarGridSpec(
            num_scalar_prefetch=2,
            grid=(rows,),
            in_specs=specs,
            out_specs=[by_row(o.shape) for o in outs],
            scratch_shapes=[
                pltpu.VMEM((heads, latent, tokens), bf16),
                pltpu.VMEM((heads, tokens), f32),
                pltpu.VMEM((heads, tokens), f32),
                pltpu.VMEM((heads, latent, tokens), f32),
            ],
        ),
        compiler_params=pltpu.CompilerParams(
            dimension_semantics=("arbitrary",), vmem_limit_bytes=48 << 20
        ),
        cost_estimate=pl.CostEstimate(
            flops=blocks * tokens * tokens * latent * 4,
            bytes_accessed=rows * heads * latent * tokens * 4,
            transcendentals=blocks * tokens * tokens,
        ),
        name="attend",
    )(lo, bases, *args)


def attend_back_kernel(count, first, last, diagonal_at, lo, bases, *refs):
    refs = list(refs)
    take = lambda k: [refs.pop(0) for _ in range(k)]
    query_ref, grad_ref, lse_ref, mix_ref, start_ref, key_lift_ref, value_lift_ref = take(7)
    segs = take(count)
    if not first:
        (back_in,) = take(1)
    if last:
        (key_lift_t_ref,) = take(1)
    seg_grads = take(count)
    if last:
        query_back_ref, key_up_ref, value_up_ref = take(3)
    else:
        (back_out,) = take(1)
    expanded, expanded_grad, delta, back, part_key, part_value = take(6)
    heads, latent_size, tokens = expanded.shape
    row = pl.program_id(0)
    scale = HEAD_WIDTH ** (-0.5)
    expand_heads(query_ref[0], key_lift_ref, scale * LOG2E, expanded)
    expand_heads(grad_ref[0], value_lift_ref, 1.0, expanded_grad)
    for h in range(heads):
        delta[h : h + 1] = jnp.sum(
            mix_ref[0, h].astype(f32) * expanded_grad[h].astype(f32), axis=0, keepdims=True
        )
    if first:
        back[...] = jnp.zeros_like(back)
    else:
        back[...] = back_in[0]
    start = start_ref[0]
    for i in range(count):
        touched = (bases[i] >= 0) & (bases[i] + tokens - 1 >= lo[row])

        @pl.when(touched)
        def _():
            latent = segs[i][0]
            latent_t = latent.T
            allow = seg_mask(i == diagonal_at, bases[i], start)
            for h in range(heads):
                score = matmul(latent, expanded[h])
                probs = jnp.where(allow, jnp.exp2(score - lse_ref[0, h : h + 1]), 0.0)
                dprobs = matmul(latent, expanded_grad[h])
                dscore = (probs * (dprobs - delta[h : h + 1])).astype(bf16)
                back[h] += matmul(latent_t, dscore)
                by_key = matmul_nt(dscore, expanded[h])
                by_value = matmul_nt(probs.astype(bf16), expanded_grad[h])
                if h == 0:
                    part_key[...] = by_key
                    part_value[...] = by_value
                else:
                    part_key[...] += by_key
                    part_value[...] += by_value
            seg_grads[i][0] = (part_key[...] * LN2 + part_value[...]).astype(bf16)

        @pl.when(jnp.logical_not(touched))
        def _():
            seg_grads[i][0] = jnp.zeros((tokens, latent_size), bf16)

    if not last:
        back_out[0] = back[...]
        return

    @pl.when(row == 0)
    def _():
        key_up_ref[...] = jnp.zeros_like(key_up_ref)
        value_up_ref[...] = jnp.zeros_like(value_up_ref)

    quads, deep, wide = key_lift_t_ref.shape
    for quad in range(quads):
        part = (back[quad * QUAD : (quad + 1) * QUAD].reshape(wide, tokens) * scale).astype(bf16)
        lifted = matmul(key_lift_t_ref[quad], part)
        query_back_ref[0, :, quad * deep : (quad + 1) * deep] = lifted.T.astype(bf16)
        key_up_ref[quad] += matmul(part, query_ref[0, :, quad * deep : (quad + 1) * deep])
        mixed = mix_ref[0, quad * QUAD : (quad + 1) * QUAD].reshape(wide, tokens)
        value_up_ref[quad] += matmul(mixed, grad_ref[0, :, quad * deep : (quad + 1) * deep])


def attend_back_part(
    queries, grads, lse, mix, start, key_lift, value_lift, key_lift_t, lo, segs, bases,
    diagonal_at, state, last,
):
    rows, tokens, width = queries.shape
    heads = width // HEAD_WIDTH
    latent = segs[0].shape[-1]
    state_shape = (rows, heads, latent, tokens)
    args = [queries, grads, lse, mix, start, key_lift, value_lift, *segs]
    specs = [by_row(a.shape) for a in (queries, grads, lse, mix, start)]
    specs += [whole(key_lift), whole(value_lift)]
    specs += [by_row(s.shape) for s in segs]
    if state is not None:
        args.append(state)
        specs.append(by_row(state_shape))
    outs = [jax.ShapeDtypeStruct(s.shape, bf16) for s in segs]
    out_specs = [by_row(s.shape) for s in segs]
    if last:
        args.append(key_lift_t)
        specs.append(whole(key_lift_t))
        outs.append(jax.ShapeDtypeStruct(queries.shape, bf16))
        out_specs.append(by_row(queries.shape))
        for _ in range(2):
            outs.append(jax.ShapeDtypeStruct(key_lift.shape, f32))
            out_specs.append(whole(key_lift))
    else:
        outs.append(jax.ShapeDtypeStruct(state_shape, f32))
        out_specs.append(by_row(state_shape))
    blocks = rows * heads * len(segs)
    return pl.pallas_call(
        functools.partial(attend_back_kernel, len(segs), state is None, last, diagonal_at),
        out_shape=outs,
        grid_spec=pltpu.PrefetchScalarGridSpec(
            num_scalar_prefetch=2,
            grid=(rows,),
            in_specs=specs,
            out_specs=out_specs,
            scratch_shapes=[
                pltpu.VMEM((heads, latent, tokens), bf16),
                pltpu.VMEM((heads, latent, tokens), bf16),
                pltpu.VMEM((heads, tokens), f32),
                pltpu.VMEM((heads, latent, tokens), f32),
                pltpu.VMEM((tokens, latent), f32),
                pltpu.VMEM((tokens, latent), f32),
            ],
        ),
        compiler_params=pltpu.CompilerParams(
            dimension_semantics=("arbitrary",), vmem_limit_bytes=48 << 20
        ),
        cost_estimate=pl.CostEstimate(
            flops=blocks * tokens * tokens * latent * 10,
            bytes_accessed=rows * heads * latent * tokens * 8,
            transcendentals=blocks * tokens * tokens,
        ),
        name="attend_back",
    )(lo, bases, *args)


def quad_lift(lift):
    latent, width = lift.shape
    deep = QUAD * HEAD_WIDTH
    quads = width // deep
    tall = jnp.tile(lift.reshape(latent, quads, deep).transpose(1, 0, 2), (1, QUAD, 1))
    row_head = lax.broadcasted_iota(jnp.int32, tall.shape, 1) // latent
    column_head = lax.broadcasted_iota(jnp.int32, tall.shape, 2) // HEAD_WIDTH
    return jnp.where(row_head == column_head, tall, jnp.zeros_like(tall))


def quad_unlift(quad_grad):
    quads, wide, deep = quad_grad.shape
    latent = wide // QUAD
    column_head = lax.broadcasted_iota(jnp.int32, (latent, deep), 1) // HEAD_WIDTH
    parts = []
    for quad in range(quads):
        part = quad_grad[quad, :latent]
        for h in range(1, QUAD):
            part = jnp.where(column_head == h, quad_grad[quad, h * latent : (h + 1) * latent], part)
        parts.append(part)
    return jnp.concatenate(parts, axis=1)


def flip(array, axis, bit):
    size = lax.axis_size(axis)
    return lax.ppermute(array, axis, [(i, i ^ (1 << bit)) for i in range(size)])


def add_sent(mine, other):
    return (mine.astype(f32) + other.astype(f32)).astype(bf16)


def reduce_rest(part):
    row_bits = lax.axis_size("rows").bit_length() - 1
    head_bits = lax.axis_size("heads").bit_length() - 1
    row_at = lax.axis_index("rows")
    head_at = lax.axis_index("heads")
    for bit in range(1, row_bits):
        mine = (row_at >> bit) & 1
        half = part.shape[-1] // 2
        keep = lax.dynamic_slice_in_dim(part, mine * half, half, 2)
        send = lax.dynamic_slice_in_dim(part, (1 - mine) * half, half, 2)
        part = add_sent(keep, flip(send, "rows", bit))
    for bit in range(head_bits):
        mine = (head_at >> bit) & 1
        pairs = part.reshape((part.shape[0] // 2, 2) + part.shape[1:])
        keep = lax.dynamic_index_in_dim(pairs, mine, 1, keepdims=False)
        send = lax.dynamic_index_in_dim(pairs, 1 - mine, 1, keepdims=False)
        part = add_sent(keep, flip(send, "heads", bit))
    return part[0]


def gather_columns(part):
    row_bits = lax.axis_size("rows").bit_length() - 1
    row_at = lax.axis_index("rows")
    for bit in reversed(range(row_bits)):
        mine = (row_at >> bit) & 1
        other = flip(part, "rows", bit)
        low = jnp.where(mine == 0, part, other)
        high = jnp.where(mine == 0, other, part)
        part = jnp.stack([low, high]) if bit == 0 else jnp.concatenate([low, high], axis=1)
    return part


def shards(
    hidden_in,
    doc_ids,
    cotangent,
    attn_gain,
    query_weight,
    latent_weight,
    key_lift_weight,
    value_lift_weight,
    output_weight,
    ffn_gain,
    gate_weight,
    up_weight,
    down_weight,
):
    rows, tokens, width = hidden_in.shape
    peers = lax.axis_size("heads")
    place = lax.axis_index("heads")
    core = lax.axis_index("rows") & 1
    groups, latent_size, group_width = key_lift_weight.shape
    count = rows * tokens
    steps = peers // 2
    side = place & 1
    level = place // 2
    swap = lambda a: flip(a, "rows", 0)
    mine = lambda a, axis: lax.dynamic_slice_in_dim(a, core * (a.shape[axis] // 2), a.shape[axis] // 2, axis)
    theirs = lambda a, axis: lax.dynamic_slice_in_dim(
        a, (1 - core) * (a.shape[axis] // 2), a.shape[axis] // 2, axis
    )

    own_base = place * tokens
    own_docs = lax.dynamic_slice_in_dim(doc_ids, own_base, tokens, 1)
    position = own_base + jnp.arange(tokens, dtype=jnp.int32)
    before = (doc_ids[:, None, :] == own_docs[:, :, None]) & (
        jnp.arange(doc_ids.shape[1], dtype=jnp.int32)[None, None, :] <= position[None, :, None]
    )
    own_start = position[None, :] + 1 - jnp.sum(before.astype(jnp.int32), axis=-1)
    start = jnp.concatenate([own_start, swap(own_start)], axis=0)
    lo = start[:, 0]
    start = start[:, None, :]

    inputs = hidden_in.reshape(count, width).astype(f32)
    inverse_one = rms_inverse(inputs)
    normed_one = (inputs * inverse_one * attn_gain).astype(bf16)
    latent_mine = matmul(normed_one, mine(latent_weight, 1)).astype(bf16)
    latent_sent = matmul(normed_one, theirs(latent_weight, 1)).astype(bf16)
    latent_got = swap(latent_sent)
    own_seg = jnp.concatenate([latent_mine, latent_got], axis=0).reshape(2 * rows, tokens, latent_size)
    query_mine = matmul(normed_one, mine(query_weight, 1)).astype(bf16)
    query_sent = matmul(normed_one, theirs(query_weight, 1)).astype(bf16)
    queries = jnp.concatenate([query_mine, swap(query_sent)], axis=0).reshape(2 * rows, tokens, group_width)

    key_mine = lax.dynamic_index_in_dim(key_lift_weight, core, 0, keepdims=False)
    value_mine = lax.dynamic_index_in_dim(value_lift_weight, core, 0, keepdims=False)
    key_lift = quad_lift(key_mine)
    value_lift = quad_lift(value_mine)
    key_lift_t = key_lift.transpose(0, 2, 1)
    value_lift_t = value_lift.transpose(0, 2, 1)

    up_chain = [(i, i + 2) for i in range(peers - 2)]
    down_chain = [(i + 2, i) for i in range(peers - 2)]
    segs = []
    bases = []
    moving = own_seg
    for k in range(steps):
        if k > 0:
            moving = lax.ppermute(moving, "heads", up_chain)
        segs.append((moving, flip(moving, "heads", 0)))
        base = ((level - k) * 2 + side) * tokens
        other = ((level - k) * 2 + 1 - side) * tokens
        there = level >= k
        bases.append(
            (jnp.where(there, base, -1), jnp.where(there & (other < own_base), other, -1))
        )

    def pick(ks):
        return (
            [s for k in ks for s in segs[k]],
            jnp.stack([b for k in ks for b in bases[k]]).astype(jnp.int32),
        )

    parts = [range(0, steps - 1), range(steps - 1, steps)]
    state = None
    for i, ks in enumerate(parts):
        seg_list, base_list = pick(ks)
        state = attend_part(
            queries, start, key_lift, value_lift_t, lo, seg_list, base_list,
            0 if i == 0 else -1, state, i == len(parts) - 1,
        )
    head_out, lse, head_mix = state
    mixed_mine = head_out[:rows].reshape(count, group_width)
    mixed_got = swap(head_out[rows:]).reshape(count, group_width)
    mixed = jnp.where(
        core == 0,
        jnp.concatenate([mixed_mine, mixed_got], axis=1),
        jnp.concatenate([mixed_got, mixed_mine], axis=1),
    )

    resid = inputs + matmul(mixed, output_weight)
    inverse_two = rms_inverse(resid)
    unit_two = resid * inverse_two
    normed_two = (unit_two * ffn_gain).astype(bf16)
    gate = matmul(normed_two, gate_weight)
    up_value = matmul(normed_two, up_weight)
    sigmoid = jax.nn.sigmoid(gate)
    active = gate * sigmoid
    hidden = (active * up_value).astype(bf16)
    result = resid + matmul(hidden, down_weight)
    hidden_out = result.astype(bf16)
    keep = (own_docs != 0).astype(f32).reshape(count, 1)
    grad_result = cotangent.reshape(count, width).astype(f32) * keep
    ffn_back = grad_result.astype(bf16)
    grad_act = matmul_nt(ffn_back, down_weight)
    up_back = (grad_act * active).astype(bf16)
    gate_back = (grad_act * up_value * sigmoid * (1.0 + gate * (1.0 - sigmoid))).astype(bf16)
    grad_two = matmul_nt(gate_back, gate_weight) + matmul_nt(up_back, up_weight)
    grad_norm, ffn_gain_part = norm_back(grad_two, unit_two, inverse_two, ffn_gain)
    grad_resid = grad_result + grad_norm
    attn_back = grad_resid.astype(bf16)
    grad_mixed_mine = matmul_nt(attn_back, mine(output_weight, 0)).astype(bf16)
    grad_mixed_sent = matmul_nt(attn_back, theirs(output_weight, 0)).astype(bf16)
    head_grads = jnp.concatenate([grad_mixed_mine, swap(grad_mixed_sent)], axis=0).reshape(
        2 * rows, tokens, group_width
    )

    def halves(left, right):
        return (
            matmul_tn(left, mine(right, 1)).astype(bf16),
            matmul_tn(left, theirs(right, 1)).astype(bf16),
        )

    def core_sum(pair):
        total = add_sent(pair[0], swap(pair[1]))
        return total.reshape((peers, total.shape[0] // peers, total.shape[1]))

    gate_sum = core_sum(halves(gate_back, normed_two))
    up_sum = core_sum(halves(up_back, normed_two))
    down_sum = core_sum(halves(hidden, ffn_back))
    output_sum = core_sum(halves(mixed, attn_back))
    early_one = reduce_rest(jnp.concatenate([gate_sum, output_sum], axis=1))
    early_two = reduce_rest(jnp.concatenate([up_sum, down_sum], axis=1))

    back_parts = [[k] for k in range(steps - 1, 1, -1)] + [list(range(min(1, steps - 1), -1, -1))]
    state = None
    passing = None
    for i, ks in enumerate(back_parts):
        seg_list, base_list = pick(ks)
        done = i == len(back_parts) - 1
        outs = attend_back_part(
            queries, head_grads, lse, head_mix, start, key_lift, value_lift, key_lift_t, lo,
            seg_list, base_list, 2 * len(ks) - 2 if done else -1, state, done,
        )
        for j, k in enumerate(ks):
            total = outs[2 * j].astype(f32) + flip(outs[2 * j + 1], "heads", 0).astype(f32)
            if passing is not None:
                total = total + passing.astype(f32)
            passing = total.astype(bf16)
            if k > 0:
                passing = lax.ppermute(passing, "heads", down_chain)
        if done:
            query_grads, key_up_quads, value_up_quads = outs[2 * len(ks) :]
        else:
            state = outs[2 * len(ks)]
    latent_grads = passing

    query_back_mine = query_grads[:rows].reshape(count, group_width)
    query_back_got = swap(query_grads[rows:]).reshape(count, group_width)
    latent_back_mine = latent_grads[:rows].reshape(count, latent_size)
    latent_back_got = swap(latent_grads[rows:]).reshape(count, latent_size)
    query_sum = core_sum(
        (
            matmul_tn(normed_one, query_back_mine).astype(bf16),
            matmul_tn(normed_one, query_back_got).astype(bf16),
        )
    )
    latent_sum = core_sum(
        (
            matmul_tn(normed_one, latent_back_mine).astype(bf16),
            matmul_tn(normed_one, latent_back_got).astype(bf16),
        )
    )
    grad_one = (
        matmul_nt(query_back_mine, mine(query_weight, 1))
        + matmul_nt(query_back_got, theirs(query_weight, 1))
        + matmul_nt(latent_back_mine, mine(latent_weight, 1))
        + matmul_nt(latent_back_got, theirs(latent_weight, 1))
    )
    unit_one = inputs * inverse_one
    grad_in_norm, attn_gain_part = norm_back(grad_one, unit_one, inverse_one, attn_gain)
    hidden_grad = (grad_resid + grad_in_norm).reshape(rows, tokens, width)

    share = width // peers
    spread = lambda a: jnp.pad(a.astype(bf16).reshape(peers, 1, share), ((0, 0), (0, 7), (0, group_width - share)))
    gain_sum = add_sent(
        spread(jnp.where(core == 0, attn_gain_part, ffn_gain_part)),
        swap(spread(jnp.where(core == 0, ffn_gain_part, attn_gain_part))),
    )
    lift_share = latent_size // peers
    key_sum = quad_unlift(key_up_quads).astype(bf16).reshape(peers, lift_share, group_width)
    value_sum = quad_unlift(value_up_quads).astype(bf16).reshape(peers, lift_share, group_width)
    folded = latent_sum.reshape(peers, 2, latent_sum.shape[1] // 2, latent_sum.shape[2])
    latent_fold = jnp.concatenate([folded[:, 0], folded[:, 1]], axis=-1)
    late = reduce_rest(
        jnp.concatenate([query_sum, latent_fold, key_sum, value_sum, gain_sum], axis=1)
    )

    full = gather_columns(jnp.concatenate([early_one, early_two, late], axis=0)).astype(f32)
    at = 0

    def cut(size):
        nonlocal at
        piece = full[:, at : at + size]
        at += size
        return piece

    beside = lambda pair: jnp.concatenate([pair[0], pair[1]], axis=-1)
    ff_share = gate_weight.shape[1] // peers
    gate_share = beside(cut(ff_share)).T
    output_share = beside(cut(share))
    up_share = beside(cut(ff_share)).T
    down_share = beside(cut(ff_share))
    query_share = beside(cut(share))
    fold = cut(share // 2)
    latent_share = jnp.concatenate(
        [
            jnp.concatenate([fold[0, :, :latent_size], fold[1, :, :latent_size]], axis=-1),
            jnp.concatenate([fold[0, :, latent_size:], fold[1, :, latent_size:]], axis=-1),
        ],
        axis=0,
    )
    key_share = cut(lift_share)
    value_share = cut(lift_share)
    gains = cut(8)
    return (
        hidden_out.reshape(rows, tokens, width),
        hidden_grad,
        gains[0, 0, :share],
        query_share,
        latent_share,
        key_share,
        value_share,
        output_share,
        gains[1, 0, :share],
        gate_share,
        up_share,
        down_share,
    )


def solution(mesh):
    placed = (
        P("rows", "heads", None),
        P("rows", None),
        P("rows", "heads", None),
        P(),
        P(),
        P(),
        P(),
        P(),
        P(),
        P(),
        P(),
        P(),
        P(),
    )
    return jax.shard_map(
        shards,
        mesh=mesh,
        in_specs=placed,
        out_specs=(
            P("rows", "heads", None),
            P("rows", "heads", None),
            P("heads"),
            P("heads", None),
            P("heads", None),
            P(None, "heads", None),
            P(None, "heads", None),
            P("heads", None),
            P("heads"),
            P(None, "heads"),
            P(None, "heads"),
            P("heads", None),
        ),
        check_vma=False,
    )
```

```python
import functools
import math

import jax
import jax.numpy as jnp
from jax import lax
from jax.experimental import pallas as pl
from jax.experimental.pallas import tpu as pltpu
from jax.sharding import PartitionSpec as P

HEAD_WIDTH = 64
epsilon = 1e-05
blocked = -1e30
LOG2E = math.log2(math.e)
LN2 = math.log(2.0)
QUAD = 4
f32 = jnp.float32
bf16 = jnp.bfloat16


def matmul(left, right):
    return jnp.dot(left, right, preferred_element_type=f32)


def matmul_nt(left, right):
    return lax.dot_general(
        left, right, (((left.ndim - 1,), (right.ndim - 1,)), ((), ())), preferred_element_type=f32
    )


def matmul_tn(left, right):
    return lax.dot_general(left, right, (((0,), (0,)), ((), ())), preferred_element_type=f32)


def rms_inverse(value_matrix):
    return lax.rsqrt(jnp.mean(value_matrix * value_matrix, axis=-1, keepdims=True) + epsilon)


def norm_back(grad_normed, unit, inverse, gain):
    scaled = grad_normed * gain
    grad_in = inverse * (scaled - unit * jnp.mean(scaled * unit, axis=-1, keepdims=True))
    return (grad_in, jnp.sum(grad_normed * unit, axis=0))


def expand_heads(source, weights, factor, out_ref):
    quads, wide, deep = weights.shape
    latent = wide // QUAD
    for quad in range(quads):
        product = matmul_nt(weights[quad], source[:, quad * deep : (quad + 1) * deep])
        if factor != 1.0:
            product = product * factor
        product = product.astype(bf16)
        for h in range(QUAD):
            out_ref[quad * QUAD + h] = product[h * latent : (h + 1) * latent]


def seg_mask(diagonal, base, start):
    keys = start.shape[-1]
    key_at = lax.broadcasted_iota(jnp.int32, (keys, keys), 0)
    allow = key_at >= (start - base)
    if diagonal:
        allow = allow & (key_at <= lax.broadcasted_iota(jnp.int32, (keys, keys), 1))
    return allow


def attend_kernel(count, first, last, diagonal_at, lo, bases, *refs):
    refs = list(refs)
    take = lambda k: [refs.pop(0) for _ in range(k)]
    query_ref, start_ref, key_lift_ref = take(3)
    segs = take(count)
    if not first:
        top_in, total_in, mix_in = take(3)
    if last:
        (value_lift_ref,) = take(1)
        out_ref, lse_ref, mix_ref = take(3)
    else:
        top_out, total_out, mix_out = take(3)
    expanded, top, total, mix = take(4)
    heads = expanded.shape[0]
    tokens = query_ref.shape[1]
    row = pl.program_id(0)
    scale = HEAD_WIDTH ** (-0.5) * LOG2E
    expand_heads(query_ref[0], key_lift_ref, scale, expanded)
    if first:
        top[...] = jnp.full_like(top, blocked)
        total[...] = jnp.zeros_like(total)
        mix[...] = jnp.zeros_like(mix)
    else:
        top[...] = top_in[0]
        total[...] = total_in[0]
        mix[...] = mix_in[0]
    start = start_ref[0]
    for i in range(count):

        @pl.when((bases[i] >= 0) & (bases[i] + tokens - 1 >= lo[row]))
        def _():
            latent = segs[i][0]
            latent_t = latent.T
            allow = seg_mask(i == diagonal_at, bases[i], start)
            for h in range(heads):
                score = jnp.where(allow, matmul(latent, expanded[h]), blocked)
                old = top[h : h + 1]
                new = jnp.maximum(old, jnp.max(score, axis=0, keepdims=True))
                probs = jnp.exp2(score - new)
                fade = jnp.exp2(old - new)
                top[h : h + 1] = new
                total[h : h + 1] = total[h : h + 1] * fade + jnp.sum(probs, axis=0, keepdims=True)
                mix[h] = mix[h] * fade + matmul(latent_t, probs.astype(bf16))

    if not last:
        top_out[0] = top[...]
        total_out[0] = total[...]
        mix_out[0] = mix[...]
        return
    lse_ref[0] = top[...] + jnp.log2(total[...])
    inverse = 1.0 / total[...]
    quads, deep, wide = value_lift_ref.shape
    for h in range(heads):
        mix_ref[0, h] = (mix[h] * inverse[h : h + 1]).astype(bf16)
    for quad in range(quads):
        part = mix_ref[0, quad * QUAD : (quad + 1) * QUAD].reshape(wide, tokens)
        lifted = matmul(value_lift_ref[quad], part)
        out_ref[0, :, quad * deep : (quad + 1) * deep] = lifted.T.astype(bf16)


def whole(array):
    return pl.BlockSpec(array.shape, lambda *_: (0,) * array.ndim)


def by_row(shape):
    return pl.BlockSpec((1,) + tuple(shape[1:]), lambda r, *_: (r,) + (0,) * (len(shape) - 1))


def attend_part(queries, start, key_lift, value_lift, lo, segs, bases, diagonal_at, state, last):
    rows, tokens, width = queries.shape
    heads = width // HEAD_WIDTH
    latent = segs[0].shape[-1]
    state_shapes = [(rows, heads, tokens), (rows, heads, tokens), (rows, heads, latent, tokens)]
    args = [queries, start, key_lift, *segs]
    specs = [by_row(queries.shape), by_row(start.shape), whole(key_lift)]
    specs += [by_row(s.shape) for s in segs]
    if state is not None:
        args += list(state)
        specs += [by_row(s) for s in state_shapes]
    if last:
        args.append(value_lift)
        specs.append(whole(value_lift))
        outs = [
            jax.ShapeDtypeStruct(queries.shape, bf16),
            jax.ShapeDtypeStruct(state_shapes[0], f32),
            jax.ShapeDtypeStruct(state_shapes[2], bf16),
        ]
    else:
        outs = [jax.ShapeDtypeStruct(s, f32) for s in state_shapes]
    blocks = rows * heads * len(segs)
    return pl.pallas_call(
        functools.partial(attend_kernel, len(segs), state is None, last, diagonal_at),
        out_shape=outs,
        grid_spec=pltpu.PrefetchScalarGridSpec(
            num_scalar_prefetch=2,
            grid=(rows,),
            in_specs=specs,
            out_specs=[by_row(o.shape) for o in outs],
            scratch_shapes=[
                pltpu.VMEM((heads, latent, tokens), bf16),
                pltpu.VMEM((heads, tokens), f32),
                pltpu.VMEM((heads, tokens), f32),
                pltpu.VMEM((heads, latent, tokens), f32),
            ],
        ),
        compiler_params=pltpu.CompilerParams(
            dimension_semantics=("arbitrary",), vmem_limit_bytes=48 << 20
        ),
        cost_estimate=pl.CostEstimate(
            flops=blocks * tokens * tokens * latent * 4,
            bytes_accessed=rows * heads * latent * tokens * 4,
            transcendentals=blocks * tokens * tokens,
        ),
        name="attend",
    )(lo, bases, *args)


def attend_back_kernel(count, first, last, diagonal_at, lo, bases, *refs):
    refs = list(refs)
    take = lambda k: [refs.pop(0) for _ in range(k)]
    query_ref, grad_ref, lse_ref, mix_ref, start_ref, key_lift_ref, value_lift_ref = take(7)
    segs = take(count)
    if not first:
        (back_in,) = take(1)
    if last:
        (key_lift_t_ref,) = take(1)
    seg_grads = take(count)
    if last:
        query_back_ref, key_up_ref, value_up_ref = take(3)
    else:
        (back_out,) = take(1)
    expanded, expanded_grad, delta, back, part_key, part_value = take(6)
    heads, latent_size, tokens = expanded.shape
    row = pl.program_id(0)
    scale = HEAD_WIDTH ** (-0.5)
    expand_heads(query_ref[0], key_lift_ref, scale * LOG2E, expanded)
    expand_heads(grad_ref[0], value_lift_ref, 1.0, expanded_grad)
    for h in range(heads):
        delta[h : h + 1] = jnp.sum(
            mix_ref[0, h].astype(f32) * expanded_grad[h].astype(f32), axis=0, keepdims=True
        )
    if first:
        back[...] = jnp.zeros_like(back)
    else:
        back[...] = back_in[0]
    start = start_ref[0]
    for i in range(count):
        touched = (bases[i] >= 0) & (bases[i] + tokens - 1 >= lo[row])

        @pl.when(touched)
        def _():
            latent = segs[i][0]
            latent_t = latent.T
            allow = seg_mask(i == diagonal_at, bases[i], start)
            for h in range(heads):
                score = matmul(latent, expanded[h])
                probs = jnp.where(allow, jnp.exp2(score - lse_ref[0, h : h + 1]), 0.0)
                dprobs = matmul(latent, expanded_grad[h])
                dscore = (probs * (dprobs - delta[h : h + 1])).astype(bf16)
                back[h] += matmul(latent_t, dscore)
                by_key = matmul_nt(dscore, expanded[h])
                by_value = matmul_nt(probs.astype(bf16), expanded_grad[h])
                if h == 0:
                    part_key[...] = by_key
                    part_value[...] = by_value
                else:
                    part_key[...] += by_key
                    part_value[...] += by_value
            seg_grads[i][0] = (part_key[...] * LN2 + part_value[...]).astype(bf16)

        @pl.when(jnp.logical_not(touched))
        def _():
            seg_grads[i][0] = jnp.zeros((tokens, latent_size), bf16)

    if not last:
        back_out[0] = back[...]
        return

    @pl.when(row == 0)
    def _():
        key_up_ref[...] = jnp.zeros_like(key_up_ref)
        value_up_ref[...] = jnp.zeros_like(value_up_ref)

    quads, deep, wide = key_lift_t_ref.shape
    for quad in range(quads):
        part = (back[quad * QUAD : (quad + 1) * QUAD].reshape(wide, tokens) * scale).astype(bf16)
        lifted = matmul(key_lift_t_ref[quad], part)
        query_back_ref[0, :, quad * deep : (quad + 1) * deep] = lifted.T.astype(bf16)
        key_up_ref[quad] += matmul(part, query_ref[0, :, quad * deep : (quad + 1) * deep])
        mixed = mix_ref[0, quad * QUAD : (quad + 1) * QUAD].reshape(wide, tokens)
        value_up_ref[quad] += matmul(mixed, grad_ref[0, :, quad * deep : (quad + 1) * deep])


def attend_back_part(
    queries, grads, lse, mix, start, key_lift, value_lift, key_lift_t, lo, segs, bases,
    diagonal_at, state, last,
):
    rows, tokens, width = queries.shape
    heads = width // HEAD_WIDTH
    latent = segs[0].shape[-1]
    state_shape = (rows, heads, latent, tokens)
    args = [queries, grads, lse, mix, start, key_lift, value_lift, *segs]
    specs = [by_row(a.shape) for a in (queries, grads, lse, mix, start)]
    specs += [whole(key_lift), whole(value_lift)]
    specs += [by_row(s.shape) for s in segs]
    if state is not None:
        args.append(state)
        specs.append(by_row(state_shape))
    outs = [jax.ShapeDtypeStruct(s.shape, bf16) for s in segs]
    out_specs = [by_row(s.shape) for s in segs]
    if last:
        args.append(key_lift_t)
        specs.append(whole(key_lift_t))
        outs.append(jax.ShapeDtypeStruct(queries.shape, bf16))
        out_specs.append(by_row(queries.shape))
        for _ in range(2):
            outs.append(jax.ShapeDtypeStruct(key_lift.shape, f32))
            out_specs.append(whole(key_lift))
    else:
        outs.append(jax.ShapeDtypeStruct(state_shape, f32))
        out_specs.append(by_row(state_shape))
    blocks = rows * heads * len(segs)
    return pl.pallas_call(
        functools.partial(attend_back_kernel, len(segs), state is None, last, diagonal_at),
        out_shape=outs,
        grid_spec=pltpu.PrefetchScalarGridSpec(
            num_scalar_prefetch=2,
            grid=(rows,),
            in_specs=specs,
            out_specs=out_specs,
            scratch_shapes=[
                pltpu.VMEM((heads, latent, tokens), bf16),
                pltpu.VMEM((heads, latent, tokens), bf16),
                pltpu.VMEM((heads, tokens), f32),
                pltpu.VMEM((heads, latent, tokens), f32),
                pltpu.VMEM((tokens, latent), f32),
                pltpu.VMEM((tokens, latent), f32),
            ],
        ),
        compiler_params=pltpu.CompilerParams(
            dimension_semantics=("arbitrary",), vmem_limit_bytes=48 << 20
        ),
        cost_estimate=pl.CostEstimate(
            flops=blocks * tokens * tokens * latent * 10,
            bytes_accessed=rows * heads * latent * tokens * 8,
            transcendentals=blocks * tokens * tokens,
        ),
        name="attend_back",
    )(lo, bases, *args)


def quad_lift(lift):
    latent, width = lift.shape
    deep = QUAD * HEAD_WIDTH
    quads = width // deep
    tall = jnp.tile(lift.reshape(latent, quads, deep).transpose(1, 0, 2), (1, QUAD, 1))
    row_head = lax.broadcasted_iota(jnp.int32, tall.shape, 1) // latent
    column_head = lax.broadcasted_iota(jnp.int32, tall.shape, 2) // HEAD_WIDTH
    return jnp.where(row_head == column_head, tall, jnp.zeros_like(tall))


def quad_unlift(quad_grad):
    quads, wide, deep = quad_grad.shape
    latent = wide // QUAD
    column_head = lax.broadcasted_iota(jnp.int32, (latent, deep), 1) // HEAD_WIDTH
    parts = []
    for quad in range(quads):
        part = quad_grad[quad, :latent]
        for h in range(1, QUAD):
            part = jnp.where(column_head == h, quad_grad[quad, h * latent : (h + 1) * latent], part)
        parts.append(part)
    return jnp.concatenate(parts, axis=1)


def feed_kernel(core_ref, *refs):
    (
        inputs_ref, mine_ref, got_ref, output_ref, gain_ref, cotangent_ref, keep_ref,
        gate_t_ref, up_t_ref, down_ref, gate_ref, up_ref, down_t_ref,
        hidden_out_ref, grad_resid_ref, attn_back_ref, head_mine_ref, head_sent_ref, gain_grad_ref,
        grads_ref,
        normed, normed_t, back, back_t, resid, inverse, result_t, grad_t, staged, staged_out, sems, out_sem,
    ) = refs
    step = pl.program_id(0)
    steps = pl.num_programs(0)
    count, width = inputs_ref.shape
    pieces, _, piece = grads_ref.shape
    chunk = gate_t_ref.shape[0]
    ff = down_t_ref.shape[1] * steps
    block = min(256, count)
    core = core_ref[0]
    slot = step % 2

    def put(ref, value, at=0):
        for j in range(pieces):
            ref[j, pl.ds(at, value.shape[0])] = value[:, j * piece : (j + 1) * piece].astype(bf16)

    def leave(at, kind, place):
        return pltpu.make_async_copy(
            staged.at[at, kind],
            grads_ref.at[:, pl.ds(pl.multiple_of(kind * ff + place * chunk, chunk), chunk)],
            sems.at[at, kind],
        )

    @pl.when(step >= 2)
    def _():
        for kind in range(3):
            leave(slot, kind, step - 2).wait()

    @pl.when(step == 0)
    def _():
        for t in range(0, count, block):
            at = slice(t, t + block)
            row = inputs_ref[at].astype(f32) + (
                matmul(mine_ref[at], output_ref[core]) + matmul(got_ref[at], output_ref[1 - core])
            )
            resid[at] = row
            scale = lax.rsqrt(jnp.mean(row * row, axis=-1, keepdims=True) + epsilon)
            inverse[at] = scale
            unit = (row * scale * gain_ref[...]).astype(bf16)
            normed[at] = unit
            normed_t[:, at] = unit.T
            kept = (cotangent_ref[at].astype(f32) * keep_ref[at]).astype(bf16)
            back[at] = kept
            back_t[:, at] = kept.T
        result_t[...] = jnp.zeros_like(result_t)
        grad_t[...] = jnp.zeros_like(grad_t)

    gate = matmul(gate_t_ref[...], normed_t[...])
    up = matmul(up_t_ref[...], normed_t[...])
    grad_act = matmul(down_ref[...], back_t[...])
    sigmoid = 1.0 / (1.0 + jnp.exp(-gate))
    active = gate * sigmoid
    hidden = (active * up).astype(bf16)
    up_back = (grad_act * active).astype(bf16)
    gate_back = (grad_act * up * (sigmoid * (1.0 + gate * (1.0 - sigmoid)))).astype(bf16)
    put(staged.at[slot, 2], matmul(hidden, back[...]))
    put(staged.at[slot, 1], matmul(up_back, normed[...]))
    put(staged.at[slot, 0], matmul(gate_back, normed[...]))
    for kind in range(3):
        leave(slot, kind, step).start()
    result_t[...] += matmul(down_t_ref[...], hidden)
    grad_t[...] += matmul(gate_ref[...], gate_back) + matmul(up_ref[...], up_back)

    @pl.when(step == steps - 1)
    def _():
        gain_total = jnp.zeros((1, width), f32)
        for t in range(0, count, block):
            at = slice(t, t + block)
            row = resid[at]
            hidden_out_ref[at] = (row + result_t[:, at].T).astype(bf16)
            scale = inverse[at]
            unit = row * scale
            grad = grad_t[:, at].T
            gain_total += jnp.sum(grad * unit, axis=0, keepdims=True)
            scaled = grad * gain_ref[...]
            grad = back[at].astype(f32) + scale * (
                scaled - unit * jnp.mean(scaled * unit, axis=-1, keepdims=True)
            )
            grad_resid_ref[at] = grad
            low = grad.astype(bf16)
            attn_back_ref[at] = low
            head_mine_ref[at] = matmul_nt(low, output_ref[core]).astype(bf16)
            head_sent_ref[at] = matmul_nt(low, output_ref[1 - core]).astype(bf16)
        gain_grad_ref[...] = gain_total
        half = mine_ref.shape[1]
        put(staged_out, matmul_tn(mine_ref[...], attn_back_ref[...]), core * half)
        put(staged_out, matmul_tn(got_ref[...], attn_back_ref[...]), (1 - core) * half)
        last = pltpu.make_async_copy(staged_out, grads_ref.at[:, pl.ds(3 * ff, width)], out_sem)
        last.start()
        for kind in range(3):
            leave(1 - slot, kind, step - 1).wait()
            leave(slot, kind, step).wait()
        last.wait()


def feed(core, inputs, mixed_mine, mixed_got, output_weight, gain, cotangent, keep, weights, pieces):
    count, width = inputs.shape
    ff = weights[0].shape[0]
    chunk = 256
    piece = width // pieces
    output_weight = output_weight.reshape(2, -1, width)
    once = lambda a: pl.BlockSpec(a.shape, lambda *_: (0,) * len(a.shape), pipeline_mode=pl.Buffered(1))
    by_rows = pl.BlockSpec((chunk, width), lambda c, *_: (c, 0))
    by_columns = pl.BlockSpec((width, chunk), lambda c, *_: (0, c))
    shape = jax.ShapeDtypeStruct
    firsts = [inputs, mixed_mine, mixed_got, output_weight, gain.reshape(1, width), cotangent, keep]
    outs = [
        shape((count, width), bf16),
        shape((count, width), f32),
        shape((count, width), bf16),
        shape(mixed_mine.shape, bf16),
        shape(mixed_mine.shape, bf16),
        shape((1, width), f32),
        shape((pieces, 3 * ff + width, piece), bf16),
    ]
    return pl.pallas_call(
        feed_kernel,
        out_shape=outs,
        grid_spec=pltpu.PrefetchScalarGridSpec(
            num_scalar_prefetch=1,
            grid=(ff // chunk,),
            in_specs=[once(a) for a in firsts] + [by_rows] * 3 + [by_columns] * 3,
            out_specs=[once(o) for o in outs[:6]] + [pl.BlockSpec(memory_space=pl.ANY)],
            scratch_shapes=[
                pltpu.VMEM((count, width), bf16),
                pltpu.VMEM((width, count), bf16),
                pltpu.VMEM((count, width), bf16),
                pltpu.VMEM((width, count), bf16),
                pltpu.VMEM((count, width), f32),
                pltpu.VMEM((count, 1), f32),
                pltpu.VMEM((width, count), f32),
                pltpu.VMEM((width, count), f32),
                pltpu.VMEM((2, 3, pieces, chunk, piece), bf16),
                pltpu.VMEM((pieces, width, piece), bf16),
                pltpu.SemaphoreType.DMA((2, 3)),
                pltpu.SemaphoreType.DMA,
            ],
        ),
        compiler_params=pltpu.CompilerParams(
            dimension_semantics=("arbitrary",), vmem_limit_bytes=60 << 20
        ),
        cost_estimate=pl.CostEstimate(
            flops=count * width * (ff * 18 + width * 6),
            bytes_accessed=width * ff * 18 + count * width * 16,
            transcendentals=count * ff,
        ),
        name="feed",
    )(core.reshape(1), *firsts, *weights)


def flip(array, axis, bit):
    size = lax.axis_size(axis)
    return lax.ppermute(array, axis, [(i, i ^ (1 << bit)) for i in range(size)])


def add_sent(mine, other):
    return (mine.astype(f32) + other.astype(f32)).astype(bf16)


def finish_kernel(
    shares, early_ref, own_ref, sent_ref, out_ref, late_got, late_from, got_first, got_next,
    core_sems, along_sems, first_sems, first_late_sems, next_sems, out_sems,
):
    along, count, late_rows, piece = own_ref.shape
    shared_rows = sent_ref.shape[2]
    early_rows = sum(shares)
    bits = count.bit_length() - 1
    row_at = lax.axis_index("rows")
    place = lax.axis_index("heads")
    core = row_at % 2
    x_at = row_at // 2
    mesh = pl.DeviceIdType.MESH
    early_part = slice(0, early_rows)
    late_part = slice(early_rows, early_rows + late_rows)

    def turned(which):
        at = place
        for bit in which:
            at = at + (1 << bit) * (1 - 2 * ((place // (1 << bit)) % 2))
        return at

    core_peer = (row_at + 1 - 2 * core, place)
    x_others = [(x_at + d) % along for d in range(1, along)]
    x_peers = [(x * 2 + core, place) for x in x_others]
    head_peers = [(row_at, turned([bit])) for bit in range(bits)]
    barrier = pltpu.get_barrier_semaphore()
    everyone = [core_peer] + x_peers + head_peers
    for peer in everyone:
        pl.semaphore_signal(barrier, inc=1, device_id=peer, device_id_type=mesh)
    pl.semaphore_wait(barrier, len(everyone))

    def remote(source, target, sems, index, peer):
        return pltpu.make_async_remote_copy(
            src_ref=source, dst_ref=target, send_sem=sems.at[(0,) + index], recv_sem=sems.at[(1,) + index],
            device_id=peer, device_id_type=mesh,
        )

    def orders(bit):
        rest = list(range(bit + 1, bits))
        return [
            [b for i, b in enumerate(rest) if not (mask >> (len(rest) - 1 - i)) & 1]
            for mask in range(1 << len(rest))
        ]

    def add_rows(target, other, size):
        block = size if size <= 600 else size // 2

        def one(i, carry):
            at = pl.ds(pl.multiple_of(i * block, 16), block)
            target[at] = (target[at].astype(f32) + other[at].astype(f32)).astype(bf16)
            return carry

        lax.fori_loop(0, size // block, one, 0)

    first = orders(0)
    sections = []
    at, row = 0, 0
    for share in shares:
        sections.append((at, row, share))
        at += share * count
        row += share

    pending = []
    core_copy = remote(sent_ref, late_got, core_sems, (0,), core_peer)
    core_copy.start()

    def first_early(i, n):
        start, row, share = sections[n]
        shard = turned([0] + first[i])
        return remote(
            early_ref.at[pl.ds(pl.multiple_of(start + shard * share, 16), share)],
            got_first.at[i, pl.ds(row, share)],
            first_sems, (i, n), head_peers[0],
        )

    for i in range(len(first)):
        for n in range(len(sections)):
            first_early(i, n).start()

    core_copy.wait()

    def core_add(i, carry):
        j, s = i // count, i % count
        late_got[j, s] = (own_ref[j, s, :shared_rows].astype(f32) + late_got[j, s].astype(f32)).astype(bf16)
        return carry

    lax.fori_loop(0, along * count, core_add, 0)
    x_copies = []
    for d, (x, peer) in enumerate(zip(x_others, x_peers)):
        x_copies.append(
            remote(late_got.at[x], late_from.at[d, :, pl.ds(0, shared_rows)], along_sems, (d, 0), peer)
        )
        x_copies.append(
            remote(
                own_ref.at[x, :, pl.ds(shared_rows, late_rows - shared_rows)],
                late_from.at[d, :, pl.ds(shared_rows, late_rows - shared_rows)],
                along_sems, (d, 1), peer,
            )
        )
    for copy in x_copies:
        copy.start()

    def next_copy(bit, j, i, part, which):
        rows = pl.ds(part.start, part.stop - part.start)
        return remote(
            got_first.at[i, rows], got_next[bit - 1].at[j, rows], next_sems[bit - 1], (j, which), head_peers[bit]
        )

    def settle(i, part, which):
        rest = first[i]
        level = rest[0] if rest else bits
        size = part.stop - part.start
        rows = pl.ds(part.start, size)
        for bit in range(1, level):
            j = orders(bit).index(rest)
            next_copy(bit, j, i, part, which).wait_recv()
            add_rows(got_first.at[i, rows], got_next[bit - 1].at[j, rows], size)
        if rest:
            copy = next_copy(level, orders(level).index(rest[1:]), i, part, which)
            copy.start()
            pending.append(copy)

    def early_step(i):
        shard = turned(first[i])
        for n, (start, row, share) in enumerate(sections):
            first_early(i, n).wait()
            add_rows(
                got_first.at[i, pl.ds(row, share)],
                early_ref.at[pl.ds(pl.multiple_of(start + shard * share, 16), share)],
                share,
            )
        settle(i, early_part, 0)

    def first_late(i):
        return remote(
            late_from.at[0, turned([0] + first[i])],
            got_first.at[i, pl.ds(early_rows, late_rows)],
            first_late_sems, (i,), head_peers[0],
        )

    def late_begin():
        for copy in x_copies:
            copy.wait()

        def x_add(s, carry):
            shared = late_got[x_at, s].astype(f32)
            alone = own_ref[x_at, s, shared_rows:].astype(f32)
            for d in range(along - 1):
                shared = shared + late_from[d, s, :shared_rows].astype(f32)
                alone = alone + late_from[d, s, shared_rows:].astype(f32)
            late_from[0, s, :shared_rows] = shared.astype(bf16)
            late_from[0, s, shared_rows:] = alone.astype(bf16)
            return carry

        lax.fori_loop(0, count, x_add, 0)
        for i in range(len(first)):
            first_late(i).start()

    def late_step(i):
        first_late(i).wait()
        add_rows(got_first.at[i, pl.ds(early_rows, late_rows)], late_from.at[0, turned(first[i])], late_rows)
        settle(i, late_part, 1)

    final = len(first) - 1
    half = max(1, len(first) // 2)
    for i in range(half):
        early_step(i)
    late_begin()
    for i in range(half, final):
        early_step(i)
    for i in range(final):
        late_step(i)

    def spread(part, which):
        size = part.stop - part.start
        rows = pl.ds(part.start, size)
        out_ref[row_at, rows] = got_first[final, rows]
        copies = [remote(out_ref.at[row_at, rows], out_ref.at[row_at, rows], out_sems, (which, 0), core_peer)]
        for d, peer in enumerate(x_peers):
            copies.append(
                remote(out_ref.at[row_at, rows], out_ref.at[row_at, rows], out_sems, (which, 1 + d), peer)
            )
        for copy in copies:
            copy.start()
        return copies

    def pass_on(part, which, copies):
        rows = pl.ds(part.start, part.stop - part.start)
        more = []
        for d in range(along - 1):
            copies[1 + d].wait_recv()
            source = ((x_at + along - 1 - d) % along) * 2 + core
            more.append(
                remote(
                    out_ref.at[source, rows], out_ref.at[source, rows], out_sems, (which, along + d), core_peer
                )
            )
            more[-1].start()
        return more

    early_step(final)
    early_out = spread(early_part, 0)
    late_step(final)
    late_out = spread(late_part, 1)
    early_more = pass_on(early_part, 0, early_out)
    late_more = pass_on(late_part, 1, late_out)
    for copies, more in ((early_out, early_more), (late_out, late_more)):
        copies[0].wait()
        for copy in copies[1:]:
            copy.wait_send()
        for copy in more:
            copy.wait()
    for copy in pending:
        copy.wait_send()


def finish(early, own, sent, shares):
    along, count, late_rows, piece = own.shape
    bits = count.bit_length() - 1
    total = sum(shares) + late_rows
    vmem = pl.BlockSpec(memory_space=pltpu.VMEM)
    dma = pltpu.SemaphoreType.DMA

    def body(early_ref, own_ref, sent_ref, out_ref, late_got, late_from, got_first, *rest):
        got_next = rest[: bits - 1]
        core_sems, along_sems, first_sems, first_late_sems = rest[bits - 1 : bits + 3]
        next_sems = rest[bits + 3 : 2 * bits + 2]
        finish_kernel(
            shares, early_ref, own_ref, sent_ref, out_ref, late_got, late_from, got_first, got_next,
            core_sems, along_sems, first_sems, first_late_sems, next_sems, rest[-1],
        )

    return pl.pallas_call(
        body,
        out_shape=jax.ShapeDtypeStruct((2 * along, total, piece), bf16),
        in_specs=[vmem] * 3,
        out_specs=vmem,
        scratch_shapes=[
            pltpu.VMEM(sent.shape, bf16),
            pltpu.VMEM((along - 1, count, late_rows, piece), bf16),
            pltpu.VMEM((count // 2, total, piece), bf16),
        ]
        + [pltpu.VMEM((count >> (bit + 1), total, piece), bf16) for bit in range(1, bits)]
        + [
            dma((2, 1)),
            dma((2, along - 1, 2)),
            dma((2, count // 2, len(shares))),
            dma((2, count // 2)),
        ]
        + [dma((2, count >> (bit + 1), 2)) for bit in range(1, bits)]
        + [dma((2, 2, 2 * along))],
        compiler_params=pltpu.CompilerParams(
            collective_id=0, has_side_effects=True, vmem_limit_bytes=48 << 20
        ),
        name="finish",
    )(early, own, sent)


def shards(
    hidden_in,
    doc_ids,
    cotangent,
    attn_gain,
    query_weight,
    latent_weight,
    key_lift_weight,
    value_lift_weight,
    output_weight,
    ffn_gain,
    gate_weight,
    up_weight,
    down_weight,
):
    rows, tokens, width = hidden_in.shape
    peers = lax.axis_size("heads")
    place = lax.axis_index("heads")
    core = lax.axis_index("rows") & 1
    groups, latent_size, group_width = key_lift_weight.shape
    count = rows * tokens
    steps = peers // 2
    pieces = lax.axis_size("rows")
    share = width // peers
    side = place & 1
    level = place // 2
    swap = lambda a: flip(a, "rows", 0)
    mine = lambda a, axis: lax.dynamic_slice_in_dim(a, core * (a.shape[axis] // 2), a.shape[axis] // 2, axis)
    theirs = lambda a, axis: lax.dynamic_slice_in_dim(
        a, (1 - core) * (a.shape[axis] // 2), a.shape[axis] // 2, axis
    )

    own_base = place * tokens
    own_docs = lax.dynamic_slice_in_dim(doc_ids, own_base, tokens, 1)
    position = own_base + jnp.arange(tokens, dtype=jnp.int32)
    before = (doc_ids[:, None, :] == own_docs[:, :, None]) & (
        jnp.arange(doc_ids.shape[1], dtype=jnp.int32)[None, None, :] <= position[None, :, None]
    )
    own_start = position[None, :] + 1 - jnp.sum(before.astype(jnp.int32), axis=-1)
    start = jnp.concatenate([own_start, swap(own_start)], axis=0)
    lo = start[:, 0]
    start = start[:, None, :]

    inputs = hidden_in.reshape(count, width).astype(f32)
    inverse_one = rms_inverse(inputs)
    normed_one = (inputs * inverse_one * attn_gain).astype(bf16)
    latent_mine = matmul(normed_one, mine(latent_weight, 1)).astype(bf16)
    latent_sent = matmul(normed_one, theirs(latent_weight, 1)).astype(bf16)
    latent_got = swap(latent_sent)
    own_seg = jnp.concatenate([latent_mine, latent_got], axis=0).reshape(2 * rows, tokens, latent_size)
    query_mine = matmul(normed_one, mine(query_weight, 1)).astype(bf16)
    query_sent = matmul(normed_one, theirs(query_weight, 1)).astype(bf16)
    queries = jnp.concatenate([query_mine, swap(query_sent)], axis=0).reshape(2 * rows, tokens, group_width)

    key_mine = lax.dynamic_index_in_dim(key_lift_weight, core, 0, keepdims=False)
    value_mine = lax.dynamic_index_in_dim(value_lift_weight, core, 0, keepdims=False)
    key_lift = quad_lift(key_mine)
    value_lift = quad_lift(value_mine)
    key_lift_t = key_lift.transpose(0, 2, 1)
    value_lift_t = value_lift.transpose(0, 2, 1)

    up_chain = [(i, i + 2) for i in range(peers - 2)]
    down_chain = [(i + 2, i) for i in range(peers - 2)]
    weights = [gate_weight.T, up_weight.T, down_weight, gate_weight, up_weight, down_weight.T]
    queries, weights[0], weights[1], weights[5] = lax.optimization_barrier(
        (queries, weights[0], weights[1], weights[5])
    )
    segs = []
    bases = []
    moving = own_seg
    for k in range(steps):
        if k > 0:
            moving = lax.ppermute(moving, "heads", up_chain)
            if k > 1:
                moving, crossed = lax.optimization_barrier((moving, segs[-1][1]))
                segs[-1] = (segs[-1][0], crossed)
        segs.append((moving, flip(moving, "heads", 0)))
        base = ((level - k) * 2 + side) * tokens
        other = ((level - k) * 2 + 1 - side) * tokens
        there = level >= k
        bases.append(
            (jnp.where(there, base, -1), jnp.where(there & (other < own_base), other, -1))
        )

    def pick(ks):
        return (
            [s for k in ks for s in segs[k]],
            jnp.stack([b for k in ks for b in bases[k]]).astype(jnp.int32),
        )

    parts = [range(0, steps - 1), range(steps - 1, steps)]
    state = None
    for i, ks in enumerate(parts):
        seg_list, base_list = pick(ks)
        state = attend_part(
            queries, start, key_lift, value_lift_t, lo, seg_list, base_list,
            0 if i == 0 else -1, state, i == len(parts) - 1,
        )
    head_out, lse, head_mix = state
    mixed_mine = head_out[:rows].reshape(count, group_width)
    mixed_got = swap(head_out[rows:]).reshape(count, group_width)
    keep = (own_docs != 0).astype(f32).reshape(count, 1)
    (
        hidden_out, grad_resid, attn_back, grad_mixed_mine, grad_mixed_sent, ffn_gain_part,
        grads,
    ) = feed(
        core, hidden_in.reshape(count, width), mixed_mine, mixed_got, output_weight, ffn_gain,
        cotangent.reshape(count, width), keep, weights, pieces,
    )
    ffn_gain_part = ffn_gain_part[0]
    head_grads = jnp.concatenate([grad_mixed_mine, swap(grad_mixed_sent)], axis=0).reshape(
        2 * rows, tokens, group_width
    )

    early = lax.psum_scatter(grads, "rows", scatter_dimension=0, tiled=True)[0]

    back_parts = [[k] for k in range(steps - 1, 1, -1)] + [list(range(min(1, steps - 1), -1, -1))]
    state = None
    passing = None
    for i, ks in enumerate(back_parts):
        seg_list, base_list = pick(ks)
        done = i == len(back_parts) - 1
        outs = attend_back_part(
            queries, head_grads, lse, head_mix, start, key_lift, value_lift, key_lift_t, lo,
            seg_list, base_list, 2 * len(ks) - 2 if done else -1, state, done,
        )
        for j, k in enumerate(ks):
            total = outs[2 * j].astype(f32) + flip(outs[2 * j + 1], "heads", 0).astype(f32)
            if passing is not None:
                total = total + passing.astype(f32)
            passing = total.astype(bf16)
            if k > 0:
                passing = lax.ppermute(passing, "heads", down_chain)
        if done:
            query_grads, key_up_quads, value_up_quads = outs[2 * len(ks) :]
        else:
            state = outs[2 * len(ks)]
    latent_grads = passing

    query_back_mine = query_grads[:rows].reshape(count, group_width)
    query_back_got = swap(query_grads[rows:]).reshape(count, group_width)
    latent_back_mine = latent_grads[:rows].reshape(count, latent_size)
    latent_back_got = swap(latent_grads[rows:]).reshape(count, latent_size)
    along = pieces // 2
    piece = width // pieces

    def to_pieces(array, shards_first):
        array = array.reshape(shards_first, array.shape[0] // shards_first, along, piece)
        return array.transpose(2, 0, 1, 3)

    def latent_fold(array):
        array = array.reshape(peers, 2, array.shape[0] // peers // 2, array.shape[1])
        return jnp.concatenate([array[:, 0], array[:, 1]], axis=-1).reshape(-1, 2 * array.shape[-1])

    def late_pieces(query_part, latent_part, gains):
        gains = jnp.pad(gains.astype(bf16).reshape(peers, 1, share), ((0, 0), (0, 15), (0, group_width - share)))
        return [
            to_pieces(query_part.astype(bf16), peers),
            to_pieces(latent_fold(latent_part.astype(bf16)), peers),
            to_pieces(gains.reshape(peers * 16, group_width), peers),
        ]

    grad_one = (
        matmul_nt(query_back_mine, mine(query_weight, 1))
        + matmul_nt(query_back_got, theirs(query_weight, 1))
        + matmul_nt(latent_back_mine, mine(latent_weight, 1))
        + matmul_nt(latent_back_got, theirs(latent_weight, 1))
    )
    unit_one = inputs * inverse_one
    grad_in_norm, attn_gain_part = norm_back(grad_one, unit_one, inverse_one, attn_gain)
    hidden_grad = (grad_resid + grad_in_norm).reshape(rows, tokens, width)

    lift_share = latent_size // peers
    ff_share = gate_weight.shape[1] // peers
    key_part = quad_unlift(key_up_quads).astype(bf16)
    value_part = quad_unlift(value_up_quads).astype(bf16)
    own = jnp.concatenate(
        late_pieces(
            matmul_tn(normed_one, query_back_mine),
            matmul_tn(normed_one, latent_back_mine),
            jnp.where(core == 0, attn_gain_part, ffn_gain_part),
        )
        + [to_pieces(key_part, peers), to_pieces(value_part, peers)],
        axis=2,
    )
    sent = jnp.concatenate(
        late_pieces(
            matmul_tn(normed_one, query_back_got),
            matmul_tn(normed_one, latent_back_got),
            jnp.where(core == 0, ffn_gain_part, attn_gain_part),
        ),
        axis=2,
    )
    full = finish(early, own, sent, (ff_share, ff_share, ff_share, share))

    early_rows = 3 * ff_share + share
    early_full = full[:, :early_rows].transpose(1, 0, 2).reshape(early_rows, width).astype(f32)
    gate_share = early_full[:ff_share].T
    up_share = early_full[ff_share : 2 * ff_share].T
    down_share = early_full[2 * ff_share : 3 * ff_share]
    output_share = early_full[3 * ff_share :]
    late_full = full[:, early_rows:].reshape(along, 2, -1, piece).transpose(1, 2, 0, 3)
    late_full = late_full.reshape(2, -1, group_width).astype(f32)
    at = 0

    def cut(size):
        nonlocal at
        found = late_full[:, at : at + size]
        at += size
        return found

    beside = lambda pair: jnp.concatenate([pair[0], pair[1]], axis=-1)
    query_share = beside(cut(share))
    fold = cut(share // 2)
    latent_share = jnp.concatenate(
        [
            jnp.concatenate([fold[0, :, :latent_size], fold[1, :, :latent_size]], axis=-1),
            jnp.concatenate([fold[0, :, latent_size:], fold[1, :, latent_size:]], axis=-1),
        ],
        axis=0,
    )
    gains = cut(16)
    key_share = cut(lift_share)
    value_share = cut(lift_share)
    return (
        hidden_out.reshape(rows, tokens, width),
        hidden_grad,
        gains[0, 0, :share],
        query_share,
        latent_share,
        key_share,
        value_share,
        output_share,
        gains[1, 0, :share],
        gate_share,
        up_share,
        down_share,
    )


def solution(mesh):
    placed = (
        P("rows", "heads", None),
        P("rows", None),
        P("rows", "heads", None),
        P(),
        P(),
        P(),
        P(),
        P(),
        P(),
        P(),
        P(),
        P(),
        P(),
    )
    return jax.shard_map(
        shards,
        mesh=mesh,
        in_specs=placed,
        out_specs=(
            P("rows", "heads", None),
            P("rows", "heads", None),
            P("heads"),
            P("heads", None),
            P("heads", None),
            P(None, "heads", None),
            P(None, "heads", None),
            P("heads", None),
            P("heads"),
            P(None, "heads"),
            P(None, "heads"),
            P("heads", None),
        ),
        check_vma=False,
    )
```

```python
import functools
import math

import jax
import jax.numpy as jnp
from jax import lax
from jax.experimental import pallas as pl
from jax.experimental.pallas import tpu as pltpu
from jax.sharding import PartitionSpec as P

HEAD_WIDTH = 64
epsilon = 1e-05
blocked = -1e30
LOG2E = math.log2(math.e)
LN2 = math.log(2.0)
QUAD = 4
FORWARD_GROUP = 1
BACKWARD_GROUP = 8
f32 = jnp.float32
bf16 = jnp.bfloat16


def matmul(left, right):
    return jnp.dot(left, right, preferred_element_type=f32)


def matmul_nt(left, right):
    return lax.dot_general(
        left, right, (((left.ndim - 1,), (right.ndim - 1,)), ((), ())), preferred_element_type=f32
    )


def matmul_tn(left, right):
    return lax.dot_general(left, right, (((0,), (0,)), ((), ())), preferred_element_type=f32)


def rms_inverse(value_matrix):
    return lax.rsqrt(jnp.mean(value_matrix * value_matrix, axis=-1, keepdims=True) + epsilon)


def expand_heads(source, weights, factor, out_ref):
    tokens = source.shape[0]
    quads, wide, deep = weights.shape
    latent = wide // QUAD
    for quad in range(quads):
        product = matmul_nt(weights[quad], source[:, quad * deep : (quad + 1) * deep])
        if factor != 1.0:
            product = product * factor
        product = product.astype(bf16)
        for h in range(QUAD):
            at = (quad * QUAD + h) * tokens
            out_ref[:, at : at + tokens] = product[h * latent : (h + 1) * latent]


def lift_heads(source, weights, tokens):
    parts = [
        matmul(weights[h], source[:, h * tokens : (h + 1) * tokens]) for h in range(weights.shape[0])
    ]
    return jnp.concatenate(parts, axis=0)


def lift_grad(left, right, tokens, out_ref):
    latent = left.shape[0]
    deep = QUAD * HEAD_WIDTH
    head = lax.broadcasted_iota(jnp.int32, (latent, deep), 1) // HEAD_WIDTH
    for quad in range(right.shape[1] // deep):
        columns = slice(quad * deep, (quad + 1) * deep)
        found = None
        for h in range(QUAD):
            at = (quad * QUAD + h) * tokens
            part = matmul(left[:, at : at + tokens], right[:, columns])
            found = part if h == 0 else jnp.where(head == h, part, found)
        out_ref[:, columns] += found


def seg_mask(diagonal, base, start, heads):
    tokens = start.shape[-1]
    start = jnp.concatenate([start - base] * heads, axis=1)
    key_at = lax.broadcasted_iota(jnp.int32, (tokens, heads * tokens), 0)
    allow = key_at >= start
    if diagonal:
        at = lax.broadcasted_iota(jnp.int32, (1, tokens), 1)
        allow = allow & (key_at <= jnp.concatenate([at] * heads, axis=1))
    return allow


def attend_kernel(count, first, last, diagonal_at, lo, bases, *refs):
    refs = list(refs)
    take = lambda k: [refs.pop(0) for _ in range(k)]
    query_ref, start_ref, key_lift_ref = take(3)
    segs = take(count)
    if not first:
        top_in, total_in, mix_in = take(3)
    if last:
        (value_lift_ref,) = take(1)
        out_ref, lse_ref, mix_ref = take(3)
    else:
        top_out, total_out, mix_out = take(3)
    expanded, top, total, mix = take(4)
    tokens = query_ref.shape[1]
    heads = expanded.shape[1] // tokens
    row = pl.program_id(0)
    scale = HEAD_WIDTH ** (-0.5) * LOG2E
    touches = [(bases[i] >= 0) & (bases[i] + tokens - 1 >= lo[row]) for i in range(count)]
    if first:
        expand_heads(query_ref[0], key_lift_ref, scale, expanded)
        top[...] = jnp.full_like(top, blocked)
        total[...] = jnp.zeros_like(total)
        mix[...] = jnp.zeros_like(mix)
    else:
        top[...] = top_in[0]
        total[...] = total_in[0]
        mix[...] = mix_in[0].astype(f32)

        @pl.when(functools.reduce(jnp.logical_or, touches))
        def _():
            expand_heads(query_ref[0], key_lift_ref, scale, expanded)

    start = start_ref[0]
    for i in range(count):

        @pl.when(touches[i])
        def _():
            latent = segs[i][0]
            latent_t = latent.T
            allow = seg_mask(i == diagonal_at, bases[i], start, FORWARD_GROUP)
            for g in range(0, heads, FORWARD_GROUP):
                at = slice(g * tokens, (g + FORWARD_GROUP) * tokens)
                score = jnp.where(allow, matmul(latent, expanded[:, at]), blocked)
                old = top[:, at]
                new = jnp.maximum(old, jnp.max(score, axis=0, keepdims=True))
                probs = jnp.exp2(score - new)
                fade = jnp.exp2(old - new)
                top[:, at] = new
                total[:, at] = total[:, at] * fade + jnp.sum(probs, axis=0, keepdims=True)
                mix[:, at] = mix[:, at] * fade + matmul(latent_t, probs.astype(bf16))

    if not last:
        top_out[0] = top[...]
        total_out[0] = total[...]
        mix_out[0] = mix[...].astype(bf16)
        return
    lse_ref[0] = top[...] + jnp.log2(total[...])
    mix_ref[0] = (mix[...] * (1.0 / total[...])).astype(bf16)
    out_ref[0] = lift_heads(mix_ref[0], value_lift_ref, tokens).T.astype(bf16)


def whole(array):
    return pl.BlockSpec(array.shape, lambda *_: (0,) * len(array.shape))


def by_row(shape):
    return pl.BlockSpec((1,) + tuple(shape[1:]), lambda r, *_: (r,) + (0,) * (len(shape) - 1))


def attend_part(queries, start, key_lift, value_lift_t, lo, segs, bases, diagonal_at, state, last):
    rows, tokens, width = queries.shape
    heads = width // HEAD_WIDTH
    latent = segs[0].shape[-1]
    shape = jax.ShapeDtypeStruct
    stat = shape((rows, 1, heads * tokens), f32)
    state_shapes = [stat, stat, shape((rows, latent, heads * tokens), bf16)]
    args = [queries, start, key_lift, *segs]
    specs = [by_row(queries.shape), by_row(start.shape), whole(key_lift)]
    specs += [by_row(s.shape) for s in segs]
    if state is not None:
        args += list(state)
        specs += [by_row(s.shape) for s in state_shapes]
    if last:
        args.append(value_lift_t)
        specs.append(whole(value_lift_t))
        outs = [shape(queries.shape, bf16), stat, state_shapes[2]]
    else:
        outs = state_shapes
    blocks = rows * heads * len(segs)
    return pl.pallas_call(
        functools.partial(attend_kernel, len(segs), state is None, last, diagonal_at),
        out_shape=outs,
        grid_spec=pltpu.PrefetchScalarGridSpec(
            num_scalar_prefetch=2,
            grid=(rows,),
            in_specs=specs,
            out_specs=[by_row(o.shape) for o in outs],
            scratch_shapes=[
                pltpu.VMEM((latent, heads * tokens), bf16),
                pltpu.VMEM((1, heads * tokens), f32),
                pltpu.VMEM((1, heads * tokens), f32),
                pltpu.VMEM((latent, heads * tokens), f32),
            ],
        ),
        compiler_params=pltpu.CompilerParams(
            dimension_semantics=("arbitrary",), vmem_limit_bytes=48 << 20
        ),
        cost_estimate=pl.CostEstimate(
            flops=blocks * tokens * tokens * latent * 4,
            bytes_accessed=rows * heads * latent * tokens * 4,
            transcendentals=blocks * tokens * tokens,
        ),
        name="attend",
    )(lo, bases, *args)


def attend_back_kernel(count, first, last, diagonal_at, lo, bases, *refs):
    refs = list(refs)
    take = lambda k: [refs.pop(0) for _ in range(k)]
    query_ref, grad_ref, lse_ref, mix_ref, start_ref, key_lift_ref, value_lift_ref, key_lift_t_ref = take(8)
    segs = take(count)
    if not first:
        query_back_in, key_up_in = take(2)
    seg_grads = take(count)
    query_back_ref, key_up_ref = take(2)
    if last:
        (value_up_ref,) = take(1)
    expanded, expanded_grad, delta, back, query_back = take(5)
    latent_size = expanded.shape[0]
    tokens = query_ref.shape[1]
    heads = expanded.shape[1] // tokens
    row = pl.program_id(0)
    scale = HEAD_WIDTH ** (-0.5)
    touches = [(bases[i] >= 0) & (bases[i] + tokens - 1 >= lo[row]) for i in range(count)]

    @pl.when(row == 0)
    def _():
        key_up_ref[...] = jnp.zeros_like(key_up_ref) if first else key_up_in[...]
        if last:
            value_up_ref[...] = jnp.zeros_like(value_up_ref)

    query_back[...] = jnp.zeros_like(query_back) if first else query_back_in[0]

    @pl.when(functools.reduce(jnp.logical_or, touches))
    def _():
        expand_heads(query_ref[0], key_lift_ref, scale * LOG2E, expanded)
        expand_heads(grad_ref[0], value_lift_ref, 1.0, expanded_grad)
        delta[...] = jnp.sum(mix_ref[0].astype(f32) * expanded_grad[...].astype(f32), axis=0, keepdims=True)
        back[...] = jnp.zeros_like(back)

    start = start_ref[0]
    for i in range(count):

        @pl.when(touches[i])
        def _():
            latent = segs[i][0]
            latent_t = latent.T
            allow = seg_mask(i == diagonal_at, bases[i], start, BACKWARD_GROUP)
            by_key = by_value = None
            for g in range(0, heads, BACKWARD_GROUP):
                at = slice(g * tokens, (g + BACKWARD_GROUP) * tokens)
                score = matmul(latent, expanded[:, at])
                dprobs = matmul(latent, expanded_grad[:, at])
                probs = jnp.where(allow, jnp.exp2(score - lse_ref[0, :, at]), 0.0)
                dscore = (probs * (dprobs - delta[:, at])).astype(bf16)
                key_term = matmul_nt(dscore, expanded[:, at])
                value_term = matmul_nt(probs.astype(bf16), expanded_grad[:, at])
                by_key = key_term if g == 0 else by_key + key_term
                by_value = value_term if g == 0 else by_value + value_term
                back[:, at] += matmul(latent_t, dscore)
            seg_grads[i][0] = (by_key * LN2 + by_value).astype(bf16)

        @pl.when(jnp.logical_not(touches[i]))
        def _():
            seg_grads[i][0] = jnp.zeros((tokens, latent_size), bf16)

    @pl.when(functools.reduce(jnp.logical_or, touches))
    def _():
        part = (back[...] * scale).astype(bf16)
        query_back[...] += lift_heads(part, key_lift_t_ref, tokens)
        lift_grad(part, query_ref[0], tokens, key_up_ref)

    if last:
        lift_grad(mix_ref[0], grad_ref[0], tokens, value_up_ref)
        query_back_ref[0] = query_back[...].T.astype(bf16)
    else:
        query_back_ref[0] = query_back[...]


def attend_back_part(
    queries, grads, lse, mix, start, key_lift, value_lift, key_lift_t, lo, segs, bases,
    diagonal_at, state, last,
):
    rows, tokens, width = queries.shape
    heads = width // HEAD_WIDTH
    latent = segs[0].shape[-1]
    shape = jax.ShapeDtypeStruct
    back_shape = shape((rows, width, tokens), f32)
    up_shape = shape((latent, width), f32)
    args = [queries, grads, lse, mix, start, key_lift, value_lift, key_lift_t, *segs]
    specs = [by_row(a.shape) for a in (queries, grads, lse, mix, start)]
    specs += [whole(key_lift), whole(value_lift), whole(key_lift_t)]
    specs += [by_row(s.shape) for s in segs]
    if state is not None:
        args += list(state)
        specs += [by_row(back_shape.shape), whole(up_shape)]
    outs = [shape(s.shape, bf16) for s in segs]
    out_specs = [by_row(s.shape) for s in segs]
    outs += [shape(queries.shape, bf16) if last else back_shape, up_shape]
    out_specs += [by_row(outs[-2].shape), whole(up_shape)]
    if last:
        outs.append(up_shape)
        out_specs.append(whole(up_shape))
    blocks = rows * heads * len(segs)
    return pl.pallas_call(
        functools.partial(attend_back_kernel, len(segs), state is None, last, diagonal_at),
        out_shape=outs,
        grid_spec=pltpu.PrefetchScalarGridSpec(
            num_scalar_prefetch=2,
            grid=(rows,),
            in_specs=specs,
            out_specs=out_specs,
            scratch_shapes=[
                pltpu.VMEM((latent, heads * tokens), bf16),
                pltpu.VMEM((latent, heads * tokens), bf16),
                pltpu.VMEM((1, heads * tokens), f32),
                pltpu.VMEM((latent, heads * tokens), f32),
                pltpu.VMEM((width, tokens), f32),
            ],
        ),
        compiler_params=pltpu.CompilerParams(
            dimension_semantics=("arbitrary",), vmem_limit_bytes=48 << 20
        ),
        cost_estimate=pl.CostEstimate(
            flops=blocks * tokens * tokens * latent * 10,
            bytes_accessed=rows * heads * latent * tokens * 8,
            transcendentals=blocks * tokens * tokens,
        ),
        name="attend_back",
    )(lo, bases, *args)


def quad_lift(lift):
    latent, width = lift.shape
    deep = QUAD * HEAD_WIDTH
    quads = width // deep
    tall = jnp.tile(lift.reshape(latent, quads, deep).transpose(1, 0, 2), (1, QUAD, 1))
    row_head = lax.broadcasted_iota(jnp.int32, tall.shape, 1) // latent
    column_head = lax.broadcasted_iota(jnp.int32, tall.shape, 2) // HEAD_WIDTH
    return jnp.where(row_head == column_head, tall, jnp.zeros_like(tall))


def head_lift(lift):
    latent, width = lift.shape
    return lift.T.reshape(width // HEAD_WIDTH, HEAD_WIDTH, latent)


def put_pieces(ref, value, at=0):
    pieces, _, piece = ref.shape
    for j in range(pieces):
        ref[j, pl.ds(at, value.shape[0])] = value[:, j * piece : (j + 1) * piece].astype(bf16)


def feed_kernel(core_ref, *refs):
    (
        inputs_ref, mine_ref, got_ref, output_ref, gain_ref, cotangent_ref, keep_ref,
        gate_ref, up_ref, down_ref,
        hidden_out_ref, resid, normed, back, active_ref, slope_ref, down_grad_ref,
        result,
    ) = refs
    step = pl.program_id(0)
    count = inputs_ref.shape[0]
    block = min(256, count)
    core = core_ref[0]

    @pl.when(step == 0)
    def _():
        for t in range(0, count, block):
            at = slice(t, t + block)
            row = inputs_ref[at].astype(f32) + (
                matmul(mine_ref[at], output_ref[core]) + matmul(got_ref[at], output_ref[1 - core])
            )
            resid[at] = row
            scale = lax.rsqrt(jnp.mean(row * row, axis=-1, keepdims=True) + epsilon)
            normed[at] = (row * scale * gain_ref[...]).astype(bf16)
            back[at] = (cotangent_ref[at].astype(f32) * keep_ref[at]).astype(bf16)
        result[...] = jnp.zeros_like(result)

    gate = matmul(normed[...], gate_ref[...])
    up = matmul(normed[...], up_ref[...])
    sigmoid = 1.0 / (1.0 + jnp.exp(-gate))
    active = gate * sigmoid
    hidden = (active * up).astype(bf16)
    active_ref[...] = active.astype(bf16)
    slope_ref[...] = (up * (sigmoid * (1.0 + gate * (1.0 - sigmoid)))).astype(bf16)
    put_pieces(down_grad_ref, matmul_tn(hidden, back[...]))
    result[...] += matmul(hidden, down_ref[...])

    @pl.when(step == pl.num_programs(0) - 1)
    def _():
        hidden_out_ref[...] = (resid[...] + result[...]).astype(bf16)


def feed_back_kernel(core_ref, *refs):
    (
        mine_ref, got_ref, output_ref, gain_ref, resid_ref, normed, back,
        active_ref, slope_ref, gate_ref, up_ref, down_ref,
        grad_resid_ref, head_mine_ref, head_sent_ref, gain_grad_ref, grads_ref,
        grad_two, low, staged, staged_out, sems, out_sem,
    ) = refs
    step = pl.program_id(0)
    steps = pl.num_programs(0)
    count, width = resid_ref.shape
    chunk = down_ref.shape[0]
    ff = (grads_ref.shape[1] - width) // 2
    block = min(256, count)
    core = core_ref[0]
    slot = step % 2

    def leave(at, kind, place):
        return pltpu.make_async_copy(
            staged.at[at, kind],
            grads_ref.at[:, pl.ds(pl.multiple_of(kind * ff + place * chunk, chunk), chunk)],
            sems.at[at, kind],
        )

    @pl.when(step >= 2)
    def _():
        for kind in range(2):
            leave(slot, kind, step - 2).wait()

    @pl.when(step == 0)
    def _():
        grad_two[...] = jnp.zeros_like(grad_two)

    grad_act = matmul_nt(back[...], down_ref[...])
    up_back = (grad_act * active_ref[...].astype(f32)).astype(bf16)
    gate_back = (grad_act * slope_ref[...].astype(f32)).astype(bf16)
    put_pieces(staged.at[slot, 1], matmul_tn(up_back, normed[...]))
    put_pieces(staged.at[slot, 0], matmul_tn(gate_back, normed[...]))
    for kind in range(2):
        leave(slot, kind, step).start()
    grad_two[...] += matmul_nt(gate_back, gate_ref[...]) + matmul_nt(up_back, up_ref[...])

    @pl.when(step == steps - 1)
    def _():
        gain_total = jnp.zeros((1, width), f32)
        for t in range(0, count, block):
            at = slice(t, t + block)
            row = resid_ref[at]
            scale = lax.rsqrt(jnp.mean(row * row, axis=-1, keepdims=True) + epsilon)
            unit = row * scale
            grad = grad_two[at]
            gain_total += jnp.sum(grad * unit, axis=0, keepdims=True)
            scaled = grad * gain_ref[...]
            grad = back[at].astype(f32) + scale * (
                scaled - unit * jnp.mean(scaled * unit, axis=-1, keepdims=True)
            )
            grad_resid_ref[at] = grad
            low[at] = grad.astype(bf16)
            head_mine_ref[at] = matmul_nt(low[at], output_ref[core]).astype(bf16)
            head_sent_ref[at] = matmul_nt(low[at], output_ref[1 - core]).astype(bf16)
        gain_grad_ref[...] = gain_total
        half = mine_ref.shape[1]
        put_pieces(staged_out, matmul_tn(mine_ref[...], low[...]), core * half)
        put_pieces(staged_out, matmul_tn(got_ref[...], low[...]), (1 - core) * half)
        last = pltpu.make_async_copy(staged_out, grads_ref.at[:, pl.ds(2 * ff, width)], out_sem)
        last.start()
        for kind in range(2):
            leave(1 - slot, kind, step - 1).wait()
            leave(slot, kind, step).wait()
        last.wait()


def once(array):
    return pl.BlockSpec(array.shape, lambda *_: (0,) * len(array.shape), pipeline_mode=pl.Buffered(1))


def feed(core, inputs, mixed_mine, mixed_got, output_weight, gain, cotangent, keep, weights, pieces):
    count, width = inputs.shape
    gate_weight, up_weight, down_weight = weights
    ff = gate_weight.shape[1]
    chunk = 256
    piece = width // pieces
    output_weight = output_weight.reshape(2, -1, width)
    gain = gain.reshape(1, width)
    by_rows = pl.BlockSpec((chunk, width), lambda c, *_: (c, 0))
    by_columns = pl.BlockSpec((width, chunk), lambda c, *_: (0, c))
    kept_columns = pl.BlockSpec((count, chunk), lambda c, *_: (0, c))
    shape = jax.ShapeDtypeStruct
    params = pltpu.CompilerParams(dimension_semantics=("arbitrary",), vmem_limit_bytes=60 << 20)
    full_bf, full_f = shape((count, width), bf16), shape((count, width), f32)
    kept = shape((count, ff), bf16)
    firsts = [inputs, mixed_mine, mixed_got, output_weight, gain, cotangent, keep]
    outs = [full_bf, full_f, full_bf, full_bf, kept, kept, shape((pieces, ff, piece), bf16)]
    hidden_out, resid, normed, back, active, slope, down_grad = pl.pallas_call(
        feed_kernel,
        out_shape=outs,
        grid_spec=pltpu.PrefetchScalarGridSpec(
            num_scalar_prefetch=1,
            grid=(ff // chunk,),
            in_specs=[once(a) for a in firsts] + [by_columns, by_columns, by_rows],
            out_specs=[once(o) for o in outs[:4]]
            + [kept_columns, kept_columns, pl.BlockSpec((pieces, chunk, piece), lambda c, *_: (0, c, 0))],
            scratch_shapes=[pltpu.VMEM((count, width), f32)],
        ),
        compiler_params=params,
        cost_estimate=pl.CostEstimate(
            flops=count * width * (ff * 8 + width * 2),
            bytes_accessed=width * ff * 8 + count * width * 16 + count * ff * 4,
            transcendentals=count * ff,
        ),
        name="feed",
    )(core.reshape(1), *firsts, *weights)
    firsts = [mixed_mine, mixed_got, output_weight, gain, resid, normed, back]
    outs = [
        full_f,
        shape(mixed_mine.shape, bf16),
        shape(mixed_mine.shape, bf16),
        shape((1, width), f32),
        shape((pieces, 2 * ff + width, piece), bf16),
    ]
    grad_resid, head_mine, head_sent, gain_grad, grads = pl.pallas_call(
        feed_back_kernel,
        out_shape=outs,
        grid_spec=pltpu.PrefetchScalarGridSpec(
            num_scalar_prefetch=1,
            grid=(ff // chunk,),
            in_specs=[once(a) for a in firsts]
            + [kept_columns, kept_columns, by_columns, by_columns, by_rows],
            out_specs=[once(o) for o in outs[:4]] + [pl.BlockSpec(memory_space=pl.ANY)],
            scratch_shapes=[
                pltpu.VMEM((count, width), f32),
                pltpu.VMEM((count, width), bf16),
                pltpu.VMEM((2, 2, pieces, chunk, piece), bf16),
                pltpu.VMEM((pieces, width, piece), bf16),
                pltpu.SemaphoreType.DMA((2, 2)),
                pltpu.SemaphoreType.DMA,
            ],
        ),
        compiler_params=params,
        cost_estimate=pl.CostEstimate(
            flops=count * width * (ff * 10 + width * 4),
            bytes_accessed=width * ff * 10 + count * width * 20 + count * ff * 4,
            transcendentals=0,
        ),
        name="feed_back",
    )(core.reshape(1), *firsts, active, slope, *weights)
    return hidden_out, grad_resid, head_mine, head_sent, gain_grad, down_grad, grads


def flip(array, axis, bit):
    size = lax.axis_size(axis)
    return lax.ppermute(array, axis, [(i, i ^ (1 << bit)) for i in range(size)])


def late_parts(core, inputs_ref, gain_ref, back_refs, query_ref, latent_ref, resid_ref, other_gain_ref, up_refs, normed, own, sent, grad_ref):
    along, count, _, piece = own.shape
    tokens, width = inputs_ref.shape
    query_mine, query_got, latent_mine, latent_got = back_refs
    share = width // count
    fold = share // 2
    latent = latent_mine.shape[1]
    half = query_mine.shape[1]
    block = min(256, tokens)
    mine = lambda ref, size: ref[:, pl.ds(pl.multiple_of(core * size, size), size)]
    theirs = lambda ref, size: ref[:, pl.ds(pl.multiple_of((1 - core) * size, size), size)]
    gain_total = jnp.zeros((1, width), f32)
    for t in range(0, tokens, block):
        at = slice(t, t + block)
        row = inputs_ref[at].astype(f32)
        scale = lax.rsqrt(jnp.mean(row * row, axis=-1, keepdims=True) + epsilon)
        unit = row * scale
        normed[at] = (unit * gain_ref[...]).astype(bf16)
        grad = (
            matmul_nt(query_mine[at], mine(query_ref, half))
            + matmul_nt(query_got[at], theirs(query_ref, half))
            + matmul_nt(latent_mine[at], mine(latent_ref, latent))
            + matmul_nt(latent_got[at], theirs(latent_ref, latent))
        )
        gain_total += jnp.sum(grad * unit, axis=0, keepdims=True)
        scaled = grad * gain_ref[...]
        grad_ref[at] = resid_ref[at] + scale * (
            scaled - unit * jnp.mean(scaled * unit, axis=-1, keepdims=True)
        )
    other = other_gain_ref[...]
    gains = (jnp.where(core == 0, gain_total, other), jnp.where(core == 0, other, gain_total))
    lane = max(share, 128)
    for target, query, latents, gain in (
        (own, query_mine, latent_mine, gains[0]),
        (sent, query_got, latent_got, gains[1]),
    ):
        query_grad = matmul_tn(normed[...], query[...]).astype(bf16)
        latent_grad = matmul_tn(normed[...], latents[...]).astype(bf16)
        for s in range(count):
            first = s * share
            begin = first // lane * lane
            for j in range(along):
                target[j, s, :share] = query_grad[first : first + share, j * piece : (j + 1) * piece]
                side, column = divmod(j * piece, latent)
                target[j, s, share : share + fold] = latent_grad[
                    first + side * fold : first + (side + 1) * fold, column : column + piece
                ]
                rows = slice(share + fold, share + fold + 16)
                if j == 0:
                    kept = jnp.broadcast_to(gain[:, begin : begin + lane], (16, lane)).astype(bf16)
                    target[j, s, rows, :lane] = kept
                    if piece > lane:
                        target[j, s, rows, lane:] = jnp.zeros((16, piece - lane), bf16)
                else:
                    target[j, s, rows] = jnp.zeros((16, piece), bf16)
    lift = latent // count
    at = share + fold + 16
    for ref in up_refs:
        for s in range(count):
            for j in range(along):
                own[j, s, at : at + lift] = ref[s * lift : (s + 1) * lift, j * piece : (j + 1) * piece].astype(bf16)
        at += lift


def finish_kernel(
    sections, early_refs, late_compute, own_ref, sent_ref, out_ref, late_got, late_from, got_first, got_next,
    core_sems, along_sems, first_sems, first_late_sems, next_sems, out_sems,
):
    along, count, late_rows, piece = own_ref.shape
    shared_rows = sent_ref.shape[2]
    early_rows = sum(section[2] for section in sections)
    bits = count.bit_length() - 1
    row_at = lax.axis_index("rows")
    place = lax.axis_index("heads")
    core = row_at % 2
    x_at = row_at // 2
    mesh = pl.DeviceIdType.MESH
    early_part = slice(0, early_rows)
    late_part = slice(early_rows, early_rows + late_rows)

    def turned(which):
        at = place
        for bit in which:
            at = at + (1 << bit) * (1 - 2 * ((place // (1 << bit)) % 2))
        return at

    core_peer = (row_at + 1 - 2 * core, place)
    x_others = [(x_at + d) % along for d in range(1, along)]
    x_peers = [(x * 2 + core, place) for x in x_others]
    head_peers = [(row_at, turned([bit])) for bit in range(bits)]
    barrier = pltpu.get_barrier_semaphore()
    everyone = [core_peer] + x_peers + head_peers
    for peer in everyone:
        pl.semaphore_signal(barrier, inc=1, device_id=peer, device_id_type=mesh)
    pl.semaphore_wait(barrier, len(everyone))

    def remote(source, target, sems, index, peer):
        return pltpu.make_async_remote_copy(
            src_ref=source, dst_ref=target, send_sem=sems.at[(0,) + index], recv_sem=sems.at[(1,) + index],
            device_id=peer, device_id_type=mesh,
        )

    def orders(bit):
        rest = list(range(bit + 1, bits))
        return [
            [b for i, b in enumerate(rest) if not (mask >> (len(rest) - 1 - i)) & 1]
            for mask in range(1 << len(rest))
        ]

    def add_rows(target, other, size):
        block = size if size <= 600 else size // 2

        def one(i, carry):
            at = pl.ds(pl.multiple_of(i * block, 16), block)
            target[at] = (target[at].astype(f32) + other[at].astype(f32)).astype(bf16)
            return carry

        lax.fori_loop(0, size // block, one, 0)

    first = orders(0)
    pending = []

    def early_rows_of(n, shard):
        which, start, share, _ = sections[n]
        return early_refs[which].at[pl.ds(pl.multiple_of(start + shard * share, 16), share)]

    def first_early(i, n):
        _, _, share, row = sections[n]
        return remote(
            early_rows_of(n, turned([0] + first[i])), got_first.at[i, pl.ds(row, share)],
            first_sems, (i, n), head_peers[0],
        )

    for i in range(len(first)):
        for n in range(len(sections)):
            first_early(i, n).start()

    late_compute(core)
    core_copy = remote(sent_ref, late_got, core_sems, (0,), core_peer)
    core_copy.start()
    core_copy.wait()

    def core_add(i, carry):
        j, s = i // count, i % count
        late_got[j, s] = (own_ref[j, s, :shared_rows].astype(f32) + late_got[j, s].astype(f32)).astype(bf16)
        return carry

    lax.fori_loop(0, along * count, core_add, 0)
    x_copies = []
    for d, (x, peer) in enumerate(zip(x_others, x_peers)):
        x_copies.append(
            remote(late_got.at[x], late_from.at[d, :, pl.ds(0, shared_rows)], along_sems, (d, 0), peer)
        )
        x_copies.append(
            remote(
                own_ref.at[x, :, pl.ds(shared_rows, late_rows - shared_rows)],
                late_from.at[d, :, pl.ds(shared_rows, late_rows - shared_rows)],
                along_sems, (d, 1), peer,
            )
        )
    for copy in x_copies:
        copy.start()

    def next_copy(bit, j, i, part, which):
        rows = pl.ds(part.start, part.stop - part.start)
        return remote(
            got_first.at[i, rows], got_next[bit - 1].at[j, rows], next_sems[bit - 1], (j, which), head_peers[bit]
        )

    def settle(i, part, which):
        rest = first[i]
        level = rest[0] if rest else bits
        size = part.stop - part.start
        rows = pl.ds(part.start, size)
        for bit in range(1, level):
            j = orders(bit).index(rest)
            next_copy(bit, j, i, part, which).wait_recv()
            add_rows(got_first.at[i, rows], got_next[bit - 1].at[j, rows], size)
        if rest:
            copy = next_copy(level, orders(level).index(rest[1:]), i, part, which)
            copy.start()
            pending.append(copy)

    def early_step(i):
        for n, (_, _, share, row) in enumerate(sections):
            first_early(i, n).wait()
            add_rows(got_first.at[i, pl.ds(row, share)], early_rows_of(n, turned(first[i])), share)
        settle(i, early_part, 0)

    def first_late(i):
        return remote(
            late_from.at[0, turned([0] + first[i])],
            got_first.at[i, pl.ds(early_rows, late_rows)],
            first_late_sems, (i,), head_peers[0],
        )

    def late_begin():
        for copy in x_copies:
            copy.wait()

        def x_add(s, carry):
            shared = late_got[x_at, s].astype(f32)
            alone = own_ref[x_at, s, shared_rows:].astype(f32)
            for d in range(along - 1):
                shared = shared + late_from[d, s, :shared_rows].astype(f32)
                alone = alone + late_from[d, s, shared_rows:].astype(f32)
            late_from[0, s, :shared_rows] = shared.astype(bf16)
            late_from[0, s, shared_rows:] = alone.astype(bf16)
            return carry

        lax.fori_loop(0, count, x_add, 0)
        for i in range(len(first)):
            first_late(i).start()

    def late_step(i):
        first_late(i).wait()
        add_rows(got_first.at[i, pl.ds(early_rows, late_rows)], late_from.at[0, turned(first[i])], late_rows)
        settle(i, late_part, 1)

    final = len(first) - 1
    half = max(1, len(first) // 2)
    for i in range(half):
        early_step(i)
    late_begin()
    for i in range(half, final):
        early_step(i)
    for i in range(final):
        late_step(i)

    def spread(part, which):
        rows = pl.ds(part.start, part.stop - part.start)
        out_ref[row_at, rows] = got_first[final, rows]
        copies = [remote(out_ref.at[row_at, rows], out_ref.at[row_at, rows], out_sems, (which, 0), core_peer)]
        for d, peer in enumerate(x_peers):
            copies.append(
                remote(out_ref.at[row_at, rows], out_ref.at[row_at, rows], out_sems, (which, 1 + d), peer)
            )
        for copy in copies:
            copy.start()
        return copies

    def pass_on(part, which, copies):
        rows = pl.ds(part.start, part.stop - part.start)
        more = []
        for d in range(along - 1):
            copies[1 + d].wait_recv()
            source = ((x_at + along - 1 - d) % along) * 2 + core
            more.append(
                remote(
                    out_ref.at[source, rows], out_ref.at[source, rows], out_sems, (which, along + d), core_peer
                )
            )
            more[-1].start()
        return more

    early_step(final)
    early_out = spread(early_part, 0)
    late_step(final)
    late_out = spread(late_part, 1)
    early_more = pass_on(early_part, 0, early_out)
    late_more = pass_on(late_part, 1, late_out)
    for copies, more in ((early_out, early_more), (late_out, late_more)):
        copies[0].wait()
        for copy in copies[1:]:
            copy.wait_send()
        for copy in more:
            copy.wait()
    for copy in pending:
        copy.wait_send()


def finish(early, shares, count, late_args):
    inputs = late_args[0]
    tokens, width = inputs.shape
    piece = early[0].shape[1]
    along = width // piece // 2
    share = width // count
    bits = count.bit_length() - 1
    shared_rows = share + share // 2 + 16
    late_rows = shared_rows + 2 * (late_args[4].shape[1] // count)
    sections = []
    row = 0
    for which, of_one in enumerate(shares):
        start = 0
        for size in of_one:
            sections.append((which, start, size, row))
            start += size * count
            row += size
    total = row + late_rows
    vmem = pl.BlockSpec(memory_space=pltpu.VMEM)
    dma = pltpu.SemaphoreType.DMA

    def body(*refs):
        refs = list(refs)
        take = lambda k: [refs.pop(0) for _ in range(k)]
        early_refs = take(len(early))
        late_refs = take(len(late_args))
        out_ref, grad_ref = take(2)
        normed, own_ref, sent_ref, late_got, late_from, got_first = take(6)
        got_next = take(bits - 1)
        core_sems, along_sems, first_sems, first_late_sems = take(4)
        next_sems = take(bits - 1)
        (out_sems,) = take(1)
        (
            inputs_ref, gain_ref, query_mine, query_got, latent_mine, latent_got,
            query_ref, latent_ref, resid_ref, other_gain_ref, key_up, value_up,
        ) = late_refs

        def late_compute(core):
            late_parts(
                core, inputs_ref, gain_ref, (query_mine, query_got, latent_mine, latent_got),
                query_ref, latent_ref, resid_ref, other_gain_ref, (key_up, value_up),
                normed, own_ref, sent_ref, grad_ref,
            )

        finish_kernel(
            sections, early_refs, late_compute, own_ref, sent_ref, out_ref, late_got, late_from,
            got_first, got_next, core_sems, along_sems, first_sems, first_late_sems, next_sems, out_sems,
        )

    return pl.pallas_call(
        body,
        out_shape=[
            jax.ShapeDtypeStruct((2 * along, total, piece), bf16),
            jax.ShapeDtypeStruct((tokens, width), f32),
        ],
        in_specs=[vmem] * (len(early) + len(late_args)),
        out_specs=[vmem] * 2,
        scratch_shapes=[
            pltpu.VMEM((tokens, width), bf16),
            pltpu.VMEM((along, count, late_rows, piece), bf16),
            pltpu.VMEM((along, count, shared_rows, piece), bf16),
            pltpu.VMEM((along, count, shared_rows, piece), bf16),
            pltpu.VMEM((along - 1, count, late_rows, piece), bf16),
            pltpu.VMEM((count // 2, total, piece), bf16),
        ]
        + [pltpu.VMEM((count >> (bit + 1), total, piece), bf16) for bit in range(1, bits)]
        + [
            dma((2, 1)),
            dma((2, along - 1, 2)),
            dma((2, count // 2, len(sections))),
            dma((2, count // 2)),
        ]
        + [dma((2, count >> (bit + 1), 2)) for bit in range(1, bits)]
        + [dma((2, 2, 2 * along))],
        compiler_params=pltpu.CompilerParams(
            collective_id=0, has_side_effects=True, vmem_limit_bytes=60 << 20
        ),
        name="finish",
    )(*early, *late_args)


def lay_out_kernel(rows, latent, full_ref, gate_ref, up_ref, output_ref, down_ref, query_ref, latent_ref, key_ref, value_ref, gains_ref):
    pieces, _, piece = full_ref.shape
    at = 0
    for ref, size, turn in zip((gate_ref, up_ref, output_ref, down_ref), rows, (True, True, False, False)):
        for j in range(pieces):
            value = full_ref[j, at : at + size].astype(f32)
            if turn:
                ref[j * piece : (j + 1) * piece] = value.T
            else:
                ref[:, j * piece : (j + 1) * piece] = value
        at += size
    share = query_ref.shape[0]
    fold = share // 2
    lift = key_ref.shape[1]
    half = key_ref.shape[2]
    lane = gains_ref.shape[1]
    for j in range(pieces):
        x, core = divmod(j, 2)
        row = at
        query_ref[:, core * half + x * piece : core * half + (x + 1) * piece] = full_ref[
            j, row : row + share
        ].astype(f32)
        row += share
        side, column = divmod(x * piece, latent)
        column += core * latent
        latent_ref[side * fold : (side + 1) * fold, column : column + piece] = full_ref[
            j, row : row + fold
        ].astype(f32)
        row += fold
        if x == 0:
            gains_ref[core : core + 1] = full_ref[j, row : row + 16, :lane].astype(f32)[:1]
        row += 16
        for ref in (key_ref, value_ref):
            ref[core, :, x * piece : (x + 1) * piece] = full_ref[j, row : row + lift].astype(f32)
            row += lift


def lay_out(full, rows, share, latent, half, count, width):
    shape = jax.ShapeDtypeStruct
    gate, up, output, down = rows
    lift = latent // count
    vmem = pl.BlockSpec(memory_space=pltpu.VMEM)
    outs = [
        shape((width, gate), f32),
        shape((width, up), f32),
        shape((output, width), f32),
        shape((down, width), f32),
        shape((share, width), f32),
        shape((share, 2 * latent), f32),
        shape((2, lift, half), f32),
        shape((2, lift, half), f32),
        shape((2, max(share, 128)), f32),
    ]
    return pl.pallas_call(
        functools.partial(lay_out_kernel, rows, latent),
        out_shape=outs,
        in_specs=[vmem],
        out_specs=[vmem] * len(outs),
        compiler_params=pltpu.CompilerParams(vmem_limit_bytes=48 << 20),
        name="lay_out",
    )(full)


def shards(
    hidden_in,
    doc_ids,
    cotangent,
    attn_gain,
    query_weight,
    latent_weight,
    key_lift_weight,
    value_lift_weight,
    output_weight,
    ffn_gain,
    gate_weight,
    up_weight,
    down_weight,
):
    rows, tokens, width = hidden_in.shape
    peers = lax.axis_size("heads")
    place = lax.axis_index("heads")
    core = lax.axis_index("rows") & 1
    groups, latent_size, group_width = key_lift_weight.shape
    count = rows * tokens
    steps = peers // 2
    pieces = lax.axis_size("rows")
    share = width // peers
    side = place & 1
    level = place // 2
    swap = lambda a: flip(a, "rows", 0)
    mine = lambda a, axis: lax.dynamic_slice_in_dim(a, core * (a.shape[axis] // 2), a.shape[axis] // 2, axis)
    theirs = lambda a, axis: lax.dynamic_slice_in_dim(
        a, (1 - core) * (a.shape[axis] // 2), a.shape[axis] // 2, axis
    )

    own_base = place * tokens
    own_docs = lax.dynamic_slice_in_dim(doc_ids, own_base, tokens, 1)
    position = own_base + jnp.arange(tokens, dtype=jnp.int32)
    before = (doc_ids[:, None, :] == own_docs[:, :, None]) & (
        jnp.arange(doc_ids.shape[1], dtype=jnp.int32)[None, None, :] <= position[None, :, None]
    )
    own_start = position[None, :] + 1 - jnp.sum(before.astype(jnp.int32), axis=-1)
    start = jnp.concatenate([own_start, swap(own_start)], axis=0)
    lo = start[:, 0]
    start = start[:, None, :]

    inputs = hidden_in.reshape(count, width).astype(f32)
    inverse_one = rms_inverse(inputs)
    normed_one = (inputs * inverse_one * attn_gain).astype(bf16)
    latent_mine = matmul(normed_one, mine(latent_weight, 1)).astype(bf16)
    latent_sent = matmul(normed_one, theirs(latent_weight, 1)).astype(bf16)
    latent_got = swap(latent_sent)
    own_seg = jnp.concatenate([latent_mine, latent_got], axis=0).reshape(2 * rows, tokens, latent_size)
    query_mine = matmul(normed_one, mine(query_weight, 1)).astype(bf16)
    query_sent = matmul(normed_one, theirs(query_weight, 1)).astype(bf16)
    queries = jnp.concatenate([query_mine, swap(query_sent)], axis=0).reshape(2 * rows, tokens, group_width)

    key_mine = lax.dynamic_index_in_dim(key_lift_weight, core, 0, keepdims=False)
    value_mine = lax.dynamic_index_in_dim(value_lift_weight, core, 0, keepdims=False)
    key_lift = quad_lift(key_mine)
    value_lift = quad_lift(value_mine)
    key_lift_t = head_lift(key_mine)
    value_lift_t = head_lift(value_mine)

    up_chain = [(i, i + 2) for i in range(peers - 2)]
    down_chain = [(i + 2, i) for i in range(peers - 2)]
    segs = []
    bases = []
    moving = own_seg
    for k in range(steps):
        if k > 0:
            moving = lax.ppermute(moving, "heads", up_chain)
            if k > 1:
                moving, crossed = lax.optimization_barrier((moving, segs[-1][1]))
                segs[-1] = (segs[-1][0], crossed)
        segs.append((moving, flip(moving, "heads", 0)))
        base = ((level - k) * 2 + side) * tokens
        other = ((level - k) * 2 + 1 - side) * tokens
        there = level >= k
        bases.append(
            (jnp.where(there, base, -1), jnp.where(there & (other < own_base), other, -1))
        )

    def pick(ks):
        return (
            [s for k in ks for s in segs[k]],
            jnp.stack([b for k in ks for b in bases[k]]).astype(jnp.int32),
        )

    parts = [range(0, steps - 1), range(steps - 1, steps)]
    state = None
    for i, ks in enumerate(parts):
        seg_list, base_list = pick(ks)
        state = attend_part(
            queries, start, key_lift, value_lift_t, lo, seg_list, base_list,
            0 if i == 0 else -1, state, i == len(parts) - 1,
        )
    head_out, lse, head_mix = state
    mixed_mine = head_out[:rows].reshape(count, group_width)
    mixed_got = swap(head_out[rows:]).reshape(count, group_width)
    keep = (own_docs != 0).astype(f32).reshape(count, 1)
    hidden_out, grad_resid, grad_mixed_mine, grad_mixed_sent, ffn_gain_part, down_grad, feed_grads = feed(
        core, hidden_in.reshape(count, width), mixed_mine, mixed_got, output_weight, ffn_gain,
        cotangent.reshape(count, width), keep, (gate_weight, up_weight, down_weight), pieces,
    )
    head_grads = jnp.concatenate([grad_mixed_mine, swap(grad_mixed_sent)], axis=0).reshape(
        2 * rows, tokens, group_width
    )
    early_down = lax.psum_scatter(down_grad, "rows", scatter_dimension=0, tiled=True)[0]
    early_feed = lax.psum_scatter(feed_grads, "rows", scatter_dimension=0, tiled=True)[0]

    back_parts = [[(k, 0), (k, 1)] for k in range(steps - 1, 0, -1)]
    back_parts[-1].append((0, 1))
    back_parts.append([(0, 0)])
    state = None
    seg_grads = {}
    passing = None
    for i, items in enumerate(back_parts):
        done = i == len(back_parts) - 1
        outs = attend_back_part(
            queries, head_grads, lse, head_mix, start, key_lift, value_lift, key_lift_t, lo,
            [segs[k][j] for k, j in items],
            jnp.stack([bases[k][j] for k, j in items]).astype(jnp.int32),
            0 if done else -1, state, done,
        )
        for item, out in zip(items, outs):
            seg_grads[item] = out
        state = outs[len(items) :]
        if not done:
            k = items[0][0]
            total = seg_grads[(k, 0)].astype(f32) + flip(seg_grads[(k, 1)], "heads", 0).astype(f32)
            if passing is not None:
                total = total + passing.astype(f32)
            passing = lax.ppermute(total.astype(bf16), "heads", down_chain)
            if k == 1:
                crossed = flip(seg_grads[(0, 1)], "heads", 0)
    query_grads, key_part, value_part = state
    latent_grads = (
        seg_grads[(0, 0)].astype(f32) + crossed.astype(f32) + passing.astype(f32)
    ).astype(bf16)

    query_back_mine = query_grads[:rows].reshape(count, group_width)
    query_back_got = swap(query_grads[rows:]).reshape(count, group_width)
    latent_back_mine = latent_grads[:rows].reshape(count, latent_size)
    latent_back_got = swap(latent_grads[rows:]).reshape(count, latent_size)
    ff_share = gate_weight.shape[1] // peers
    full, hidden_grad = finish(
        (early_feed, early_down),
        ((ff_share, ff_share, share), (ff_share,)),
        peers,
        (
            hidden_in.reshape(count, width), attn_gain.reshape(1, width),
            query_back_mine, query_back_got, latent_back_mine, latent_back_got,
            query_weight, latent_weight, grad_resid, ffn_gain_part, key_part, value_part,
        ),
    )
    (
        gate_share, up_share, output_share, down_share, query_share, latent_share, key_share, value_share, gains,
    ) = lay_out(full, (ff_share, ff_share, share, ff_share), share, latent_size, group_width, peers, width)
    gains = lax.dynamic_slice_in_dim(gains, (place * share) % gains.shape[1], share, 1)
    return (
        hidden_out.reshape(rows, tokens, width),
        hidden_grad.reshape(rows, tokens, width),
        gains[0],
        query_share,
        latent_share,
        key_share,
        value_share,
        output_share,
        gains[1],
        gate_share,
        up_share,
        down_share,
    )


def solution(mesh):
    placed = (
        P("rows", "heads", None),
        P("rows", None),
        P("rows", "heads", None),
        P(),
        P(),
        P(),
        P(),
        P(),
        P(),
        P(),
        P(),
        P(),
        P(),
    )
    return jax.shard_map(
        shards,
        mesh=mesh,
        in_specs=placed,
        out_specs=(
            P("rows", "heads", None),
            P("rows", "heads", None),
            P("heads"),
            P("heads", None),
            P("heads", None),
            P(None, "heads", None),
            P(None, "heads", None),
            P("heads", None),
            P("heads"),
            P(None, "heads"),
            P(None, "heads"),
            P("heads", None),
        ),
        check_vma=False,
    )
```

```python
import functools
import math

import jax
import jax.numpy as jnp
from jax import lax
from jax.experimental import pallas as pl
from jax.experimental.pallas import tpu as pltpu
from jax.sharding import PartitionSpec as P

HEAD_WIDTH = 64
epsilon = 1e-05
blocked = -1e30
LOG2E = math.log2(math.e)
LN2 = math.log(2.0)
QUAD = 4
f32 = jnp.float32
bf16 = jnp.bfloat16


def matmul(left, right):
    return jnp.dot(left, right, preferred_element_type=f32)


def matmul_nt(left, right):
    return lax.dot_general(
        left, right, (((left.ndim - 1,), (right.ndim - 1,)), ((), ())), preferred_element_type=f32
    )


def matmul_tn(left, right):
    return lax.dot_general(left, right, (((0,), (0,)), ((), ())), preferred_element_type=f32)


def rms_inverse(value_matrix):
    return lax.rsqrt(jnp.mean(value_matrix * value_matrix, axis=-1, keepdims=True) + epsilon)


def expand_heads(source, weights, factor, out_ref):
    tokens = source.shape[0]
    quads, wide, deep = weights.shape
    latent = wide // QUAD
    for quad in range(quads):
        product = matmul_nt(weights[quad], source[:, quad * deep : (quad + 1) * deep])
        if factor != 1.0:
            product = product * factor
        product = product.astype(bf16)
        for h in range(QUAD):
            at = (quad * QUAD + h) * tokens
            out_ref[:, at : at + tokens] = product[h * latent : (h + 1) * latent]


def lift_heads(source, weights, tokens):
    parts = [
        matmul(weights[h], source[:, h * tokens : (h + 1) * tokens]) for h in range(weights.shape[0])
    ]
    return jnp.concatenate(parts, axis=0)


def lift_grad(left, right, tokens, out_ref):
    latent = left.shape[0]
    deep = QUAD * HEAD_WIDTH
    head = lax.broadcasted_iota(jnp.int32, (latent, deep), 1) // HEAD_WIDTH
    for quad in range(right.shape[1] // deep):
        columns = slice(quad * deep, (quad + 1) * deep)
        found = None
        for h in range(QUAD):
            at = (quad * QUAD + h) * tokens
            part = matmul(left[:, at : at + tokens], right[:, columns])
            found = part if h == 0 else jnp.where(head == h, part, found)
        out_ref[:, columns] += found


def seg_mask(base, own_base, start):
    tokens = start.shape[-1]
    key_at = lax.broadcasted_iota(jnp.int32, (tokens, tokens), 0)
    query_at = lax.broadcasted_iota(jnp.int32, (tokens, tokens), 1)
    return (key_at >= start - base) & (key_at <= query_at + (own_base - base))


def attend_kernel(count, first, last, lo, bases, *refs):
    refs = list(refs)
    take = lambda k: [refs.pop(0) for _ in range(k)]
    query_ref, start_ref, key_lift_ref = take(3)
    seg_refs = take(count)
    if not first:
        top_in, total_in, mix_in = take(3)
    if last:
        (value_lift_ref,) = take(1)
        out_ref, lse_ref, mix_ref = take(3)
    else:
        top_out, total_out, mix_out = take(3)
    expanded, top, total, mix, segs = take(5)
    tokens = query_ref.shape[1]
    heads = expanded.shape[1] // tokens
    row = pl.program_id(0)
    scale = HEAD_WIDTH ** (-0.5) * LOG2E
    touched = lambda i: (bases[i] >= 0) & (bases[i] + tokens - 1 >= lo[row])
    if first:
        expand_heads(query_ref[0], key_lift_ref, scale, expanded)
        top[...] = jnp.full_like(top, blocked)
        total[...] = jnp.zeros_like(total)
        mix[...] = jnp.zeros_like(mix)
    else:
        top[...] = top_in[0]
        total[...] = total_in[0]
        mix[...] = mix_in[0].astype(f32)

        @pl.when(functools.reduce(jnp.logical_or, [touched(i) for i in range(count)]))
        def _():
            expand_heads(query_ref[0], key_lift_ref, scale, expanded)

    for i in range(count):
        segs[i] = seg_refs[i][0]

    @pl.loop(0, count)
    def _(i):
        @pl.when(touched(i))
        def _():
            latent = segs[i]
            latent_t = latent.T
            allow = seg_mask(bases[i], bases[count], start_ref[0])
            for h in range(heads):
                at = slice(h * tokens, (h + 1) * tokens)
                score = jnp.where(allow, matmul(latent, expanded[:, at]), blocked)
                old = top[:, at]
                new = jnp.maximum(old, jnp.max(score, axis=0, keepdims=True))
                probs = jnp.exp2(score - new)
                fade = jnp.exp2(old - new)
                top[:, at] = new
                total[:, at] = total[:, at] * fade + jnp.sum(probs, axis=0, keepdims=True)
                mix[:, at] = mix[:, at] * fade + matmul(latent_t, probs.astype(bf16))

    if not last:
        top_out[0] = top[...]
        total_out[0] = total[...]
        mix_out[0] = mix[...].astype(bf16)
        return
    lse_ref[0] = top[...] + jnp.log2(total[...])
    mix_ref[0] = (mix[...] * (1.0 / total[...])).astype(bf16)
    out_ref[0] = lift_heads(mix_ref[0], value_lift_ref, tokens).T.astype(bf16)


def whole(array):
    return pl.BlockSpec(array.shape, lambda *_: (0,) * len(array.shape))


def by_row(shape, begin=0):
    return pl.BlockSpec((1,) + tuple(shape[1:]), lambda r, *_: (r + begin,) + (0,) * (len(shape) - 1))


def attend_part(queries, start, key_lift, value_lift_t, lo, segs, bases, state, last):
    rows, tokens, width = queries.shape
    heads = width // HEAD_WIDTH
    latent = segs[0].shape[-1]
    shape = jax.ShapeDtypeStruct
    stat = shape((rows, 1, heads * tokens), f32)
    state_shapes = [stat, stat, shape((rows, latent, heads * tokens), bf16)]
    args = [queries, start, key_lift, *segs]
    specs = [by_row(queries.shape), by_row(start.shape), whole(key_lift)]
    specs += [by_row(s.shape) for s in segs]
    if state is not None:
        args += list(state)
        specs += [by_row(s.shape) for s in state_shapes]
    if last:
        args.append(value_lift_t)
        specs.append(whole(value_lift_t))
        outs = [shape(queries.shape, bf16), stat, state_shapes[2]]
    else:
        outs = state_shapes
    blocks = rows * heads * len(segs)
    return pl.pallas_call(
        functools.partial(attend_kernel, len(segs), state is None, last),
        out_shape=outs,
        grid_spec=pltpu.PrefetchScalarGridSpec(
            num_scalar_prefetch=2,
            grid=(rows,),
            in_specs=specs,
            out_specs=[by_row(o.shape) for o in outs],
            scratch_shapes=[
                pltpu.VMEM((latent, heads * tokens), bf16),
                pltpu.VMEM((1, heads * tokens), f32),
                pltpu.VMEM((1, heads * tokens), f32),
                pltpu.VMEM((latent, heads * tokens), f32),
                pltpu.VMEM((len(segs), tokens, latent), bf16),
            ],
        ),
        compiler_params=pltpu.CompilerParams(
            dimension_semantics=("arbitrary",), vmem_limit_bytes=48 << 20
        ),
        cost_estimate=pl.CostEstimate(
            flops=blocks * tokens * tokens * latent * 4,
            bytes_accessed=rows * heads * latent * tokens * 4,
            transcendentals=0,
        ),
        name="attend",
    )(lo, bases, *args)


def attend_back_kernel(count, begin, first, last, lo, bases, *refs):
    refs = list(refs)
    take = lambda k: [refs.pop(0) for _ in range(k)]
    query_ref, grad_ref, lse_ref, mix_ref, start_ref, key_lift_ref, value_lift_ref, key_lift_t_ref = take(8)
    seg_refs = take(count)
    if not first:
        query_back_in, key_up_in = take(2)
        if last:
            (value_up_in,) = take(1)
    grad_refs = take(count)
    query_back_ref, key_up_ref = take(2)
    if last:
        (value_up_ref,) = take(1)
    expanded, expanded_grad, delta, back, query_back, segs, seg_grads = take(7)
    latent_size = expanded.shape[0]
    tokens = query_ref.shape[1]
    heads = expanded.shape[1] // tokens
    row = pl.program_id(0)
    scale = HEAD_WIDTH ** (-0.5)
    touched = lambda i: (bases[i] >= 0) & (bases[i] + tokens - 1 >= lo[row + begin])
    any_touched = functools.reduce(jnp.logical_or, [touched(i) for i in range(count)])

    @pl.when(row == 0)
    def _():
        key_up_ref[...] = jnp.zeros_like(key_up_ref) if first else key_up_in[...]
        if last:
            value_up_ref[...] = value_up_in[...]

    query_back[...] = jnp.zeros_like(query_back) if first else query_back_in[0]
    seg_grads[...] = jnp.zeros_like(seg_grads)

    @pl.when(any_touched)
    def _():
        expand_heads(query_ref[0], key_lift_ref, scale * LOG2E, expanded)
        expand_heads(grad_ref[0], value_lift_ref, 1.0, expanded_grad)
        delta[...] = jnp.sum(mix_ref[0].astype(f32) * expanded_grad[...].astype(f32), axis=0, keepdims=True)
        back[...] = jnp.zeros_like(back)
        for i in range(count):
            segs[i] = seg_refs[i][0]

    @pl.loop(0, count)
    def _(i):
        @pl.when(touched(i))
        def _():
            latent = segs[i]
            allow = seg_mask(bases[i], bases[count], start_ref[0])
            allow = jnp.concatenate([allow] * heads, axis=1)
            score = matmul(latent, expanded[...])
            probs = jnp.where(allow, jnp.exp2(score - lse_ref[0]), 0.0)
            dprobs = matmul(latent, expanded_grad[...])
            dscore = (probs * (dprobs - delta[...])).astype(bf16)
            by_key = matmul_nt(dscore, expanded[...])
            by_value = matmul_nt(probs.astype(bf16), expanded_grad[...])
            seg_grads[i] = (by_key * LN2 + by_value).astype(bf16)
            back[...] += matmul(latent.T, dscore)

    for i in range(count):
        grad_refs[i][0] = seg_grads[i]

    @pl.when(any_touched)
    def _():
        part = (back[...] * scale).astype(bf16)
        query_back[...] += lift_heads(part, key_lift_t_ref, tokens)
        lift_grad(part, query_ref[0], tokens, key_up_ref)

    if last:
        lift_grad(mix_ref[0], grad_ref[0], tokens, value_up_ref)
        query_back_ref[0] = query_back[...].T.astype(bf16)
    else:
        query_back_ref[0] = query_back[...]


def attend_back_part(
    queries, grads, lse, mix, start, key_lift, value_lift, key_lift_t, lo, segs, bases, state, last, begin, rows,
):
    _, tokens, width = queries.shape
    heads = width // HEAD_WIDTH
    latent = segs[0].shape[-1]
    shape = jax.ShapeDtypeStruct
    back_shape = shape((rows, width, tokens), f32)
    up_shape = shape((latent, width), f32)
    args = [queries, grads, lse, mix, start, key_lift, value_lift, key_lift_t, *segs]
    specs = [by_row(a.shape, begin) for a in (queries, grads, lse, mix, start)]
    specs += [whole(key_lift), whole(value_lift), whole(key_lift_t)]
    specs += [by_row(s.shape, begin) for s in segs]
    if state is not None:
        args += list(state)
        specs.append(by_row(state[0].shape, begin))
        specs += [whole(up_shape)] * (len(state) - 1)
    outs = [shape((rows, tokens, latent), bf16) for _ in segs]
    outs += [shape((rows, tokens, width), bf16) if last else back_shape, up_shape]
    out_specs = [by_row(o.shape) for o in outs[:-1]] + [whole(up_shape)]
    if last:
        outs.append(up_shape)
        out_specs.append(whole(up_shape))
    blocks = rows * heads * len(segs)
    return pl.pallas_call(
        functools.partial(attend_back_kernel, len(segs), begin, state is None, last),
        out_shape=outs,
        grid_spec=pltpu.PrefetchScalarGridSpec(
            num_scalar_prefetch=2,
            grid=(rows,),
            in_specs=specs,
            out_specs=out_specs,
            scratch_shapes=[
                pltpu.VMEM((latent, heads * tokens), bf16),
                pltpu.VMEM((latent, heads * tokens), bf16),
                pltpu.VMEM((1, heads * tokens), f32),
                pltpu.VMEM((latent, heads * tokens), f32),
                pltpu.VMEM((width, tokens), f32),
                pltpu.VMEM((len(segs), tokens, latent), bf16),
                pltpu.VMEM((len(segs), tokens, latent), bf16),
            ],
        ),
        compiler_params=pltpu.CompilerParams(
            dimension_semantics=("arbitrary",), vmem_limit_bytes=48 << 20
        ),
        cost_estimate=pl.CostEstimate(
            flops=blocks * tokens * tokens * latent,
            bytes_accessed=rows * heads * latent * tokens,
            transcendentals=0,
        ),
        name="attend_back",
    )(lo, bases, *args)


def quad_lift(lift):
    latent, width = lift.shape
    deep = QUAD * HEAD_WIDTH
    quads = width // deep
    tall = jnp.tile(lift.reshape(latent, quads, deep).transpose(1, 0, 2), (1, QUAD, 1))
    row_head = lax.broadcasted_iota(jnp.int32, tall.shape, 1) // latent
    column_head = lax.broadcasted_iota(jnp.int32, tall.shape, 2) // HEAD_WIDTH
    return jnp.where(row_head == column_head, tall, jnp.zeros_like(tall))


def head_lift(lift):
    latent, width = lift.shape
    return lift.T.reshape(width // HEAD_WIDTH, HEAD_WIDTH, latent)


def put_pieces(ref, value, at=0):
    pieces, _, piece = ref.shape
    for j in range(pieces):
        ref[j, pl.ds(at, value.shape[0])] = value[:, j * piece : (j + 1) * piece].astype(bf16)


def feed_kernel(core_ref, *refs):
    (
        inputs_ref, mine_ref, got_ref, output_ref, gain_ref, cotangent_ref, keep_ref,
        gate_ref, up_ref, down_ref,
        hidden_out_ref, resid, normed, back, active_ref, slope_ref, down_grad_ref,
        result, hidden,
    ) = refs
    step = pl.program_id(0)
    count = inputs_ref.shape[0]
    block = min(256, count)
    core = core_ref[0]

    @pl.when(step == 0)
    def _():
        for t in range(0, count, block):
            at = slice(t, t + block)
            row = inputs_ref[at].astype(f32) + (
                matmul(mine_ref[at], output_ref[core]) + matmul(got_ref[at], output_ref[1 - core])
            )
            resid[at] = row
            scale = lax.rsqrt(jnp.mean(row * row, axis=-1, keepdims=True) + epsilon)
            normed[at] = (row * scale * gain_ref[...]).astype(bf16)
            back[at] = (cotangent_ref[at].astype(f32) * keep_ref[at]).astype(bf16)
        result[...] = jnp.zeros_like(result)

    part = count // 4
    for t in range(0, count, part):
        at = slice(t, t + part)
        gate = matmul(normed[at], gate_ref[...])
        up = matmul(normed[at], up_ref[...])
        sigmoid = 1.0 / (1.0 + jnp.exp(-gate))
        active = gate * sigmoid
        hidden[at] = (active * up).astype(bf16)
        active_ref[at] = active.astype(bf16)
        slope_ref[at] = (up * (sigmoid * (1.0 + gate * (1.0 - sigmoid)))).astype(bf16)
    put_pieces(down_grad_ref, matmul_tn(hidden[...], back[...]))
    result[...] += matmul(hidden[...], down_ref[...])

    @pl.when(step == pl.num_programs(0) - 1)
    def _():
        hidden_out_ref[...] = (resid[...] + result[...]).astype(bf16)


def feed_back_kernel(core_ref, *refs):
    (
        mine_ref, got_ref, output_ref, gain_ref, resid_ref, normed, back,
        active_ref, slope_ref, gate_ref, up_ref, down_ref,
        grad_resid_ref, head_mine_ref, head_sent_ref, gain_grad_ref, grads_ref,
        grad_two, both, low, staged, staged_out, sems, out_sem,
    ) = refs
    step = pl.program_id(0)
    steps = pl.num_programs(0)
    count, width = resid_ref.shape
    chunk = down_ref.shape[0]
    ff = (grads_ref.shape[1] - width) // 2
    block = min(256, count)
    core = core_ref[0]
    slot = step % 2

    def leave(at, kind, place):
        return pltpu.make_async_copy(
            staged.at[at, kind],
            grads_ref.at[:, pl.ds(pl.multiple_of(kind * ff + place * chunk, chunk), chunk)],
            sems.at[at, kind],
        )

    @pl.when(step >= 2)
    def _():
        for kind in range(2):
            leave(slot, kind, step - 2).wait()

    @pl.when(step == 0)
    def _():
        grad_two[...] = jnp.zeros_like(grad_two)

    part = count // 4
    for t in range(0, count, part):
        at = slice(t, t + part)
        grad_act = matmul_nt(back[at], down_ref[...])
        both[at, :chunk] = (grad_act * slope_ref[at].astype(f32)).astype(bf16)
        both[at, chunk:] = (grad_act * active_ref[at].astype(f32)).astype(bf16)
    for kind in range(2):
        put_pieces(staged.at[slot, kind], matmul_tn(both[:, kind * chunk : (kind + 1) * chunk], normed[...]))
        leave(slot, kind, step).start()
    weights = jnp.concatenate([gate_ref[...], up_ref[...]], axis=1)
    for t in range(0, count, part):
        at = slice(t, t + part)
        grad_two[at] += matmul_nt(both[at], weights)

    @pl.when(step == steps - 1)
    def _():
        gain_total = jnp.zeros((1, width), f32)
        for t in range(0, count, block):
            at = slice(t, t + block)
            row = resid_ref[at]
            scale = lax.rsqrt(jnp.mean(row * row, axis=-1, keepdims=True) + epsilon)
            unit = row * scale
            grad = grad_two[at]
            gain_total += jnp.sum(grad * unit, axis=0, keepdims=True)
            scaled = grad * gain_ref[...]
            grad = back[at].astype(f32) + scale * (
                scaled - unit * jnp.mean(scaled * unit, axis=-1, keepdims=True)
            )
            grad_resid_ref[at] = grad
            low[at] = grad.astype(bf16)
            head_mine_ref[at] = matmul_nt(low[at], output_ref[core]).astype(bf16)
            head_sent_ref[at] = matmul_nt(low[at], output_ref[1 - core]).astype(bf16)
        gain_grad_ref[...] = gain_total
        half = mine_ref.shape[1]
        put_pieces(staged_out, matmul_tn(mine_ref[...], low[...]), core * half)
        put_pieces(staged_out, matmul_tn(got_ref[...], low[...]), (1 - core) * half)
        last = pltpu.make_async_copy(staged_out, grads_ref.at[:, pl.ds(2 * ff, width)], out_sem)
        last.start()
        for kind in range(2):
            leave(1 - slot, kind, step - 1).wait()
            leave(slot, kind, step).wait()
        last.wait()


def once(array):
    return pl.BlockSpec(array.shape, lambda *_: (0,) * len(array.shape), pipeline_mode=pl.Buffered(1))


def feed(core, inputs, mixed_mine, mixed_got, output_weight, gain, cotangent, keep, weights, pieces):
    count, width = inputs.shape
    gate_weight, up_weight, down_weight = weights
    ff = gate_weight.shape[1]
    chunk = 256
    piece = width // pieces
    output_weight = output_weight.reshape(2, -1, width)
    gain = gain.reshape(1, width)
    by_rows = pl.BlockSpec((chunk, width), lambda c, *_: (c, 0))
    by_columns = pl.BlockSpec((width, chunk), lambda c, *_: (0, c))
    kept_columns = pl.BlockSpec((count, chunk), lambda c, *_: (0, c))
    shape = jax.ShapeDtypeStruct
    params = pltpu.CompilerParams(dimension_semantics=("arbitrary",), vmem_limit_bytes=60 << 20)
    full_bf, full_f = shape((count, width), bf16), shape((count, width), f32)
    kept = shape((count, ff), bf16)
    firsts = [inputs, mixed_mine, mixed_got, output_weight, gain, cotangent, keep]
    outs = [full_bf, full_f, full_bf, full_bf, kept, kept, shape((pieces, ff, piece), bf16)]
    hidden_out, resid, normed, back, active, slope, down_grad = pl.pallas_call(
        feed_kernel,
        out_shape=outs,
        grid_spec=pltpu.PrefetchScalarGridSpec(
            num_scalar_prefetch=1,
            grid=(ff // chunk,),
            in_specs=[once(a) for a in firsts] + [by_columns, by_columns, by_rows],
            out_specs=[once(o) for o in outs[:4]]
            + [kept_columns, kept_columns, pl.BlockSpec((pieces, chunk, piece), lambda c, *_: (0, c, 0))],
            scratch_shapes=[pltpu.VMEM((count, width), f32), pltpu.VMEM((count, chunk), bf16)],
        ),
        compiler_params=params,
        cost_estimate=pl.CostEstimate(
            flops=count * width * (ff * 8 + width * 2),
            bytes_accessed=width * ff * 8 + count * width * 16 + count * ff * 4,
            transcendentals=count * ff,
        ),
        name="feed",
    )(core.reshape(1), *firsts, *weights)
    firsts = [mixed_mine, mixed_got, output_weight, gain, resid, normed, back]
    outs = [
        full_f,
        shape(mixed_mine.shape, bf16),
        shape(mixed_mine.shape, bf16),
        shape((1, width), f32),
        shape((pieces, 2 * ff + width, piece), bf16),
    ]
    grad_resid, head_mine, head_sent, gain_grad, grads = pl.pallas_call(
        feed_back_kernel,
        out_shape=outs,
        grid_spec=pltpu.PrefetchScalarGridSpec(
            num_scalar_prefetch=1,
            grid=(ff // chunk,),
            in_specs=[once(a) for a in firsts]
            + [kept_columns, kept_columns, by_columns, by_columns, by_rows],
            out_specs=[once(o) for o in outs[:4]] + [pl.BlockSpec(memory_space=pl.ANY)],
            scratch_shapes=[
                pltpu.VMEM((count, width), f32),
                pltpu.VMEM((count, 2 * chunk), bf16),
                pltpu.VMEM((count, width), bf16),
                pltpu.VMEM((2, 2, pieces, chunk, piece), bf16),
                pltpu.VMEM((pieces, width, piece), bf16),
                pltpu.SemaphoreType.DMA((2, 2)),
                pltpu.SemaphoreType.DMA,
            ],
        ),
        compiler_params=params,
        cost_estimate=pl.CostEstimate(
            flops=count * width * (ff * 10 + width * 4),
            bytes_accessed=width * ff * 10 + count * width * 20 + count * ff * 4,
            transcendentals=0,
        ),
        name="feed_back",
    )(core.reshape(1), *firsts, active, slope, *weights)
    return hidden_out, grad_resid, head_mine, head_sent, gain_grad, down_grad, grads


def flip(array, axis, bit):
    size = lax.axis_size(axis)
    return lax.ppermute(array, axis, [(i, i ^ (1 << bit)) for i in range(size)])


def late_parts(core, inputs_ref, gain_ref, back_refs, before, query_ref, latent_ref, resid_ref, other_gain_ref, up_refs, normed, own, sent, grad_ref):
    along, count, _, piece = own.shape
    tokens, width = inputs_ref.shape
    query_mine, query_got, latent_mine, latent_got = back_refs
    share = width // count
    fold = share // 2
    latent = latent_mine.shape[1]
    half = query_mine.shape[1]
    block = min(256, tokens)
    mine = lambda ref, size: ref[:, pl.ds(pl.multiple_of(core * size, size), size)]
    theirs = lambda ref, size: ref[:, pl.ds(pl.multiple_of((1 - core) * size, size), size)]
    for t in range(0, tokens, block):
        at = slice(t, t + block)
        row = inputs_ref[at].astype(f32)
        scale = lax.rsqrt(jnp.mean(row * row, axis=-1, keepdims=True) + epsilon)
        normed[at] = (row * scale * gain_ref[...]).astype(bf16)
    before()
    gain_total = jnp.zeros((1, width), f32)
    for t in range(0, tokens, block):
        at = slice(t, t + block)
        row = inputs_ref[at].astype(f32)
        scale = lax.rsqrt(jnp.mean(row * row, axis=-1, keepdims=True) + epsilon)
        unit = row * scale
        grad = (
            matmul_nt(query_mine[at], mine(query_ref, half))
            + matmul_nt(query_got[at], theirs(query_ref, half))
            + matmul_nt(latent_mine[at], mine(latent_ref, latent))
            + matmul_nt(latent_got[at], theirs(latent_ref, latent))
        )
        gain_total += jnp.sum(grad * unit, axis=0, keepdims=True)
        scaled = grad * gain_ref[...]
        grad_ref[at] = resid_ref[at] + scale * (
            scaled - unit * jnp.mean(scaled * unit, axis=-1, keepdims=True)
        )
    other = other_gain_ref[...]
    gains = (jnp.where(core == 0, gain_total, other), jnp.where(core == 0, other, gain_total))
    lane = max(share, 128)
    for target, query, latents, gain in (
        (own, query_mine, latent_mine, gains[0]),
        (sent, query_got, latent_got, gains[1]),
    ):
        query_grad = matmul_tn(normed[...], query[...]).astype(bf16)
        latent_grad = matmul_tn(normed[...], latents[...]).astype(bf16)
        for s in range(count):
            first = s * share
            begin = first // lane * lane
            for j in range(along):
                target[j, s, :share] = query_grad[first : first + share, j * piece : (j + 1) * piece]
                side, column = divmod(j * piece, latent)
                target[j, s, share : share + fold] = latent_grad[
                    first + side * fold : first + (side + 1) * fold, column : column + piece
                ]
                rows = slice(share + fold, share + fold + 16)
                if j == 0:
                    kept = jnp.broadcast_to(gain[:, begin : begin + lane], (16, lane)).astype(bf16)
                    target[j, s, rows, :lane] = kept
                    if piece > lane:
                        target[j, s, rows, lane:] = jnp.zeros((16, piece - lane), bf16)
                else:
                    target[j, s, rows] = jnp.zeros((16, piece), bf16)
    lift = latent // count
    at = share + fold + 16
    for ref in up_refs:
        for s in range(count):
            for j in range(along):
                own[j, s, at : at + lift] = ref[s * lift : (s + 1) * lift, j * piece : (j + 1) * piece].astype(bf16)
        at += lift


def finish_kernel(
    sections, early_refs, late_compute, chain_refs, own_ref, sent_ref, out_ref, late_got, late_from, got_first, got_next,
    chain_sems, core_sems, along_sems, first_sems, first_late_sems, next_sems, out_sems,
):
    along, count, late_rows, piece = own_ref.shape
    shared_rows = sent_ref.shape[2]
    early_rows = sum(section[2] for section in sections)
    bits = count.bit_length() - 1
    row_at = lax.axis_index("rows")
    place = lax.axis_index("heads")
    core = row_at % 2
    x_at = row_at // 2
    mesh = pl.DeviceIdType.MESH
    early_part = slice(0, early_rows)
    late_part = slice(early_rows, early_rows + late_rows)

    def turned(which):
        at = place
        for bit in which:
            at = at + (1 << bit) * (1 - 2 * ((place // (1 << bit)) % 2))
        return at

    core_peer = (row_at + 1 - 2 * core, place)
    x_others = [(x_at + d) % along for d in range(1, along)]
    x_peers = [(x * 2 + core, place) for x in x_others]
    head_peers = [(row_at, turned([bit])) for bit in range(bits)]
    barrier = pltpu.get_barrier_semaphore()
    above = (row_at, (place + 2) % count)
    below = (row_at, (place + count - 2) % count)
    everyone = [core_peer, above, below] + x_peers + head_peers
    for peer in everyone:
        pl.semaphore_signal(barrier, inc=1, device_id=peer, device_id_type=mesh)
    pl.semaphore_wait(barrier, len(everyone))

    def remote(source, target, sems, index, peer):
        return pltpu.make_async_remote_copy(
            src_ref=source, dst_ref=target, send_sem=sems.at[(0,) + index], recv_sem=sems.at[(1,) + index],
            device_id=peer, device_id_type=mesh,
        )

    def orders(bit):
        rest = list(range(bit + 1, bits))
        return [
            [b for i, b in enumerate(rest) if not (mask >> (len(rest) - 1 - i)) & 1]
            for mask in range(1 << len(rest))
        ]

    def add_rows(target, other, size):
        block = size if size <= 600 else size // 2

        def one(i, carry):
            at = pl.ds(pl.multiple_of(i * block, 16), block)
            target[at] = (target[at].astype(f32) + other[at].astype(f32)).astype(bf16)
            return carry

        lax.fori_loop(0, size // block, one, 0)

    first = orders(0)
    pending = []

    def early_rows_of(n, shard):
        which, start, share, _ = sections[n]
        return early_refs[which].at[pl.ds(pl.multiple_of(start + shard * share, 16), share)]

    def first_early(i, n):
        _, _, share, row = sections[n]
        return remote(
            early_rows_of(n, turned([0] + first[i])), got_first.at[i, pl.ds(row, share)],
            first_sems, (i, n), head_peers[0],
        )

    query_grad_ref, latent_grad_ref, joined_ref, chain_got, query_got, latent_low, latent_got = chain_refs
    chain_copy = remote(joined_ref, chain_got, chain_sems, (0,), below)
    chain_copy.start()
    query_copy = remote(query_grad_ref.at[1], query_got, chain_sems, (1,), core_peer)
    query_copy.start()
    latent_copy = remote(latent_low.at[1], latent_got, chain_sems, (2,), core_peer)
    for i in range(len(first)):
        for n in range(len(sections)):
            first_early(i, n).start()

    def settle_latents():
        chain_copy.wait()
        for side in (1, 0):
            size = latent_low.shape[1] // 2
            for t in range(2):
                at = slice(t * size, (t + 1) * size)
                latent_low[side, at] = (latent_grad_ref[side, at] + chain_got[side, at].astype(f32)).astype(bf16)
            if side == 1:
                latent_copy.start()
        query_copy.wait()
        latent_copy.wait()

    def next_copy(bit, j, i, part, which):
        rows = pl.ds(part.start, part.stop - part.start)
        return remote(
            got_first.at[i, rows], got_next[bit - 1].at[j, rows], next_sems[bit - 1], (j, which), head_peers[bit]
        )

    def settle(i, part, which):
        rest = first[i]
        level = rest[0] if rest else bits
        size = part.stop - part.start
        rows = pl.ds(part.start, size)
        for bit in range(1, level):
            j = orders(bit).index(rest)
            next_copy(bit, j, i, part, which).wait_recv()
            add_rows(got_first.at[i, rows], got_next[bit - 1].at[j, rows], size)
        if rest:
            copy = next_copy(level, orders(level).index(rest[1:]), i, part, which)
            copy.start()
            pending.append(copy)

    def early_step(i):
        for n, (_, _, share, row) in enumerate(sections):
            first_early(i, n).wait()
            add_rows(got_first.at[i, pl.ds(row, share)], early_rows_of(n, turned(first[i])), share)
        settle(i, early_part, 0)

    def first_late(i):
        return remote(
            late_from.at[0, turned([0] + first[i])],
            got_first.at[i, pl.ds(early_rows, late_rows)],
            first_late_sems, (i,), head_peers[0],
        )

    def late_begin():
        for copy in x_copies:
            copy.wait()

        def x_add(s, carry):
            shared = late_got[x_at, s].astype(f32)
            alone = own_ref[x_at, s, shared_rows:].astype(f32)
            for d in range(along - 1):
                shared = shared + late_from[d, s, :shared_rows].astype(f32)
                alone = alone + late_from[d, s, shared_rows:].astype(f32)
            late_from[0, s, :shared_rows] = shared.astype(bf16)
            late_from[0, s, shared_rows:] = alone.astype(bf16)
            return carry

        lax.fori_loop(0, count, x_add, 0)
        for i in range(len(first)):
            first_late(i).start()

    def late_step(i):
        first_late(i).wait()
        add_rows(got_first.at[i, pl.ds(early_rows, late_rows)], late_from.at[0, turned(first[i])], late_rows)
        settle(i, late_part, 1)

    final = len(first) - 1
    half = max(1, len(first) // 2)
    for i in range(half):
        early_step(i)
    late_compute(core, settle_latents)
    core_copy = remote(sent_ref, late_got, core_sems, (0,), core_peer)
    core_copy.start()
    core_copy.wait()

    def core_add(i, carry):
        j, s = i // count, i % count
        late_got[j, s] = (own_ref[j, s, :shared_rows].astype(f32) + late_got[j, s].astype(f32)).astype(bf16)
        return carry

    lax.fori_loop(0, along * count, core_add, 0)
    x_copies = []
    for d, (x, peer) in enumerate(zip(x_others, x_peers)):
        x_copies.append(
            remote(late_got.at[x], late_from.at[d, :, pl.ds(0, shared_rows)], along_sems, (d, 0), peer)
        )
        x_copies.append(
            remote(
                own_ref.at[x, :, pl.ds(shared_rows, late_rows - shared_rows)],
                late_from.at[d, :, pl.ds(shared_rows, late_rows - shared_rows)],
                along_sems, (d, 1), peer,
            )
        )
    for copy in x_copies:
        copy.start()

    early_step(half)
    late_begin()
    for i in range(half + 1, final):
        early_step(i)
    for i in range(final):
        late_step(i)

    def spread(part, which):
        rows = pl.ds(part.start, part.stop - part.start)
        out_ref[row_at, rows] = got_first[final, rows]
        copies = [remote(out_ref.at[row_at, rows], out_ref.at[row_at, rows], out_sems, (which, 0), core_peer)]
        for d, peer in enumerate(x_peers):
            copies.append(
                remote(out_ref.at[row_at, rows], out_ref.at[row_at, rows], out_sems, (which, 1 + d), peer)
            )
        for copy in copies:
            copy.start()
        return copies

    def pass_on(part, which, copies):
        rows = pl.ds(part.start, part.stop - part.start)
        more = []
        for d in range(along - 1):
            copies[1 + d].wait_recv()
            source = ((x_at + along - 1 - d) % along) * 2 + core
            more.append(
                remote(
                    out_ref.at[source, rows], out_ref.at[source, rows], out_sems, (which, along + d), core_peer
                )
            )
            more[-1].start()
        return more

    early_step(final)
    early_out = spread(early_part, 0)
    late_step(final)
    late_out = spread(late_part, 1)
    early_more = pass_on(early_part, 0, early_out)
    late_more = pass_on(late_part, 1, late_out)
    for copies, more in ((early_out, early_more), (late_out, late_more)):
        copies[0].wait()
        for copy in copies[1:]:
            copy.wait_send()
        for copy in more:
            copy.wait()
    for copy in pending:
        copy.wait_send()


def finish(early, shares, count, late_args):
    inputs = late_args[0]
    tokens, width = inputs.shape
    piece = early[0].shape[1]
    along = width // piece // 2
    share = width // count
    bits = count.bit_length() - 1
    shared_rows = share + share // 2 + 16
    late_rows = shared_rows + 2 * (late_args[3].shape[2] // count)
    sections = []
    row = 0
    for which, of_one in enumerate(shares):
        start = 0
        for size in of_one:
            sections.append((which, start, size, row))
            start += size * count
            row += size
    total = row + late_rows
    vmem = pl.BlockSpec(memory_space=pltpu.VMEM)
    dma = pltpu.SemaphoreType.DMA

    def body(*refs):
        refs = list(refs)
        take = lambda k: [refs.pop(0) for _ in range(k)]
        early_refs = take(len(early))
        late_refs = take(len(late_args))
        out_ref, grad_ref = take(2)
        normed, own_ref, sent_ref, late_got, late_from, got_first = take(6)
        got_next = take(bits - 1)
        chain_got, query_got, latent_low, latent_got, chain_sems = take(5)
        core_sems, along_sems, first_sems, first_late_sems = take(4)
        next_sems = take(bits - 1)
        (out_sems,) = take(1)
        (
            inputs_ref, gain_ref, query_grad_ref, latent_grad_ref, joined_ref,
            query_ref, latent_ref, resid_ref, other_gain_ref, key_up, value_up,
        ) = late_refs

        def late_compute(core, before):
            late_parts(
                core, inputs_ref, gain_ref, (query_grad_ref.at[0], query_got, latent_low.at[0], latent_got), before,
                query_ref, latent_ref, resid_ref, other_gain_ref, (key_up, value_up),
                normed, own_ref, sent_ref, grad_ref,
            )

        finish_kernel(
            sections, early_refs, late_compute,
            (query_grad_ref, latent_grad_ref, joined_ref, chain_got, query_got, latent_low, latent_got),
            own_ref, sent_ref, out_ref, late_got, late_from,
            got_first, got_next, chain_sems, core_sems, along_sems, first_sems, first_late_sems, next_sems, out_sems,
        )

    return pl.pallas_call(
        body,
        out_shape=[
            jax.ShapeDtypeStruct((2 * along, total, piece), bf16),
            jax.ShapeDtypeStruct((tokens, width), f32),
        ],
        in_specs=[vmem] * (len(early) + len(late_args)),
        out_specs=[vmem] * 2,
        scratch_shapes=[
            pltpu.VMEM((tokens, width), bf16),
            pltpu.VMEM((along, count, late_rows, piece), bf16),
            pltpu.VMEM((along, count, shared_rows, piece), bf16),
            pltpu.VMEM((along, count, shared_rows, piece), bf16),
            pltpu.VMEM((along - 1, count, late_rows, piece), bf16),
            pltpu.VMEM((count // 2, total, piece), bf16),
        ]
        + [pltpu.VMEM((count >> (bit + 1), total, piece), bf16) for bit in range(1, bits)]
        + [
            pltpu.VMEM(late_args[4].shape, bf16),
            pltpu.VMEM(late_args[2].shape[1:], bf16),
            pltpu.VMEM(late_args[4].shape, bf16),
            pltpu.VMEM(late_args[4].shape[1:], bf16),
            dma((2, 3)),
            dma((2, 1)),
            dma((2, along - 1, 2)),
            dma((2, count // 2, len(sections))),
            dma((2, count // 2)),
        ]
        + [dma((2, count >> (bit + 1), 2)) for bit in range(1, bits)]
        + [dma((2, 2, 2 * along))],
        compiler_params=pltpu.CompilerParams(
            collective_id=0, has_side_effects=True, vmem_limit_bytes=60 << 20
        ),
        name="finish",
    )(*early, *late_args)


def lay_out_kernel(rows, latent, full_ref, gate_ref, up_ref, output_ref, down_ref, query_ref, latent_ref, key_ref, value_ref, gains_ref):
    pieces, _, piece = full_ref.shape
    at = 0
    for ref, size, turn in zip((gate_ref, up_ref, output_ref, down_ref), rows, (True, True, False, False)):
        for j in range(pieces):
            value = full_ref[j, at : at + size].astype(f32)
            if turn:
                ref[j * piece : (j + 1) * piece] = value.T
            else:
                ref[:, j * piece : (j + 1) * piece] = value
        at += size
    share = query_ref.shape[0]
    fold = share // 2
    lift = key_ref.shape[1]
    half = key_ref.shape[2]
    lane = gains_ref.shape[1]
    for j in range(pieces):
        x, core = divmod(j, 2)
        row = at
        query_ref[:, core * half + x * piece : core * half + (x + 1) * piece] = full_ref[
            j, row : row + share
        ].astype(f32)
        row += share
        side, column = divmod(x * piece, latent)
        column += core * latent
        latent_ref[side * fold : (side + 1) * fold, column : column + piece] = full_ref[
            j, row : row + fold
        ].astype(f32)
        row += fold
        if x == 0:
            gains_ref[core : core + 1] = full_ref[j, row : row + 16, :lane].astype(f32)[:1]
        row += 16
        for ref in (key_ref, value_ref):
            ref[core, :, x * piece : (x + 1) * piece] = full_ref[j, row : row + lift].astype(f32)
            row += lift


def lay_out(full, rows, share, latent, half, count, width):
    shape = jax.ShapeDtypeStruct
    gate, up, output, down = rows
    lift = latent // count
    vmem = pl.BlockSpec(memory_space=pltpu.VMEM)
    outs = [
        shape((width, gate), f32),
        shape((width, up), f32),
        shape((output, width), f32),
        shape((down, width), f32),
        shape((share, width), f32),
        shape((share, 2 * latent), f32),
        shape((2, lift, half), f32),
        shape((2, lift, half), f32),
        shape((2, max(share, 128)), f32),
    ]
    return pl.pallas_call(
        functools.partial(lay_out_kernel, rows, latent),
        out_shape=outs,
        in_specs=[vmem],
        out_specs=[vmem] * len(outs),
        compiler_params=pltpu.CompilerParams(vmem_limit_bytes=48 << 20),
        name="lay_out",
    )(full)


def shards(
    hidden_in,
    doc_ids,
    cotangent,
    attn_gain,
    query_weight,
    latent_weight,
    key_lift_weight,
    value_lift_weight,
    output_weight,
    ffn_gain,
    gate_weight,
    up_weight,
    down_weight,
):
    rows, tokens, width = hidden_in.shape
    peers = lax.axis_size("heads")
    place = lax.axis_index("heads")
    core = lax.axis_index("rows") & 1
    groups, latent_size, group_width = key_lift_weight.shape
    count = rows * tokens
    steps = peers // 2
    pieces = lax.axis_size("rows")
    share = width // peers
    side = place & 1
    level = place // 2
    swap = lambda a: flip(a, "rows", 0)
    mine = lambda a, axis: lax.dynamic_slice_in_dim(a, core * (a.shape[axis] // 2), a.shape[axis] // 2, axis)
    theirs = lambda a, axis: lax.dynamic_slice_in_dim(
        a, (1 - core) * (a.shape[axis] // 2), a.shape[axis] // 2, axis
    )

    own_base = place * tokens
    own_docs = lax.dynamic_slice_in_dim(doc_ids, own_base, tokens, 1)
    position = own_base + jnp.arange(tokens, dtype=jnp.int32)
    before = (doc_ids[:, None, :] == own_docs[:, :, None]) & (
        jnp.arange(doc_ids.shape[1], dtype=jnp.int32)[None, None, :] <= position[None, :, None]
    )
    own_start = position[None, :] + 1 - jnp.sum(before.astype(jnp.int32), axis=-1)
    start = jnp.concatenate([own_start, swap(own_start)], axis=0)
    lo = start[:, 0]
    start = start[:, None, :]

    inputs = hidden_in.reshape(count, width).astype(f32)
    inverse_one = rms_inverse(inputs)
    normed_one = (inputs * inverse_one * attn_gain).astype(bf16)
    latent_mine = matmul(normed_one, mine(latent_weight, 1)).astype(bf16)
    latent_sent = matmul(normed_one, theirs(latent_weight, 1)).astype(bf16)
    latent_got = swap(latent_sent)
    own_seg = jnp.concatenate([latent_mine, latent_got], axis=0).reshape(2 * rows, tokens, latent_size)
    query_mine = matmul(normed_one, mine(query_weight, 1)).astype(bf16)
    query_sent = matmul(normed_one, theirs(query_weight, 1)).astype(bf16)
    queries = jnp.concatenate([query_mine, swap(query_sent)], axis=0).reshape(2 * rows, tokens, group_width)

    key_mine = lax.dynamic_index_in_dim(key_lift_weight, core, 0, keepdims=False)
    value_mine = lax.dynamic_index_in_dim(value_lift_weight, core, 0, keepdims=False)
    key_lift = quad_lift(key_mine)
    value_lift = quad_lift(value_mine)
    key_lift_t = head_lift(key_mine)
    value_lift_t = head_lift(value_mine)

    up_chain = [(i, i + 2) for i in range(peers - 2)]
    down_chain = [(i + 2, i) for i in range(peers - 2)]
    segs = []
    bases = []
    moving = own_seg
    for k in range(steps):
        if k > 0:
            moving = lax.ppermute(moving, "heads", up_chain)
            if k > 1:
                moving, crossed = lax.optimization_barrier((moving, segs[-1][1]))
                segs[-1] = (segs[-1][0], crossed)
        segs.append((moving, flip(moving, "heads", 0)))
        base = ((level - k) * 2 + side) * tokens
        other = ((level - k) * 2 + 1 - side) * tokens
        there = level >= k
        bases.append(
            (jnp.where(there, base, -1), jnp.where(there & (other < own_base), other, -1))
        )

    def pick(items):
        return (
            [segs[k][j] for k, j in items],
            jnp.stack([bases[k][j] for k, j in items] + [own_base]).astype(jnp.int32),
        )

    parts = [range(0, steps - 1), range(steps - 1, steps)]
    state = None
    for i, ks in enumerate(parts):
        seg_list, base_list = pick([(k, j) for k in ks for j in range(2)])
        state = attend_part(
            queries, start, key_lift, value_lift_t, lo, seg_list, base_list, state, i == len(parts) - 1
        )
    head_out, lse, head_mix = state
    mixed_mine = head_out[:rows].reshape(count, group_width)
    mixed_got = swap(head_out[rows:]).reshape(count, group_width)
    keep = (own_docs != 0).astype(f32).reshape(count, 1)
    hidden_out, grad_resid, grad_mixed_mine, grad_mixed_sent, ffn_gain_part, down_grad, feed_grads = feed(
        core, hidden_in.reshape(count, width), mixed_mine, mixed_got, output_weight, ffn_gain,
        cotangent.reshape(count, width), keep, (gate_weight, up_weight, down_weight), pieces,
    )
    head_grads = jnp.concatenate([grad_mixed_mine, swap(grad_mixed_sent)], axis=0).reshape(
        2 * rows, tokens, group_width
    )
    early_down = lax.psum_scatter(down_grad, "rows", scatter_dimension=0, tiled=True)[0]
    early_feed = lax.psum_scatter(feed_grads, "rows", scatter_dimension=0, tiled=True)[0]

    calls = [[(k, 0), (k, 1)] for k in range(steps - 1, 0, -1)]
    calls[-1].append((0, 1))
    calls.append([(0, 0)])
    state = None
    pieces_in = []
    waiting = []
    passing = None
    now = queries

    def join(parts):
        total = parts[0].astype(f32) + parts[1].astype(f32)
        if passing is not None:
            total = total + passing.astype(f32)
        return total.astype(bf16)

    for i, items in enumerate(calls):
        if len(waiting) == 2:
            now, joined = lax.optimization_barrier((queries, join(waiting.pop(0))))
            passing = lax.ppermute(joined, "heads", down_chain)
        seg_list, base_list = pick(items)
        made = attend_back_part(
            now, head_grads, lse, head_mix, start, key_lift, value_lift, key_lift_t, lo,
            seg_list, base_list, state, len(items) == 1, 0, 2 * rows,
        )
        state = list(made[len(items) :])
        k = items[0][0]
        if k == 0:
            pieces_in.append(made[0])
            continue
        waiting.append((made[0], flip(made[1], "heads", 0)))
        if k == 1:
            state.append(jnp.zeros_like(state[1]))
            pieces_in.append(flip(made[2], "heads", 0))
    joined = join(waiting.pop())
    query_grads, key_part, value_part = state
    latent_grads = sum(p.astype(f32) for p in pieces_in)

    ff_share = gate_weight.shape[1] // peers
    full, hidden_grad = finish(
        (early_feed, early_down),
        ((ff_share, ff_share, share), (ff_share,)),
        peers,
        (
            hidden_in.reshape(count, width), attn_gain.reshape(1, width),
            query_grads.reshape(2, count, group_width), latent_grads.reshape(2, count, latent_size),
            joined.reshape(2, count, latent_size),
            query_weight, latent_weight, grad_resid, ffn_gain_part, key_part, value_part,
        ),
    )
    (
        gate_share, up_share, output_share, down_share, query_share, latent_share, key_share, value_share, gains,
    ) = lay_out(full, (ff_share, ff_share, share, ff_share), share, latent_size, group_width, peers, width)
    gains = lax.dynamic_slice_in_dim(gains, (place * share) % gains.shape[1], share, 1)
    return (
        hidden_out.reshape(rows, tokens, width),
        hidden_grad.reshape(rows, tokens, width),
        gains[0],
        query_share,
        latent_share,
        key_share,
        value_share,
        output_share,
        gains[1],
        gate_share,
        up_share,
        down_share,
    )


def solution(mesh):
    placed = (
        P("rows", "heads", None),
        P("rows", None),
        P("rows", "heads", None),
        P(),
        P(),
        P(),
        P(),
        P(),
        P(),
        P(),
        P(),
        P(),
        P(),
    )
    return jax.shard_map(
        shards,
        mesh=mesh,
        in_specs=placed,
        out_specs=(
            P("rows", "heads", None),
            P("rows", "heads", None),
            P("heads"),
            P("heads", None),
            P("heads", None),
            P(None, "heads", None),
            P(None, "heads", None),
            P("heads", None),
            P("heads"),
            P(None, "heads"),
            P(None, "heads"),
            P("heads", None),
        ),
        check_vma=False,
    )
```

```python
import functools
import math

import jax
import jax.numpy as jnp
from jax import lax
from jax.experimental import pallas as pl
from jax.experimental.pallas import tpu as pltpu
from jax.sharding import PartitionSpec as P

HEAD_WIDTH = 64
epsilon = 1e-05
blocked = -1e30
LOG2E = math.log2(math.e)
LN2 = math.log(2.0)
QUAD = 4
f32 = jnp.float32
bf16 = jnp.bfloat16


def matmul(left, right):
    return jnp.dot(left, right, preferred_element_type=f32)


def matmul_nt(left, right):
    return lax.dot_general(
        left, right, (((left.ndim - 1,), (right.ndim - 1,)), ((), ())), preferred_element_type=f32
    )


def matmul_tn(left, right):
    return lax.dot_general(left, right, (((0,), (0,)), ((), ())), preferred_element_type=f32)


def rms_inverse(value_matrix):
    return lax.rsqrt(jnp.mean(value_matrix * value_matrix, axis=-1, keepdims=True) + epsilon)


def expand_heads(source, weights, factor, out_ref):
    tokens = source.shape[0]
    quads, wide, deep = weights.shape
    latent = wide // QUAD
    for quad in range(quads):
        product = matmul_nt(weights[quad], source[:, quad * deep : (quad + 1) * deep])
        if factor != 1.0:
            product = product * factor
        product = product.astype(bf16)
        for h in range(QUAD):
            at = (quad * QUAD + h) * tokens
            out_ref[:, at : at + tokens] = product[h * latent : (h + 1) * latent]


def lift_heads(source, weights, tokens):
    parts = [
        matmul(weights[h], source[:, h * tokens : (h + 1) * tokens]) for h in range(weights.shape[0])
    ]
    return jnp.concatenate(parts, axis=0)


def lift_grad(left, right, tokens, out_ref):
    latent = left.shape[0]
    deep = QUAD * HEAD_WIDTH
    head = lax.broadcasted_iota(jnp.int32, (latent, deep), 1) // HEAD_WIDTH
    for quad in range(right.shape[1] // deep):
        columns = slice(quad * deep, (quad + 1) * deep)
        found = None
        for h in range(QUAD):
            at = (quad * QUAD + h) * tokens
            part = matmul(left[:, at : at + tokens], right[:, columns])
            found = part if h == 0 else jnp.where(head == h, part, found)
        out_ref[:, columns] += found


def seg_mask(base, own_base, start):
    tokens = start.shape[-1]
    key_at = lax.broadcasted_iota(jnp.int32, (tokens, tokens), 0)
    query_at = lax.broadcasted_iota(jnp.int32, (tokens, tokens), 1)
    return (key_at >= start - base) & (key_at <= query_at + (own_base - base))


def attend_kernel(count, first, last, lo, bases, *refs):
    refs = list(refs)
    take = lambda k: [refs.pop(0) for _ in range(k)]
    (start_ref,) = take(1)
    if first:
        query_ref, key_lift_ref = take(2)
    else:
        expanded_ref, top_in, total_in, mix_in = take(4)
    seg_refs = take(count)
    if last:
        (value_lift_ref,) = take(1)
        out_ref, lse_ref, mix_ref = take(3)
    else:
        top_out, total_out, mix_out = take(3)
    if first:
        (expanded_ref,) = take(1)
    top, total, mix, segs = take(4)
    expanded = expanded_ref.at[0]
    tokens = start_ref.shape[2]
    heads = expanded.shape[1] // tokens
    row = pl.program_id(0)
    touched = lambda i: (bases[i] >= 0) & (bases[i] + tokens - 1 >= lo[row])
    if first:
        expand_heads(query_ref[0], key_lift_ref, HEAD_WIDTH ** (-0.5) * LOG2E, expanded)
        top[...] = jnp.full_like(top, blocked)
        total[...] = jnp.zeros_like(total)
        mix[...] = jnp.zeros_like(mix)
    else:
        top[...] = top_in[0]
        total[...] = total_in[0]
        mix[...] = mix_in[0].astype(f32)
    for i in range(count):
        segs[i] = seg_refs[i][0]

    @pl.loop(0, count)
    def _(i):
        @pl.when(touched(i))
        def _():
            latent = segs[i]
            latent_t = latent.T
            allow = seg_mask(bases[i], bases[count], start_ref[0])
            for h in range(heads):
                at = slice(h * tokens, (h + 1) * tokens)
                score = jnp.where(allow, matmul(latent, expanded[:, at]), blocked)
                old = top[:, at]
                new = jnp.maximum(old, jnp.max(score, axis=0, keepdims=True))
                probs = jnp.exp2(score - new)
                fade = jnp.exp2(old - new)
                top[:, at] = new
                total[:, at] = total[:, at] * fade + jnp.sum(probs, axis=0, keepdims=True)
                mix[:, at] = mix[:, at] * fade + matmul(latent_t, probs.astype(bf16))

    if not last:
        top_out[0] = top[...]
        total_out[0] = total[...]
        mix_out[0] = mix[...].astype(bf16)
        return
    lse_ref[0] = top[...] + jnp.log2(total[...])
    mix_ref[0] = (mix[...] * (1.0 / total[...])).astype(bf16)
    out_ref[0] = lift_heads(mix_ref[0], value_lift_ref, tokens).T.astype(bf16)


def whole(array):
    return pl.BlockSpec(array.shape, lambda *_: (0,) * len(array.shape))


def by_row(shape):
    return pl.BlockSpec((1,) + tuple(shape[1:]), lambda r, *_: (r,) + (0,) * (len(shape) - 1))


def attend_part(queries, start, key_lift, value_lift_t, lo, segs, bases, expanded, state, last):
    rows, tokens, width = queries.shape
    heads = width // HEAD_WIDTH
    latent = segs[0].shape[-1]
    shape = jax.ShapeDtypeStruct
    stat = shape((rows, 1, heads * tokens), f32)
    flat = shape((rows, latent, heads * tokens), bf16)
    if state is None:
        args = [start, queries, key_lift, *segs]
        specs = [by_row(start.shape), by_row(queries.shape), whole(key_lift)]
    else:
        args = [start, expanded, *state, *segs]
        specs = [by_row(a.shape) for a in args[:5]]
    specs += [by_row(s.shape) for s in segs]
    if last:
        args.append(value_lift_t)
        specs.append(whole(value_lift_t))
        outs = [shape(queries.shape, bf16), stat, flat]
    else:
        outs = [stat, stat, flat]
    if state is None:
        outs.append(flat)
    blocks = rows * heads * len(segs)
    return pl.pallas_call(
        functools.partial(attend_kernel, len(segs), state is None, last),
        out_shape=outs,
        grid_spec=pltpu.PrefetchScalarGridSpec(
            num_scalar_prefetch=2,
            grid=(rows,),
            in_specs=specs,
            out_specs=[by_row(o.shape) for o in outs],
            scratch_shapes=[
                pltpu.VMEM((1, heads * tokens), f32),
                pltpu.VMEM((1, heads * tokens), f32),
                pltpu.VMEM((latent, heads * tokens), f32),
                pltpu.VMEM((len(segs), tokens, latent), bf16),
            ],
        ),
        compiler_params=pltpu.CompilerParams(
            dimension_semantics=("arbitrary",), vmem_limit_bytes=48 << 20
        ),
        cost_estimate=pl.CostEstimate(
            flops=blocks * tokens * tokens * latent * 4,
            bytes_accessed=rows * heads * latent * tokens * 4,
            transcendentals=blocks * tokens * tokens,
        ),
        name="attend",
    )(lo, bases, *args)


def attend_back_kernel(count, first, last, lo, bases, *refs):
    refs = list(refs)
    take = lambda k: [refs.pop(0) for _ in range(k)]
    query_ref, lse_ref, start_ref, expanded_ref, key_lift_t_ref = take(5)
    seg_refs = take(count)
    if first or last:
        grad_ref, mix_ref = take(2)
    if first:
        (value_lift_ref,) = take(1)
    else:
        expanded_grad_ref, delta_ref, query_back_in, key_up_in = take(4)
    grad_refs = take(count)
    query_back_ref, key_up_ref = take(2)
    if last:
        (value_up_ref,) = take(1)
    if first:
        expanded_grad_ref, delta_ref = take(2)
    back, query_back, segs, seg_grads = take(4)
    expanded, expanded_grad = expanded_ref.at[0], expanded_grad_ref.at[0]
    tokens = query_ref.shape[1]
    heads = expanded.shape[1] // tokens
    row = pl.program_id(0)
    scale = HEAD_WIDTH ** (-0.5)
    touched = lambda i: (bases[i] >= 0) & (bases[i] + tokens - 1 >= lo[row])
    any_touched = functools.reduce(jnp.logical_or, [touched(i) for i in range(count)])

    @pl.when(row == 0)
    def _():
        key_up_ref[...] = jnp.zeros_like(key_up_ref) if first else key_up_in[...]
        if last:
            value_up_ref[...] = jnp.zeros_like(value_up_ref)

    query_back[...] = jnp.zeros_like(query_back) if first else query_back_in[0]
    seg_grads[...] = jnp.zeros_like(seg_grads)
    if first:
        expand_heads(grad_ref[0], value_lift_ref, 1.0, expanded_grad)
        delta_ref[0] = jnp.sum(mix_ref[0].astype(f32) * expanded_grad[...].astype(f32), axis=0, keepdims=True)

    @pl.when(any_touched)
    def _():
        back[...] = jnp.zeros_like(back)
        for i in range(count):
            segs[i] = seg_refs[i][0]

    @pl.loop(0, count)
    def _(i):
        @pl.when(touched(i))
        def _():
            latent = segs[i]
            allow = seg_mask(bases[i], bases[count], start_ref[0])
            allow = jnp.concatenate([allow] * heads, axis=1)
            score = matmul(latent, expanded[...])
            probs = jnp.where(allow, jnp.exp2(score - lse_ref[0]), 0.0)
            dprobs = matmul(latent, expanded_grad[...])
            dscore = (probs * (dprobs - delta_ref[0])).astype(bf16)
            by_key = matmul_nt(dscore, expanded[...])
            by_value = matmul_nt(probs.astype(bf16), expanded_grad[...])
            seg_grads[i] = (by_key * LN2 + by_value).astype(bf16)
            back[...] += matmul(latent.T, dscore)

    for i in range(count):
        grad_refs[i][0] = seg_grads[i]

    @pl.when(any_touched)
    def _():
        part = (back[...] * scale).astype(bf16)
        query_back[...] += lift_heads(part, key_lift_t_ref, tokens)
        lift_grad(part, query_ref[0], tokens, key_up_ref)

    if last:
        lift_grad(mix_ref[0], grad_ref[0], tokens, value_up_ref)
        query_back_ref[0] = query_back[...].T.astype(bf16)
    else:
        query_back_ref[0] = query_back[...]


def attend_back_part(queries, grads, lse, mix, start, expanded, value_lift, key_lift_t, lo, segs, bases, kept, state, last):
    rows, tokens, width = queries.shape
    heads = width // HEAD_WIDTH
    latent = segs[0].shape[-1]
    shape = jax.ShapeDtypeStruct
    back_shape = shape((rows, width, tokens), f32)
    up_shape = shape((latent, width), f32)
    first = state is None
    args = [queries, lse, start, expanded, key_lift_t, *segs]
    specs = [by_row(a.shape) for a in args[:4]] + [whole(key_lift_t)]
    specs += [by_row(s.shape) for s in segs]
    if first or last:
        args += [grads, mix]
        specs += [by_row(grads.shape), by_row(mix.shape)]
    if first:
        args.append(value_lift)
        specs.append(whole(value_lift))
    else:
        args += [*kept, *state]
        specs += [by_row(kept[0].shape), by_row(kept[1].shape), by_row(back_shape.shape), whole(up_shape)]
    outs = [shape(s.shape, bf16) for s in segs]
    outs += [shape(queries.shape, bf16) if last else back_shape, up_shape]
    out_specs = [by_row(o.shape) for o in outs[:-1]] + [whole(up_shape)]
    if last:
        outs.append(up_shape)
        out_specs.append(whole(up_shape))
    if first:
        outs += [shape(expanded.shape, bf16), shape(lse.shape, f32)]
        out_specs += [by_row(expanded.shape), by_row(lse.shape)]
    blocks = rows * heads * len(segs)
    return pl.pallas_call(
        functools.partial(attend_back_kernel, len(segs), first, last),
        out_shape=outs,
        grid_spec=pltpu.PrefetchScalarGridSpec(
            num_scalar_prefetch=2,
            grid=(rows,),
            in_specs=specs,
            out_specs=out_specs,
            scratch_shapes=[
                pltpu.VMEM((latent, heads * tokens), f32),
                pltpu.VMEM((width, tokens), f32),
                pltpu.VMEM((len(segs), tokens, latent), bf16),
                pltpu.VMEM((len(segs), tokens, latent), bf16),
            ],
        ),
        compiler_params=pltpu.CompilerParams(
            dimension_semantics=("arbitrary",), vmem_limit_bytes=48 << 20
        ),
        cost_estimate=pl.CostEstimate(
            flops=blocks * tokens * tokens * latent,
            bytes_accessed=rows * heads * latent * tokens,
            transcendentals=0,
        ),
        name="attend_back",
    )(lo, bases, *args)


def quad_lift(lift):
    latent, width = lift.shape
    deep = QUAD * HEAD_WIDTH
    quads = width // deep
    tall = jnp.tile(lift.reshape(latent, quads, deep).transpose(1, 0, 2), (1, QUAD, 1))
    row_head = lax.broadcasted_iota(jnp.int32, tall.shape, 1) // latent
    column_head = lax.broadcasted_iota(jnp.int32, tall.shape, 2) // HEAD_WIDTH
    return jnp.where(row_head == column_head, tall, jnp.zeros_like(tall))


def head_lift(lift):
    latent, width = lift.shape
    return lift.T.reshape(width // HEAD_WIDTH, HEAD_WIDTH, latent)


def put_pieces(ref, value, at=0):
    pieces, _, piece = ref.shape
    for j in range(pieces):
        ref[j, pl.ds(at, value.shape[0])] = value[:, j * piece : (j + 1) * piece].astype(bf16)


def feed_kernel(core_ref, *refs):
    (
        inputs_ref, mine_ref, got_ref, output_ref, gain_ref, cotangent_ref, keep_ref,
        gate_ref, up_ref, down_ref,
        hidden_out_ref, resid, normed, back, active_ref, slope_ref, down_grad_ref,
        result, hidden,
    ) = refs
    step = pl.program_id(0)
    count = inputs_ref.shape[0]
    block = min(256, count)
    core = core_ref[0]

    @pl.when(step == 0)
    def _():
        for t in range(0, count, block):
            at = slice(t, t + block)
            row = inputs_ref[at].astype(f32) + (
                matmul(mine_ref[at], output_ref[core]) + matmul(got_ref[at], output_ref[1 - core])
            )
            resid[at] = row
            scale = lax.rsqrt(jnp.mean(row * row, axis=-1, keepdims=True) + epsilon)
            normed[at] = (row * scale * gain_ref[...]).astype(bf16)
            back[at] = (cotangent_ref[at].astype(f32) * keep_ref[at]).astype(bf16)
        result[...] = jnp.zeros_like(result)

    part = count // 4
    for t in range(0, count, part):
        at = slice(t, t + part)
        gate = matmul(normed[at], gate_ref[...])
        up = matmul(normed[at], up_ref[...])
        sigmoid = 1.0 / (1.0 + jnp.exp(-gate))
        active = gate * sigmoid
        hidden[at] = (active * up).astype(bf16)
        active_ref[at] = active.astype(bf16)
        slope_ref[at] = (up * (sigmoid * (1.0 + gate * (1.0 - sigmoid)))).astype(bf16)
    put_pieces(down_grad_ref, matmul_tn(hidden[...], back[...]))
    result[...] += matmul(hidden[...], down_ref[...])

    @pl.when(step == pl.num_programs(0) - 1)
    def _():
        hidden_out_ref[...] = (resid[...] + result[...]).astype(bf16)


def feed_back_kernel(core_ref, *refs):
    (
        mine_ref, got_ref, output_ref, gain_ref, resid_ref, normed, back,
        active_ref, slope_ref, gate_ref, up_ref, down_ref,
        grad_resid_ref, head_mine_ref, head_sent_ref, gain_grad_ref, grads_ref,
        grad_two, both, low, staged, staged_out, sems, out_sem,
    ) = refs
    step = pl.program_id(0)
    steps = pl.num_programs(0)
    count, width = resid_ref.shape
    chunk = down_ref.shape[0]
    ff = (grads_ref.shape[1] - width) // 2
    block = min(256, count)
    core = core_ref[0]
    slot = step % 2

    def leave(at, kind, place):
        return pltpu.make_async_copy(
            staged.at[at, kind],
            grads_ref.at[:, pl.ds(pl.multiple_of(kind * ff + place * chunk, chunk), chunk)],
            sems.at[at, kind],
        )

    @pl.when(step >= 2)
    def _():
        for kind in range(2):
            leave(slot, kind, step - 2).wait()

    @pl.when(step == 0)
    def _():
        grad_two[...] = jnp.zeros_like(grad_two)

    part = count // 4
    for t in range(0, count, part):
        at = slice(t, t + part)
        grad_act = matmul_nt(back[at], down_ref[...])
        both[at, :chunk] = (grad_act * slope_ref[at].astype(f32)).astype(bf16)
        both[at, chunk:] = (grad_act * active_ref[at].astype(f32)).astype(bf16)
    for kind in range(2):
        put_pieces(staged.at[slot, kind], matmul_tn(both[:, kind * chunk : (kind + 1) * chunk], normed[...]))
        leave(slot, kind, step).start()
    weights = jnp.concatenate([gate_ref[...], up_ref[...]], axis=1)
    for t in range(0, count, part):
        at = slice(t, t + part)
        grad_two[at] += matmul_nt(both[at], weights)

    @pl.when(step == steps - 1)
    def _():
        gain_total = jnp.zeros((1, width), f32)
        for t in range(0, count, block):
            at = slice(t, t + block)
            row = resid_ref[at]
            scale = lax.rsqrt(jnp.mean(row * row, axis=-1, keepdims=True) + epsilon)
            unit = row * scale
            grad = grad_two[at]
            gain_total += jnp.sum(grad * unit, axis=0, keepdims=True)
            scaled = grad * gain_ref[...]
            grad = back[at].astype(f32) + scale * (
                scaled - unit * jnp.mean(scaled * unit, axis=-1, keepdims=True)
            )
            grad_resid_ref[at] = grad
            low[at] = grad.astype(bf16)
            head_mine_ref[at] = matmul_nt(low[at], output_ref[core]).astype(bf16)
            head_sent_ref[at] = matmul_nt(low[at], output_ref[1 - core]).astype(bf16)
        gain_grad_ref[...] = gain_total
        half = mine_ref.shape[1]
        put_pieces(staged_out, matmul_tn(mine_ref[...], low[...]), core * half)
        put_pieces(staged_out, matmul_tn(got_ref[...], low[...]), (1 - core) * half)
        last = pltpu.make_async_copy(staged_out, grads_ref.at[:, pl.ds(2 * ff, width)], out_sem)
        last.start()
        for kind in range(2):
            leave(1 - slot, kind, step - 1).wait()
            leave(slot, kind, step).wait()
        last.wait()


def once(array):
    return pl.BlockSpec(array.shape, lambda *_: (0,) * len(array.shape), pipeline_mode=pl.Buffered(1))


def feed(core, inputs, mixed_mine, mixed_got, output_weight, gain, cotangent, keep, weights, pieces):
    count, width = inputs.shape
    gate_weight, up_weight, down_weight = weights
    ff = gate_weight.shape[1]
    chunk = 256
    piece = width // pieces
    output_weight = output_weight.reshape(2, -1, width)
    gain = gain.reshape(1, width)
    by_rows = pl.BlockSpec((chunk, width), lambda c, *_: (c, 0))
    by_columns = pl.BlockSpec((width, chunk), lambda c, *_: (0, c))
    kept_columns = pl.BlockSpec((count, chunk), lambda c, *_: (0, c))
    shape = jax.ShapeDtypeStruct
    params = pltpu.CompilerParams(dimension_semantics=("arbitrary",), vmem_limit_bytes=60 << 20)
    full_bf, full_f = shape((count, width), bf16), shape((count, width), f32)
    kept = shape((count, ff), bf16)
    firsts = [inputs, mixed_mine, mixed_got, output_weight, gain, cotangent, keep]
    outs = [full_bf, full_f, full_bf, full_bf, kept, kept, shape((pieces, ff, piece), bf16)]
    hidden_out, resid, normed, back, active, slope, down_grad = pl.pallas_call(
        feed_kernel,
        out_shape=outs,
        grid_spec=pltpu.PrefetchScalarGridSpec(
            num_scalar_prefetch=1,
            grid=(ff // chunk,),
            in_specs=[once(a) for a in firsts] + [by_columns, by_columns, by_rows],
            out_specs=[once(o) for o in outs[:4]]
            + [kept_columns, kept_columns, pl.BlockSpec((pieces, chunk, piece), lambda c, *_: (0, c, 0))],
            scratch_shapes=[pltpu.VMEM((count, width), f32), pltpu.VMEM((count, chunk), bf16)],
        ),
        compiler_params=params,
        cost_estimate=pl.CostEstimate(
            flops=count * width * (ff * 8 + width * 2),
            bytes_accessed=width * ff * 8 + count * width * 16 + count * ff * 4,
            transcendentals=count * ff,
        ),
        name="feed",
    )(core.reshape(1), *firsts, *weights)
    firsts = [mixed_mine, mixed_got, output_weight, gain, resid, normed, back]
    outs = [
        full_f,
        shape(mixed_mine.shape, bf16),
        shape(mixed_mine.shape, bf16),
        shape((1, width), f32),
        shape((pieces, 2 * ff + width, piece), bf16),
    ]
    grad_resid, head_mine, head_sent, gain_grad, grads = pl.pallas_call(
        feed_back_kernel,
        out_shape=outs,
        grid_spec=pltpu.PrefetchScalarGridSpec(
            num_scalar_prefetch=1,
            grid=(ff // chunk,),
            in_specs=[once(a) for a in firsts]
            + [kept_columns, kept_columns, by_columns, by_columns, by_rows],
            out_specs=[once(o) for o in outs[:4]] + [pl.BlockSpec(memory_space=pl.ANY)],
            scratch_shapes=[
                pltpu.VMEM((count, width), f32),
                pltpu.VMEM((count, 2 * chunk), bf16),
                pltpu.VMEM((count, width), bf16),
                pltpu.VMEM((2, 2, pieces, chunk, piece), bf16),
                pltpu.VMEM((pieces, width, piece), bf16),
                pltpu.SemaphoreType.DMA((2, 2)),
                pltpu.SemaphoreType.DMA,
            ],
        ),
        compiler_params=params,
        cost_estimate=pl.CostEstimate(
            flops=count * width * (ff * 10 + width * 4),
            bytes_accessed=width * ff * 10 + count * width * 20 + count * ff * 4,
            transcendentals=0,
        ),
        name="feed_back",
    )(core.reshape(1), *firsts, active, slope, *weights)
    return hidden_out, grad_resid, head_mine, head_sent, gain_grad, down_grad, grads


def flip(array, axis, bit):
    size = lax.axis_size(axis)
    return lax.ppermute(array, axis, [(i, i ^ (1 << bit)) for i in range(size)])


def fill_shards(target, at, grad, count):
    along, piece = target.shape[0], target.shape[3]
    size = grad.shape[0] // count
    for s in range(count):
        for j in range(along):
            target[j, s, at : at + size] = grad[s * size : (s + 1) * size, j * piece : (j + 1) * piece].astype(bf16)


def fill_folded(target, at, grad, count):
    along, piece = target.shape[0], target.shape[3]
    size = grad.shape[0] // count
    latent = grad.shape[1]
    fold = size // 2
    for s in range(count):
        for j in range(along):
            side, column = divmod(j * piece, latent)
            first = s * size + side * fold
            target[j, s, at : at + fold] = grad[first : first + fold, column : column + piece].astype(bf16)


def fill_gains(target, at, gain, count):
    along, piece = target.shape[0], target.shape[3]
    share = gain.shape[1] // count
    lane = max(share, 128)
    for s in range(count):
        begin = s * share // lane * lane
        kept = jnp.broadcast_to(gain[:, begin : begin + lane], (16, lane)).astype(bf16)
        target[0, s, at : at + 16, :lane] = kept
        if piece > lane:
            target[0, s, at : at + 16, lane:] = jnp.zeros((16, piece - lane), bf16)
        for j in range(1, along):
            target[j, s, at : at + 16] = jnp.zeros((16, piece), bf16)


def finish_kernel(sections, groups, sizes, refs):
    (
        early_refs, inputs_ref, gain_ref, query_grad_ref, latent_grad_ref, joined_ref,
        query_ref, latent_ref, resid_ref, other_gain_ref, key_up, value_up,
        out_ref, grad_ref,
        normed, own_ref, sent_ref, late_got, late_from, got_first, got_next,
        chain_got, query_got, latent_low, latent_got,
        chain_sems, core_sems, along_sems, first_sems, first_late_sems, next_sems, out_sems,
    ) = refs
    along, count, late_rows, piece = own_ref.shape
    early_rows, share, fold, lift = sizes
    bits = count.bit_length() - 1
    row_at = lax.axis_index("rows")
    place = lax.axis_index("heads")
    core = row_at % 2
    x_at = row_at // 2
    mesh = pl.DeviceIdType.MESH
    tokens, width = inputs_ref.shape
    latent = latent_low.shape[2]
    half = query_got.shape[1]
    block = min(256, tokens)
    parts = [slice(0, early_rows)] + [slice(early_rows + g[0], early_rows + g[1]) for g in groups]

    def turned(which):
        at = place
        for bit in which:
            at = at + (1 << bit) * (1 - 2 * ((place // (1 << bit)) % 2))
        return at

    core_peer = (row_at + 1 - 2 * core, place)
    x_others = [(x_at + d) % along for d in range(1, along)]
    x_peers = [(x * 2 + core, place) for x in x_others]
    head_peers = [(row_at, turned([bit])) for bit in range(bits)]
    above = (row_at, (place + 2) % count)
    below = (row_at, (place + count - 2) % count)
    barrier = pltpu.get_barrier_semaphore()
    everyone = [core_peer, above, below] + x_peers + head_peers
    for peer in everyone:
        pl.semaphore_signal(barrier, inc=1, device_id=peer, device_id_type=mesh)
    pl.semaphore_wait(barrier, len(everyone))

    def remote(source, target, sems, index, peer):
        return pltpu.make_async_remote_copy(
            src_ref=source, dst_ref=target, send_sem=sems.at[(0,) + index], recv_sem=sems.at[(1,) + index],
            device_id=peer, device_id_type=mesh,
        )

    def orders(bit):
        rest = list(range(bit + 1, bits))
        return [
            [b for i, b in enumerate(rest) if not (mask >> (len(rest) - 1 - i)) & 1]
            for mask in range(1 << len(rest))
        ]

    def add_rows(target, other, size):
        step = size if size <= 600 else size // 2

        def one(i, carry):
            at = pl.ds(pl.multiple_of(i * step, 16), step)
            target[at] = (target[at].astype(f32) + other[at].astype(f32)).astype(bf16)
            return carry

        lax.fori_loop(0, size // step, one, 0)

    def rows_of(part):
        return pl.ds(part.start, part.stop - part.start)

    first = orders(0)
    final = len(first) - 1
    pending = []

    def early_rows_of(n, shard):
        which, start, size, _ = sections[n]
        return early_refs[which].at[pl.ds(pl.multiple_of(start + shard * size, 16), size)]

    def first_early(i, n):
        _, _, size, row = sections[n]
        return remote(
            early_rows_of(n, turned([0] + first[i])), got_first.at[i, pl.ds(row, size)],
            first_sems, (i, n), head_peers[0],
        )

    def next_copy(bit, j, i, which):
        rows = rows_of(parts[which])
        return remote(
            got_first.at[i, rows], got_next[bit - 1].at[j, rows], next_sems[bit - 1], (j, which), head_peers[bit]
        )

    def settle(i, which):
        rest = first[i]
        level = rest[0] if rest else bits
        rows = rows_of(parts[which])
        for bit in range(1, level):
            j = orders(bit).index(rest)
            next_copy(bit, j, i, which).wait_recv()
            add_rows(got_first.at[i, rows], got_next[bit - 1].at[j, rows], rows.size)
        if rest:
            copy = next_copy(level, orders(level).index(rest[1:]), i, which)
            copy.start()
            pending.append(copy)

    def early_step(i):
        for n, (_, _, size, row) in enumerate(sections):
            first_early(i, n).wait()
            add_rows(got_first.at[i, pl.ds(row, size)], early_rows_of(n, turned(first[i])), size)
        settle(i, 0)

    def core_copy(g):
        _, _, begin, end = groups[g]
        rows = pl.ds(begin, end - begin)
        return remote(sent_ref.at[:, :, rows], late_got.at[:, :, rows], core_sems, (g,), core_peer)

    def x_copies(g):
        low, high, begin, end = groups[g]
        shared = end - begin
        copies = []
        for d, (x, peer) in enumerate(zip(x_others, x_peers)):
            copies.append(
                remote(
                    late_got.at[x, :, pl.ds(begin, shared)], late_from.at[d, :, pl.ds(low, shared)],
                    along_sems, (d, g, 0), peer,
                )
            )
            if low + shared < high:
                rows = pl.ds(low + shared, high - low - shared)
                copies.append(
                    remote(own_ref.at[x, :, rows], late_from.at[d, :, rows], along_sems, (d, g, 1), peer)
                )
        return copies

    def along_x(g):
        low, _, begin, end = groups[g]
        core_copy(g).wait()

        def core_add(i, carry):
            j, s = i // count, i % count
            mine = own_ref[j, s, low : low + end - begin].astype(f32)
            late_got[j, s, begin:end] = (mine + late_got[j, s, begin:end].astype(f32)).astype(bf16)
            return carry

        lax.fori_loop(0, along * count, core_add, 0)
        for copy in x_copies(g):
            copy.start()

    def first_late(i, g):
        low, high, _, _ = groups[g]
        return remote(
            late_from.at[0, turned([0] + first[i]), pl.ds(low, high - low)],
            got_first.at[i, rows_of(parts[1 + g])], first_late_sems, (i, g), head_peers[0],
        )

    def over_heads(g):
        low, high, begin, end = groups[g]
        middle = low + end - begin
        for copy in x_copies(g):
            copy.wait()

        def x_add(s, carry):
            total = late_got[x_at, s, begin:end].astype(f32)
            for d in range(along - 1):
                total = total + late_from[d, s, low:middle].astype(f32)
            late_from[0, s, low:middle] = total.astype(bf16)
            if middle < high:
                total = own_ref[x_at, s, middle:high].astype(f32)
                for d in range(along - 1):
                    total = total + late_from[d, s, middle:high].astype(f32)
                late_from[0, s, middle:high] = total.astype(bf16)
            return carry

        lax.fori_loop(0, count, x_add, 0)
        for i in range(len(first)):
            first_late(i, g).start()

    def late_step(i, g):
        low, high, _, _ = groups[g]
        first_late(i, g).wait()
        add_rows(
            got_first.at[i, rows_of(parts[1 + g])],
            late_from.at[0, turned(first[i]), pl.ds(low, high - low)],
            high - low,
        )
        settle(i, 1 + g)

    mine = lambda ref, size: ref[:, pl.ds(pl.multiple_of(core * size, size), size)]
    theirs = lambda ref, size: ref[:, pl.ds(pl.multiple_of((1 - core) * size, size), size)]
    chain_copy = remote(joined_ref, chain_got, chain_sems, (0,), below)
    chain_copy.start()
    query_copy = remote(query_grad_ref.at[1], query_got, chain_sems, (1,), core_peer)
    query_copy.start()
    for i in range(len(first)):
        for n in range(len(sections)):
            first_early(i, n).start()

    @pl.loop(0, tokens // block)
    def _(t):
        at = pl.ds(pl.multiple_of(t * block, block), block)
        row = inputs_ref[at].astype(f32)
        scale = lax.rsqrt(jnp.mean(row * row, axis=-1, keepdims=True) + epsilon)
        normed[at] = (row * scale * gain_ref[...]).astype(bf16)

    fill_shards(own_ref, 0, matmul_tn(normed[...], query_grad_ref[0]), count)
    fill_shards(own_ref, share, key_up[...], count)
    fill_shards(own_ref, share + lift, value_up[...], count)
    query_copy.wait()
    fill_shards(sent_ref, 0, matmul_tn(normed[...], query_got[...]), count)
    core_copy(0).start()
    early_step(0)
    along_x(0)
    for i in range(1, len(first) // 2):
        early_step(i)

    chain_copy.wait()
    for side in (1, 0):
        for t in range(0, tokens, block):
            at = slice(t, t + block)
            latent_low[side, at] = (latent_grad_ref[side, at] + chain_got[side, at].astype(f32)).astype(bf16)
        if side == 1:
            latent_copy = remote(latent_low.at[1], latent_got, chain_sems, (2,), core_peer)
            latent_copy.start()
    latent_copy.wait()

    def back(t, gain_total):
        at = pl.ds(pl.multiple_of(t * block, block), block)
        row = inputs_ref[at].astype(f32)
        scale = lax.rsqrt(jnp.mean(row * row, axis=-1, keepdims=True) + epsilon)
        unit = row * scale
        grad = (
            matmul_nt(query_grad_ref[0, at], mine(query_ref, half))
            + matmul_nt(query_got[at], theirs(query_ref, half))
            + matmul_nt(latent_low[0, at], mine(latent_ref, latent))
            + matmul_nt(latent_got[at], theirs(latent_ref, latent))
        )
        scaled = grad * gain_ref[...]
        grad_ref[at] = resid_ref[at] + scale * (
            scaled - unit * jnp.mean(scaled * unit, axis=-1, keepdims=True)
        )
        return gain_total + jnp.sum(grad * unit, axis=0, keepdims=True)

    gain_total = lax.fori_loop(0, tokens // block, back, jnp.zeros((1, width), f32))
    other = other_gain_ref[...]
    low = groups[1][0]
    for target, at, latents, gain in (
        (own_ref, low, latent_low[0], jnp.where(core == 0, gain_total, other)),
        (sent_ref, groups[1][2], latent_got[...], jnp.where(core == 0, other, gain_total)),
    ):
        fill_folded(target, at, matmul_tn(normed[...], latents), count)
        fill_gains(target, at + fold, gain, count)
    core_copy(1).start()
    over_heads(0)
    along_x(1)
    for i in range(max(1, len(first) // 2), final):
        early_step(i)
    over_heads(1)
    for i in range(final):
        for g in range(len(groups)):
            late_step(i, g)

    def spread(which):
        rows = rows_of(parts[which])
        out_ref[row_at, rows] = got_first[final, rows]
        copies = [remote(out_ref.at[row_at, rows], out_ref.at[row_at, rows], out_sems, (which, 0), core_peer)]
        for d, peer in enumerate(x_peers):
            copies.append(
                remote(out_ref.at[row_at, rows], out_ref.at[row_at, rows], out_sems, (which, 1 + d), peer)
            )
        for copy in copies:
            copy.start()
        return copies

    def pass_on(which, copies):
        rows = rows_of(parts[which])
        more = []
        for d in range(along - 1):
            copies[1 + d].wait_recv()
            source = ((x_at + along - 1 - d) % along) * 2 + core
            more.append(
                remote(
                    out_ref.at[source, rows], out_ref.at[source, rows], out_sems, (which, along + d), core_peer
                )
            )
            more[-1].start()
        return more

    early_step(final)
    spreads = [spread(0)]
    for g in range(len(groups)):
        late_step(final, g)
        spreads.append(spread(1 + g))
    passes = [pass_on(which, copies) for which, copies in enumerate(spreads)]
    for copies, more in zip(spreads, passes):
        copies[0].wait()
        for copy in copies[1:]:
            copy.wait_send()
        for copy in more:
            copy.wait()
    for copy in pending:
        copy.wait_send()


def finish(early, shares, count, late_args):
    inputs, _, query_grads, latent_grads = late_args[:4]
    tokens, width = inputs.shape
    latent = latent_grads.shape[2]
    piece = early[0].shape[1]
    along = width // piece // 2
    share = width // count
    fold, lift = share // 2, latent // count
    bits = count.bit_length() - 1
    groups = [
        (0, share + 2 * lift, 0, share),
        (share + 2 * lift, share + 2 * lift + fold + 16, share, share + fold + 16),
    ]
    late_rows, shared_rows = groups[1][1], groups[1][3]
    sections = []
    row = 0
    for which, of_one in enumerate(shares):
        start = 0
        for size in of_one:
            sections.append((which, start, size, row))
            start += size * count
            row += size
    total = row + late_rows
    vmem = pl.BlockSpec(memory_space=pltpu.VMEM)
    dma = pltpu.SemaphoreType.DMA

    def body(*refs):
        refs = list(refs)
        take = lambda k: [refs.pop(0) for _ in range(k)]
        given = [take(len(early))] + take(len(late_args)) + take(2)
        given += take(6) + [take(bits - 1)] + take(4) + take(5) + [take(bits - 1)] + take(1)
        finish_kernel(sections, groups, (row, share, fold, lift), given)

    return pl.pallas_call(
        body,
        out_shape=[
            jax.ShapeDtypeStruct((2 * along, total, piece), bf16),
            jax.ShapeDtypeStruct((tokens, width), f32),
        ],
        in_specs=[vmem] * (len(early) + len(late_args)),
        out_specs=[vmem] * 2,
        scratch_shapes=[
            pltpu.VMEM((tokens, width), bf16),
            pltpu.VMEM((along, count, late_rows, piece), bf16),
            pltpu.VMEM((along, count, shared_rows, piece), bf16),
            pltpu.VMEM((along, count, shared_rows, piece), bf16),
            pltpu.VMEM((along - 1, count, late_rows, piece), bf16),
            pltpu.VMEM((count // 2, total, piece), bf16),
        ]
        + [pltpu.VMEM((count >> (bit + 1), total, piece), bf16) for bit in range(1, bits)]
        + [
            pltpu.VMEM((2, tokens, latent), bf16),
            pltpu.VMEM(query_grads.shape[1:], bf16),
            pltpu.VMEM((2, tokens, latent), bf16),
            pltpu.VMEM((tokens, latent), bf16),
            dma((2, 3)),
            dma((2, 2)),
            dma((2, along - 1, 2, 2)),
            dma((2, count // 2, len(sections))),
            dma((2, count // 2, 2)),
        ]
        + [dma((2, count >> (bit + 1), 3)) for bit in range(1, bits)]
        + [dma((2, 3, 2 * along))],
        compiler_params=pltpu.CompilerParams(
            collective_id=0, has_side_effects=True, vmem_limit_bytes=60 << 20
        ),
        name="finish",
    )(*early, *late_args)


def lay_out_kernel(rows, latent, full_ref, gate_ref, up_ref, output_ref, down_ref, query_ref, latent_ref, key_ref, value_ref, gains_ref):
    pieces, _, piece = full_ref.shape
    at = 0
    for ref, size in zip((gate_ref, up_ref, output_ref, down_ref), rows):
        for j in range(pieces):
            ref[:, j * piece : (j + 1) * piece] = full_ref[j, at : at + size].astype(f32)
        at += size
    share = query_ref.shape[0]
    fold = share // 2
    lift = key_ref.shape[1]
    half = key_ref.shape[2]
    lane = gains_ref.shape[1]
    for j in range(pieces):
        x, core = divmod(j, 2)
        row = at
        query_ref[:, core * half + x * piece : core * half + (x + 1) * piece] = full_ref[
            j, row : row + share
        ].astype(f32)
        row += share
        for ref in (key_ref, value_ref):
            ref[core, :, x * piece : (x + 1) * piece] = full_ref[j, row : row + lift].astype(f32)
            row += lift
        side, column = divmod(x * piece, latent)
        column += core * latent
        latent_ref[side * fold : (side + 1) * fold, column : column + piece] = full_ref[
            j, row : row + fold
        ].astype(f32)
        row += fold
        if x == 0:
            gains_ref[core : core + 1] = full_ref[j, row : row + 16, :lane].astype(f32)[:1]


def lay_out(full, rows, share, latent, half, count, width):
    shape = jax.ShapeDtypeStruct
    gate, up, output, down = rows
    lift = latent // count
    vmem = pl.BlockSpec(memory_space=pltpu.VMEM)
    outs = [
        shape((gate, width), f32),
        shape((up, width), f32),
        shape((output, width), f32),
        shape((down, width), f32),
        shape((share, width), f32),
        shape((share, 2 * latent), f32),
        shape((2, lift, half), f32),
        shape((2, lift, half), f32),
        shape((2, max(share, 128)), f32),
    ]
    return pl.pallas_call(
        functools.partial(lay_out_kernel, rows, latent),
        out_shape=outs,
        in_specs=[vmem],
        out_specs=[vmem] * len(outs),
        compiler_params=pltpu.CompilerParams(vmem_limit_bytes=48 << 20),
        name="lay_out",
    )(full)


def shards(
    hidden_in,
    doc_ids,
    cotangent,
    attn_gain,
    query_weight,
    latent_weight,
    key_lift_weight,
    value_lift_weight,
    output_weight,
    ffn_gain,
    gate_weight,
    up_weight,
    down_weight,
):
    rows, tokens, width = hidden_in.shape
    peers = lax.axis_size("heads")
    place = lax.axis_index("heads")
    core = lax.axis_index("rows") & 1
    groups, latent_size, group_width = key_lift_weight.shape
    count = rows * tokens
    steps = peers // 2
    pieces = lax.axis_size("rows")
    share = width // peers
    side = place & 1
    level = place // 2
    swap = lambda a: flip(a, "rows", 0)
    mine = lambda a, axis: lax.dynamic_slice_in_dim(a, core * (a.shape[axis] // 2), a.shape[axis] // 2, axis)
    theirs = lambda a, axis: lax.dynamic_slice_in_dim(
        a, (1 - core) * (a.shape[axis] // 2), a.shape[axis] // 2, axis
    )

    own_base = place * tokens
    own_docs = lax.dynamic_slice_in_dim(doc_ids, own_base, tokens, 1)
    position = own_base + jnp.arange(tokens, dtype=jnp.int32)
    before = (doc_ids[:, None, :] == own_docs[:, :, None]) & (
        jnp.arange(doc_ids.shape[1], dtype=jnp.int32)[None, None, :] <= position[None, :, None]
    )
    own_start = position[None, :] + 1 - jnp.sum(before.astype(jnp.int32), axis=-1)
    start = jnp.concatenate([own_start, swap(own_start)], axis=0)
    lo = start[:, 0]
    start = start[:, None, :]

    inputs = hidden_in.reshape(count, width).astype(f32)
    inverse_one = rms_inverse(inputs)
    normed_one = (inputs * inverse_one * attn_gain).astype(bf16)
    latent_mine = matmul(normed_one, mine(latent_weight, 1)).astype(bf16)
    latent_sent = matmul(normed_one, theirs(latent_weight, 1)).astype(bf16)
    latent_got = swap(latent_sent)
    own_seg = jnp.concatenate([latent_mine, latent_got], axis=0).reshape(2 * rows, tokens, latent_size)
    query_mine = matmul(normed_one, mine(query_weight, 1)).astype(bf16)
    query_sent = matmul(normed_one, theirs(query_weight, 1)).astype(bf16)
    queries = jnp.concatenate([query_mine, swap(query_sent)], axis=0).reshape(2 * rows, tokens, group_width)

    key_mine = lax.dynamic_index_in_dim(key_lift_weight, core, 0, keepdims=False)
    value_mine = lax.dynamic_index_in_dim(value_lift_weight, core, 0, keepdims=False)
    key_lift = quad_lift(key_mine)
    value_lift = quad_lift(value_mine)
    key_lift_t = head_lift(key_mine)
    value_lift_t = head_lift(value_mine)

    up_chain = [(i, i + 2) for i in range(peers - 2)]
    down_chain = [(i + 2, i) for i in range(peers - 2)]
    segs = []
    bases = []
    moving = own_seg
    for k in range(steps):
        if k > 0:
            moving = lax.ppermute(moving, "heads", up_chain)
            moving, crossed = lax.optimization_barrier((moving, segs[-1][1]))
            segs[-1] = (segs[-1][0], crossed)
        segs.append((moving, flip(moving, "heads", 0)))
        base = ((level - k) * 2 + side) * tokens
        other = ((level - k) * 2 + 1 - side) * tokens
        there = level >= k
        bases.append(
            (jnp.where(there, base, -1), jnp.where(there & (other < own_base), other, -1))
        )

    def pick(items):
        return (
            [segs[k][j] for k, j in items],
            jnp.stack([bases[k][j] for k, j in items] + [own_base]).astype(jnp.int32),
        )

    parts = [range(0, steps - 1), range(steps - 1, steps)]
    state = expanded = None
    for i, ks in enumerate(parts):
        seg_list, base_list = pick([(k, j) for k in ks for j in range(2)])
        made = attend_part(
            queries, start, key_lift, value_lift_t, lo, seg_list, base_list, expanded, state, i == len(parts) - 1
        )
        state = made[:3]
        if i == 0:
            expanded = made[3]
    head_out, lse, head_mix = state
    mixed_mine = head_out[:rows].reshape(count, group_width)
    mixed_got = swap(head_out[rows:]).reshape(count, group_width)
    keep = (own_docs != 0).astype(f32).reshape(count, 1)
    hidden_out, grad_resid, grad_mixed_mine, grad_mixed_sent, ffn_gain_part, down_grad, feed_grads = feed(
        core, hidden_in.reshape(count, width), mixed_mine, mixed_got, output_weight, ffn_gain,
        cotangent.reshape(count, width), keep, (gate_weight, up_weight, down_weight), pieces,
    )
    head_grads = jnp.concatenate([grad_mixed_mine, swap(grad_mixed_sent)], axis=0).reshape(
        2 * rows, tokens, group_width
    )
    early_down = lax.psum_scatter(down_grad, "rows", scatter_dimension=0, tiled=True)[0]
    early_feed = lax.psum_scatter(feed_grads, "rows", scatter_dimension=0, tiled=True)[0]

    calls = [[(k, 0), (k, 1)] for k in range(steps - 1, 0, -1)]
    calls[-1].append((0, 1))
    calls.append([(0, 0)])
    state = kept = None
    pieces_in = []
    waiting = []
    passing = None
    now = queries

    def join(parts):
        total = parts[0].astype(f32) + parts[1].astype(f32)
        if passing is not None:
            total = total + passing.astype(f32)
        return total.astype(bf16)

    for i, items in enumerate(calls):
        if len(waiting) == 2:
            now, joined = lax.optimization_barrier((queries, join(waiting.pop(0))))
            passing = lax.ppermute(joined, "heads", down_chain)
        seg_list, base_list = pick(items)
        made = attend_back_part(
            now, head_grads, lse, head_mix, start, expanded, value_lift, key_lift_t, lo,
            seg_list, base_list, kept, state, len(items) == 1,
        )
        state = made[len(items) : len(items) + 2]
        if i == 0:
            kept = made[len(items) + 2 :]
        k = items[0][0]
        if k == 0:
            pieces_in.append(made[0])
            continue
        waiting.append((made[0], flip(made[1], "heads", 0)))
        if k == 1:
            pieces_in.append(flip(made[2], "heads", 0))
    joined = join(waiting.pop())
    query_grads, key_part, value_part = made[1:]
    latent_grads = sum(p.astype(f32) for p in pieces_in)

    ff_share = gate_weight.shape[1] // peers
    full, hidden_grad = finish(
        (early_feed, early_down),
        ((ff_share, ff_share, share), (ff_share,)),
        peers,
        (
            hidden_in.reshape(count, width), attn_gain.reshape(1, width),
            query_grads.reshape(2, count, group_width), latent_grads.reshape(2, count, latent_size),
            joined.reshape(2, count, latent_size),
            query_weight, latent_weight, grad_resid, ffn_gain_part, key_part, value_part,
        ),
    )
    (
        gate_share, up_share, output_share, down_share, query_share, latent_share, key_share, value_share, gains,
    ) = lay_out(full, (ff_share, ff_share, share, ff_share), share, latent_size, group_width, peers, width)
    gains = lax.dynamic_slice_in_dim(gains, (place * share) % gains.shape[1], share, 1)
    return (
        hidden_out.reshape(rows, tokens, width),
        hidden_grad.reshape(rows, tokens, width),
        gains[0],
        query_share,
        latent_share,
        key_share,
        value_share,
        output_share,
        gains[1],
        gate_share.T,
        up_share.T,
        down_share,
    )


def solution(mesh):
    placed = (
        P("rows", "heads", None),
        P("rows", None),
        P("rows", "heads", None),
        P(),
        P(),
        P(),
        P(),
        P(),
        P(),
        P(),
        P(),
        P(),
        P(),
    )
    return jax.shard_map(
        shards,
        mesh=mesh,
        in_specs=placed,
        out_specs=(
            P("rows", "heads", None),
            P("rows", "heads", None),
            P("heads"),
            P("heads", None),
            P("heads", None),
            P(None, "heads", None),
            P(None, "heads", None),
            P("heads", None),
            P("heads"),
            P(None, "heads"),
            P(None, "heads"),
            P("heads", None),
        ),
        check_vma=False,
    )
```

```python
import functools
import math

import jax
import jax.numpy as jnp
from jax import lax
from jax.experimental import pallas as pl
from jax.experimental.pallas import tpu as pltpu
from jax.sharding import PartitionSpec as P

HEAD_WIDTH = 64
epsilon = 1e-05
blocked = -1e30
LOG2E = math.log2(math.e)
LN2 = math.log(2.0)
QUAD = 4
f32 = jnp.float32
bf16 = jnp.bfloat16


def matmul(left, right):
    return jnp.dot(left, right, preferred_element_type=f32)


def matmul_nt(left, right):
    return lax.dot_general(
        left, right, (((left.ndim - 1,), (right.ndim - 1,)), ((), ())), preferred_element_type=f32
    )


def matmul_tn(left, right):
    return lax.dot_general(left, right, (((0,), (0,)), ((), ())), preferred_element_type=f32)


def rms_inverse(value_matrix):
    return lax.rsqrt(jnp.mean(value_matrix * value_matrix, axis=-1, keepdims=True) + epsilon)


def expand_heads(source, weights, factor, out_ref):
    tokens = source.shape[0]
    quads, wide, deep = weights.shape
    latent = wide // QUAD
    for quad in range(quads):
        product = matmul_nt(weights[quad], source[:, quad * deep : (quad + 1) * deep])
        if factor != 1.0:
            product = product * factor
        product = product.astype(bf16)
        for h in range(QUAD):
            at = (quad * QUAD + h) * tokens
            out_ref[:, at : at + tokens] = product[h * latent : (h + 1) * latent]


def lift_heads(source, weights, tokens):
    parts = [
        matmul(weights[h], source[:, h * tokens : (h + 1) * tokens]) for h in range(weights.shape[0])
    ]
    return jnp.concatenate(parts, axis=0)


def lift_grad(left, right, tokens, out_ref):
    latent = left.shape[0]
    deep = QUAD * HEAD_WIDTH
    head = lax.broadcasted_iota(jnp.int32, (latent, deep), 1) // HEAD_WIDTH
    for quad in range(right.shape[1] // deep):
        columns = slice(quad * deep, (quad + 1) * deep)
        found = None
        for h in range(QUAD):
            at = (quad * QUAD + h) * tokens
            part = matmul(left[:, at : at + tokens], right[:, columns])
            found = part if h == 0 else jnp.where(head == h, part, found)
        out_ref[:, columns] += found


def seg_mask(base, own_base, start):
    tokens = start.shape[-1]
    key_at = lax.broadcasted_iota(jnp.int32, (tokens, tokens), 0)
    query_at = lax.broadcasted_iota(jnp.int32, (tokens, tokens), 1)
    return (key_at >= start - base) & (key_at <= query_at + (own_base - base))


def attend_kernel(count, first, last, lo, bases, *refs):
    refs = list(refs)
    take = lambda k: [refs.pop(0) for _ in range(k)]
    (start_ref,) = take(1)
    if first:
        query_ref, key_lift_ref = take(2)
    else:
        expanded_ref, top_in, total_in, mix_in = take(4)
    seg_refs = take(count)
    if last:
        (value_lift_ref,) = take(1)
        out_ref, lse_ref, mix_ref = take(3)
    else:
        top_out, total_out, mix_out = take(3)
    if first:
        (expanded_ref,) = take(1)
    top, total, mix, segs = take(4)
    expanded = expanded_ref.at[0]
    tokens = start_ref.shape[2]
    heads = expanded.shape[1] // tokens
    row = pl.program_id(0)
    touched = lambda i: (bases[i] >= 0) & (bases[i] + tokens - 1 >= lo[row])
    if first:
        expand_heads(query_ref[0], key_lift_ref, HEAD_WIDTH ** (-0.5) * LOG2E, expanded)
        top[...] = jnp.full_like(top, blocked)
        total[...] = jnp.zeros_like(total)
        mix[...] = jnp.zeros_like(mix)
    else:
        top[...] = top_in[0]
        total[...] = total_in[0]
        mix[...] = mix_in[0].astype(f32)
    for i in range(count):
        segs[i] = seg_refs[i][0]

    @pl.loop(0, count)
    def _(i):
        @pl.when(touched(i))
        def _():
            latent = segs[i]
            latent_t = latent.T
            allow = seg_mask(bases[i], bases[count], start_ref[0])
            for h in range(heads):
                at = slice(h * tokens, (h + 1) * tokens)
                score = jnp.where(allow, matmul(latent, expanded[:, at]), blocked)
                old = top[:, at]
                new = jnp.maximum(old, jnp.max(score, axis=0, keepdims=True))
                probs = jnp.exp2(score - new)
                fade = jnp.exp2(old - new)
                top[:, at] = new
                total[:, at] = total[:, at] * fade + jnp.sum(probs, axis=0, keepdims=True)
                mix[:, at] = mix[:, at] * fade + matmul(latent_t, probs.astype(bf16))

    if not last:
        top_out[0] = top[...]
        total_out[0] = total[...]
        mix_out[0] = mix[...].astype(bf16)
        return
    lse_ref[0] = top[...] + jnp.log2(total[...])
    mix_ref[0] = (mix[...] * (1.0 / total[...])).astype(bf16)
    out_ref[0] = lift_heads(mix_ref[0], value_lift_ref, tokens).T.astype(bf16)


def whole(array):
    return pl.BlockSpec(array.shape, lambda *_: (0,) * len(array.shape))


def by_row(shape):
    return pl.BlockSpec((1,) + tuple(shape[1:]), lambda r, *_: (r,) + (0,) * (len(shape) - 1))


def attend_part(queries, start, key_lift, value_lift_t, lo, segs, bases, expanded, state, last):
    rows, tokens, width = queries.shape
    heads = width // HEAD_WIDTH
    latent = segs[0].shape[-1]
    shape = jax.ShapeDtypeStruct
    stat = shape((rows, 1, heads * tokens), f32)
    flat = shape((rows, latent, heads * tokens), bf16)
    if state is None:
        args = [start, queries, key_lift, *segs]
        specs = [by_row(start.shape), by_row(queries.shape), whole(key_lift)]
    else:
        args = [start, expanded, *state, *segs]
        specs = [by_row(a.shape) for a in args[:5]]
    specs += [by_row(s.shape) for s in segs]
    if last:
        args.append(value_lift_t)
        specs.append(whole(value_lift_t))
        outs = [shape(queries.shape, bf16), stat, flat]
    else:
        outs = [stat, stat, flat]
    if state is None:
        outs.append(flat)
    blocks = rows * heads * len(segs)
    return pl.pallas_call(
        functools.partial(attend_kernel, len(segs), state is None, last),
        out_shape=outs,
        grid_spec=pltpu.PrefetchScalarGridSpec(
            num_scalar_prefetch=2,
            grid=(rows,),
            in_specs=specs,
            out_specs=[by_row(o.shape) for o in outs],
            scratch_shapes=[
                pltpu.VMEM((1, heads * tokens), f32),
                pltpu.VMEM((1, heads * tokens), f32),
                pltpu.VMEM((latent, heads * tokens), f32),
                pltpu.VMEM((len(segs), tokens, latent), bf16),
            ],
        ),
        compiler_params=pltpu.CompilerParams(
            dimension_semantics=("arbitrary",), vmem_limit_bytes=48 << 20
        ),
        cost_estimate=pl.CostEstimate(
            flops=blocks * tokens * tokens * latent * 64,
            bytes_accessed=rows * heads * latent * tokens * 64,
            transcendentals=blocks * tokens * tokens,
        ),
        name="attend",
    )(lo, bases, *args)


def attend_back_kernel(count, first, last, lo, bases, *refs):
    refs = list(refs)
    take = lambda k: [refs.pop(0) for _ in range(k)]
    query_ref, lse_ref, start_ref, expanded_ref, key_lift_t_ref = take(5)
    seg_refs = take(count)
    if first:
        grad_mine, grad_got, mix_ref, value_lift_ref = take(4)
    else:
        expanded_grad_ref, delta_ref, query_back_in, key_up_in = take(4)
    grad_refs = take(count)
    query_back_ref, key_up_ref = take(2)
    if first:
        expanded_grad_ref, delta_ref, value_up_ref = take(3)
    back, query_back, segs, seg_grads = take(4)
    expanded, expanded_grad = expanded_ref.at[0], expanded_grad_ref.at[0]
    tokens = query_ref.shape[1]
    heads = expanded.shape[1] // tokens
    row = pl.program_id(0)
    scale = HEAD_WIDTH ** (-0.5)
    touched = lambda i: (bases[i] >= 0) & (bases[i] + tokens - 1 >= lo[row])
    any_touched = functools.reduce(jnp.logical_or, [touched(i) for i in range(count)])

    @pl.when(row == 0)
    def _():
        key_up_ref[...] = jnp.zeros_like(key_up_ref) if first else key_up_in[...]
        if first:
            value_up_ref[...] = jnp.zeros_like(value_up_ref)

    query_back[...] = jnp.zeros_like(query_back) if first else query_back_in[0]
    seg_grads[...] = jnp.zeros_like(seg_grads)
    if first:
        grads = jnp.where(row < pl.num_programs(0) // 2, grad_mine[0], grad_got[0])
        expand_heads(grads, value_lift_ref, 1.0, expanded_grad)
        delta_ref[0] = jnp.sum(mix_ref[0].astype(f32) * expanded_grad[...].astype(f32), axis=0, keepdims=True)
        lift_grad(mix_ref[0], grads, tokens, value_up_ref)

    @pl.when(any_touched)
    def _():
        back[...] = jnp.zeros_like(back)
        for i in range(count):
            segs[i] = seg_refs[i][0]

    @pl.loop(0, count)
    def _(i):
        @pl.when(touched(i))
        def _():
            latent = segs[i]
            allow = seg_mask(bases[i], bases[count], start_ref[0])
            allow = jnp.concatenate([allow] * heads, axis=1)
            score = matmul(latent, expanded[...])
            probs = jnp.where(allow, jnp.exp2(score - lse_ref[0]), 0.0)
            dprobs = matmul(latent, expanded_grad[...])
            dscore = (probs * (dprobs - delta_ref[0])).astype(bf16)
            by_key = matmul_nt(dscore, expanded[...])
            by_value = matmul_nt(probs.astype(bf16), expanded_grad[...])
            seg_grads[i] = (by_key * LN2 + by_value).astype(bf16)
            back[...] += matmul(latent.T, dscore)

    for i in range(count):
        grad_refs[i][0] = seg_grads[i]

    @pl.when(any_touched)
    def _():
        part = (back[...] * scale).astype(bf16)
        query_back[...] += lift_heads(part, key_lift_t_ref, tokens)
        lift_grad(part, query_ref[0], tokens, key_up_ref)

    if last:
        query_back_ref[0] = query_back[...].T.astype(bf16)
    else:
        query_back_ref[0] = query_back[...]


def attend_back_part(queries, grads, lse, mix, start, expanded, value_lift, key_lift_t, lo, segs, bases, kept, state, last):
    rows, tokens, width = queries.shape
    heads = width // HEAD_WIDTH
    latent = segs[0].shape[-1]
    shape = jax.ShapeDtypeStruct
    back_shape = shape((rows, width, tokens), f32)
    up_shape = shape((latent, width), f32)
    first = state is None
    args = [queries, lse, start, expanded, key_lift_t, *segs]
    specs = [by_row(a.shape) for a in args[:4]] + [whole(key_lift_t)]
    specs += [by_row(s.shape) for s in segs]
    if first:
        args += [*grads, mix, value_lift]
        half = (1, tokens, width)
        specs.append(pl.BlockSpec(half, lambda r, *_: (jnp.minimum(r, rows // 2 - 1), 0, 0)))
        specs.append(pl.BlockSpec(half, lambda r, *_: (jnp.maximum(r - rows // 2, 0), 0, 0)))
        specs += [by_row(mix.shape), whole(value_lift)]
    else:
        args += [*kept, *state]
        specs += [by_row(kept[0].shape), by_row(kept[1].shape), by_row(back_shape.shape), whole(up_shape)]
    outs = [shape(s.shape, bf16) for s in segs]
    outs += [shape(queries.shape, bf16) if last else back_shape, up_shape]
    out_specs = [by_row(o.shape) for o in outs[:-1]] + [whole(up_shape)]
    if first:
        outs += [shape(expanded.shape, bf16), shape(lse.shape, f32), up_shape]
        out_specs += [by_row(expanded.shape), by_row(lse.shape), whole(up_shape)]
    blocks = rows * heads * len(segs)
    return pl.pallas_call(
        functools.partial(attend_back_kernel, len(segs), first, last),
        out_shape=outs,
        grid_spec=pltpu.PrefetchScalarGridSpec(
            num_scalar_prefetch=2,
            grid=(rows,),
            in_specs=specs,
            out_specs=out_specs,
            scratch_shapes=[
                pltpu.VMEM((latent, heads * tokens), f32),
                pltpu.VMEM((width, tokens), f32),
                pltpu.VMEM((len(segs), tokens, latent), bf16),
                pltpu.VMEM((len(segs), tokens, latent), bf16),
            ],
        ),
        compiler_params=pltpu.CompilerParams(
            dimension_semantics=("arbitrary",), vmem_limit_bytes=48 << 20
        ),
        cost_estimate=pl.CostEstimate(
            flops=blocks * tokens * tokens * latent,
            bytes_accessed=rows * heads * latent * tokens,
            transcendentals=0,
        ),
        name="attend_back",
    )(lo, bases, *args)


def quad_lift(lift):
    latent, width = lift.shape
    deep = QUAD * HEAD_WIDTH
    quads = width // deep
    tall = jnp.tile(lift.reshape(latent, quads, deep).transpose(1, 0, 2), (1, QUAD, 1))
    row_head = lax.broadcasted_iota(jnp.int32, tall.shape, 1) // latent
    column_head = lax.broadcasted_iota(jnp.int32, tall.shape, 2) // HEAD_WIDTH
    return jnp.where(row_head == column_head, tall, jnp.zeros_like(tall))


def head_lift(lift):
    latent, width = lift.shape
    return lift.T.reshape(width // HEAD_WIDTH, HEAD_WIDTH, latent)


def put_pieces(ref, value, at=0):
    pieces, _, piece = ref.shape
    for j in range(pieces):
        ref[j, pl.ds(at, value.shape[0])] = value[:, j * piece : (j + 1) * piece].astype(bf16)


def feed_kernel(core_ref, *refs):
    (
        inputs_ref, mine_ref, got_ref, output_ref, gain_ref, cotangent_ref, keep_ref,
        gate_ref, up_ref, down_ref,
        hidden_out_ref, resid_out, normed_out, back_out, active_ref, slope_ref, down_grad_ref,
        result, hidden, resid, normed, back, sems,
    ) = refs
    step = pl.program_id(0)
    leaving = [
        pltpu.make_async_copy(source, target, sems.at[i])
        for i, (source, target) in enumerate(((resid, resid_out), (normed, normed_out), (back, back_out)))
    ]
    count = inputs_ref.shape[0]
    block = min(256, count)
    core = core_ref[0]

    @pl.when(step == 0)
    def _():
        for t in range(0, count, block):
            at = slice(t, t + block)
            row = inputs_ref[at].astype(f32) + (
                matmul(mine_ref[at], output_ref[core]) + matmul(got_ref[at], output_ref[1 - core])
            )
            resid[at] = row
            scale = lax.rsqrt(jnp.mean(row * row, axis=-1, keepdims=True) + epsilon)
            normed[at] = (row * scale * gain_ref[...]).astype(bf16)
            back[at] = (cotangent_ref[at].astype(f32) * keep_ref[at]).astype(bf16)
        for copy in leaving:
            copy.start()
        result[...] = jnp.zeros_like(result)

    part = count // 4
    for t in range(0, count, part):
        at = slice(t, t + part)
        gate = matmul(normed[at], gate_ref[...])
        up = matmul(normed[at], up_ref[...])
        sigmoid = 1.0 / (1.0 + jnp.exp(-gate))
        active = gate * sigmoid
        hidden[at] = (active * up).astype(bf16)
        active_ref[at] = active.astype(bf16)
        slope_ref[at] = (up * (sigmoid * (1.0 + gate * (1.0 - sigmoid)))).astype(bf16)
    put_pieces(down_grad_ref, matmul_tn(hidden[...], back[...]))
    result[...] += matmul(hidden[...], down_ref[...])

    @pl.when(step == pl.num_programs(0) - 1)
    def _():
        hidden_out_ref[...] = (resid[...] + result[...]).astype(bf16)
        for copy in leaving:
            copy.wait()


def feed_back_kernel(core_ref, *refs):
    (
        mine_in, got_in, output_in, resid_in, gain_ref, normed, back,
        active_ref, slope_ref, gate_ref, up_ref, down_ref,
        grad_resid_out, head_mine_out, head_sent_out, gain_grad_ref, grads_ref,
        grad_two, both, low, staged, staged_out, mine_ref, got_ref, output_ref, resid_ref, head_mine_ref, head_sent_ref,
        sems, out_sem, in_sems, leave_sems,
    ) = refs
    step = pl.program_id(0)
    steps = pl.num_programs(0)
    count, width = resid_ref.shape
    coming = [
        pltpu.make_async_copy(source, target, in_sems.at[i])
        for i, (source, target) in enumerate(
            ((mine_in, mine_ref), (got_in, got_ref), (output_in, output_ref), (resid_in, resid_ref))
        )
    ]
    chunk = down_ref.shape[0]
    ff = (grads_ref.shape[1] - width) // 2
    block = min(256, count)
    core = core_ref[0]
    slot = step % 2

    def leave(at, kind, place):
        return pltpu.make_async_copy(
            staged.at[at, kind],
            grads_ref.at[:, pl.ds(pl.multiple_of(kind * ff + place * chunk, chunk), chunk)],
            sems.at[at, kind],
        )

    @pl.when(step >= 2)
    def _():
        for kind in range(2):
            leave(slot, kind, step - 2).wait()

    @pl.when(step == 0)
    def _():
        for copy in coming:
            copy.start()
        grad_two[...] = jnp.zeros_like(grad_two)

    part = count // 4
    for t in range(0, count, part):
        at = slice(t, t + part)
        grad_act = matmul_nt(back[at], down_ref[...])
        both[at, :chunk] = (grad_act * slope_ref[at].astype(f32)).astype(bf16)
        both[at, chunk:] = (grad_act * active_ref[at].astype(f32)).astype(bf16)
    for kind in range(2):
        put_pieces(staged.at[slot, kind], matmul_tn(both[:, kind * chunk : (kind + 1) * chunk], normed[...]))
        leave(slot, kind, step).start()
    weights = jnp.concatenate([gate_ref[...], up_ref[...]], axis=1)
    for t in range(0, count, part):
        at = slice(t, t + part)
        grad_two[at] += matmul_nt(both[at], weights)

    @pl.when(step == steps - 1)
    def _():
        for copy in coming:
            copy.wait()
        gain_total = jnp.zeros((1, width), f32)
        leaving = []
        for t in range(0, count, block):
            at = slice(t, t + block)
            row = resid_ref[at]
            scale = lax.rsqrt(jnp.mean(row * row, axis=-1, keepdims=True) + epsilon)
            unit = row * scale
            grad = grad_two[at]
            gain_total += jnp.sum(grad * unit, axis=0, keepdims=True)
            scaled = grad * gain_ref[...]
            grad = back[at].astype(f32) + scale * (
                scaled - unit * jnp.mean(scaled * unit, axis=-1, keepdims=True)
            )
            grad_two[at] = grad
            low[at] = grad.astype(bf16)
            head_mine_ref[at] = matmul_nt(low[at], output_ref[core]).astype(bf16)
            head_sent_ref[at] = matmul_nt(low[at], output_ref[1 - core]).astype(bf16)
            for i, (source, target) in enumerate(
                ((grad_two, grad_resid_out), (head_mine_ref, head_mine_out), (head_sent_ref, head_sent_out))
            ):
                rows = pl.ds(t, block)
                copy = pltpu.make_async_copy(source.at[rows], target.at[rows], leave_sems.at[t // block, i])
                copy.start()
                leaving.append(copy)
        gain_grad_ref[...] = gain_total
        half = mine_ref.shape[1]
        put_pieces(staged_out, matmul_tn(mine_ref[...], low[...]), core * half)
        put_pieces(staged_out, matmul_tn(got_ref[...], low[...]), (1 - core) * half)
        last = pltpu.make_async_copy(staged_out, grads_ref.at[:, pl.ds(2 * ff, width)], out_sem)
        last.start()
        for kind in range(2):
            leave(1 - slot, kind, step - 1).wait()
            leave(slot, kind, step).wait()
        last.wait()
        for copy in leaving:
            copy.wait()


def once(array):
    return pl.BlockSpec(array.shape, lambda *_: (0,) * len(array.shape), pipeline_mode=pl.Buffered(1))


def feed(core, inputs, mixed_mine, mixed_got, output_weight, gain, cotangent, keep, weights, pieces):
    count, width = inputs.shape
    gate_weight, up_weight, down_weight = weights
    ff = gate_weight.shape[1]
    chunk = 256
    piece = width // pieces
    output_weight = output_weight.reshape(2, -1, width)
    gain = gain.reshape(1, width)
    by_rows = pl.BlockSpec((chunk, width), lambda c, *_: (c, 0))
    by_columns = pl.BlockSpec((width, chunk), lambda c, *_: (0, c))
    kept_columns = pl.BlockSpec((count, chunk), lambda c, *_: (0, c))
    shape = jax.ShapeDtypeStruct
    params = pltpu.CompilerParams(dimension_semantics=("arbitrary",), vmem_limit_bytes=60 << 20)
    full_bf, full_f = shape((count, width), bf16), shape((count, width), f32)
    kept = shape((count, ff), bf16)
    firsts = [inputs, mixed_mine, mixed_got, output_weight, gain, cotangent, keep]
    outs = [full_bf, full_f, full_bf, full_bf, kept, kept, shape((pieces, ff, piece), bf16)]
    hidden_out, resid, normed, back, active, slope, down_grad = pl.pallas_call(
        feed_kernel,
        out_shape=outs,
        grid_spec=pltpu.PrefetchScalarGridSpec(
            num_scalar_prefetch=1,
            grid=(ff // chunk,),
            in_specs=[once(a) for a in firsts] + [by_columns, by_columns, by_rows],
            out_specs=[once(outs[0])]
            + [pl.BlockSpec(memory_space=pl.ANY)] * 3
            + [kept_columns, kept_columns, pl.BlockSpec((pieces, chunk, piece), lambda c, *_: (0, c, 0))],
            scratch_shapes=[
                pltpu.VMEM((count, width), f32),
                pltpu.VMEM((count, chunk), bf16),
                pltpu.VMEM((count, width), f32),
                pltpu.VMEM((count, width), bf16),
                pltpu.VMEM((count, width), bf16),
                pltpu.SemaphoreType.DMA((3,)),
            ],
        ),
        compiler_params=params,
        cost_estimate=pl.CostEstimate(
            flops=count * width * (ff * 8 + width * 2),
            bytes_accessed=width * ff * 8 + count * width * 16 + count * ff * 4,
            transcendentals=count * ff,
        ),
        name="feed",
    )(core.reshape(1), *firsts, *weights)
    firsts = [mixed_mine, mixed_got, output_weight, resid, gain, normed, back]
    anywhere = pl.BlockSpec(memory_space=pl.ANY)
    outs = [
        full_f,
        shape(mixed_mine.shape, bf16),
        shape(mixed_mine.shape, bf16),
        shape((1, width), f32),
        shape((pieces, 2 * ff + width, piece), bf16),
    ]
    grad_resid, head_mine, head_sent, gain_grad, grads = pl.pallas_call(
        feed_back_kernel,
        out_shape=outs,
        grid_spec=pltpu.PrefetchScalarGridSpec(
            num_scalar_prefetch=1,
            grid=(ff // chunk,),
            in_specs=[anywhere] * 4
            + [once(a) for a in firsts[4:]]
            + [kept_columns, kept_columns, by_columns, by_columns, by_rows],
            out_specs=[anywhere] * 3 + [once(outs[3]), anywhere],
            scratch_shapes=[
                pltpu.VMEM((count, width), f32),
                pltpu.VMEM((count, 2 * chunk), bf16),
                pltpu.VMEM((count, width), bf16),
                pltpu.VMEM((2, 2, pieces, chunk, piece), bf16),
                pltpu.VMEM((pieces, width, piece), bf16),
                pltpu.VMEM(mixed_mine.shape, bf16),
                pltpu.VMEM(mixed_mine.shape, bf16),
                pltpu.VMEM(output_weight.shape, bf16),
                pltpu.VMEM((count, width), f32),
                pltpu.VMEM(mixed_mine.shape, bf16),
                pltpu.VMEM(mixed_mine.shape, bf16),
                pltpu.SemaphoreType.DMA((2, 2)),
                pltpu.SemaphoreType.DMA,
                pltpu.SemaphoreType.DMA((4,)),
                pltpu.SemaphoreType.DMA((max(1, count // 256), 3)),
            ],
        ),
        compiler_params=params,
        cost_estimate=pl.CostEstimate(
            flops=count * width * (ff * 10 + width * 4),
            bytes_accessed=width * ff * 10 + count * width * 20 + count * ff * 4,
            transcendentals=0,
        ),
        name="feed_back",
    )(core.reshape(1), *firsts, active, slope, *weights)
    return hidden_out, grad_resid, head_mine, head_sent, gain_grad, down_grad, grads


def flip(array, axis, bit):
    size = lax.axis_size(axis)
    return lax.ppermute(array, axis, [(i, i ^ (1 << bit)) for i in range(size)])


def fill_shards(target, at, grad, count):
    along, piece = target.shape[0], target.shape[3]
    size = grad.shape[0] // count
    for s in range(count):
        for j in range(along):
            target[j, s, at : at + size] = grad[s * size : (s + 1) * size, j * piece : (j + 1) * piece].astype(bf16)


def fill_folded(target, at, grad, count):
    along, piece = target.shape[0], target.shape[3]
    size = grad.shape[0] // count
    latent = grad.shape[1]
    fold = size // 2
    for s in range(count):
        for j in range(along):
            side, column = divmod(j * piece, latent)
            first = s * size + side * fold
            target[j, s, at : at + fold] = grad[first : first + fold, column : column + piece].astype(bf16)


def fill_gains(target, at, gain, count):
    along, piece = target.shape[0], target.shape[3]
    share = gain.shape[1] // count
    lane = max(share, 128)
    for s in range(count):
        begin = s * share // lane * lane
        kept = jnp.broadcast_to(gain[:, begin : begin + lane], (16, lane)).astype(bf16)
        target[0, s, at : at + 16, :lane] = kept
        if piece > lane:
            target[0, s, at : at + 16, lane:] = jnp.zeros((16, piece - lane), bf16)
        for j in range(1, along):
            target[j, s, at : at + 16] = jnp.zeros((16, piece), bf16)


def finish_kernel(sections, groups, sizes, refs):
    (
        early_refs, inputs_ref, gain_ref, query_grad_ref, latent_grad_ref, joined_ref,
        query_ref, latent_ref, resid_ref, other_gain_ref, key_up, value_up,
        out_ref, grad_ref,
        normed, own_ref, sent_ref, late_got, late_from, got_first, got_next,
        chain_got, query_got, latent_low, latent_got,
        chain_sems, core_sems, along_sems, first_sems, first_late_sems, next_sems, out_sems,
    ) = refs
    along, count, late_rows, piece = own_ref.shape
    early_rows, share, fold, lift = sizes
    bits = count.bit_length() - 1
    row_at = lax.axis_index("rows")
    place = lax.axis_index("heads")
    core = row_at % 2
    x_at = row_at // 2
    mesh = pl.DeviceIdType.MESH
    tokens, width = inputs_ref.shape
    latent = latent_low.shape[2]
    half = query_got.shape[1]
    block = min(256, tokens)
    parts = [slice(0, early_rows)] + [slice(early_rows + g[0], early_rows + g[1]) for g in groups]

    def turned(which):
        at = place
        for bit in which:
            at = at + (1 << bit) * (1 - 2 * ((place // (1 << bit)) % 2))
        return at

    core_peer = (row_at + 1 - 2 * core, place)
    x_others = [(x_at + d) % along for d in range(1, along)]
    x_peers = [(x * 2 + core, place) for x in x_others]
    head_peers = [(row_at, turned([bit])) for bit in range(bits)]
    above = (row_at, (place + 2) % count)
    below = (row_at, (place + count - 2) % count)
    barrier = pltpu.get_barrier_semaphore()
    everyone = [core_peer, above, below] + x_peers + head_peers
    for peer in everyone:
        pl.semaphore_signal(barrier, inc=1, device_id=peer, device_id_type=mesh)
    pl.semaphore_wait(barrier, len(everyone))

    def remote(source, target, sems, index, peer):
        return pltpu.make_async_remote_copy(
            src_ref=source, dst_ref=target, send_sem=sems.at[(0,) + index], recv_sem=sems.at[(1,) + index],
            device_id=peer, device_id_type=mesh,
        )

    def orders(bit):
        rest = list(range(bit + 1, bits))
        return [
            [b for i, b in enumerate(rest) if not (mask >> (len(rest) - 1 - i)) & 1]
            for mask in range(1 << len(rest))
        ]

    def add_rows(target, other, size):
        step = size if size <= 600 else size // 2

        def one(i, carry):
            at = pl.ds(pl.multiple_of(i * step, 16), step)
            target[at] = (target[at].astype(f32) + other[at].astype(f32)).astype(bf16)
            return carry

        lax.fori_loop(0, size // step, one, 0)

    def rows_of(part):
        return pl.ds(part.start, part.stop - part.start)

    first = orders(0)
    final = len(first) - 1
    pending = []

    def early_rows_of(n, shard):
        which, start, size, _ = sections[n]
        return early_refs[which].at[pl.ds(pl.multiple_of(start + shard * size, 16), size)]

    def first_early(i, n):
        _, _, size, row = sections[n]
        return remote(
            early_rows_of(n, turned([0] + first[i])), got_first.at[i, pl.ds(row, size)],
            first_sems, (i, n), head_peers[0],
        )

    def next_copy(bit, j, i, which):
        rows = rows_of(parts[which])
        return remote(
            got_first.at[i, rows], got_next[bit - 1].at[j, rows], next_sems[bit - 1], (j, which), head_peers[bit]
        )

    def settle(i, which):
        rest = first[i]
        level = rest[0] if rest else bits
        rows = rows_of(parts[which])
        for bit in range(1, level):
            j = orders(bit).index(rest)
            next_copy(bit, j, i, which).wait_recv()
            add_rows(got_first.at[i, rows], got_next[bit - 1].at[j, rows], rows.size)
        if rest:
            copy = next_copy(level, orders(level).index(rest[1:]), i, which)
            copy.start()
            pending.append(copy)

    def early_step(i):
        for n, (_, _, size, row) in enumerate(sections):
            first_early(i, n).wait()
            add_rows(got_first.at[i, pl.ds(row, size)], early_rows_of(n, turned(first[i])), size)
        settle(i, 0)

    def core_copy(g):
        _, _, begin, end = groups[g]
        rows = pl.ds(begin, end - begin)
        return remote(sent_ref.at[:, :, rows], late_got.at[:, :, rows], core_sems, (g,), core_peer)

    def x_copies(g):
        low, high, begin, end = groups[g]
        shared = end - begin
        copies = []
        for d, (x, peer) in enumerate(zip(x_others, x_peers)):
            copies.append(
                remote(
                    late_got.at[x, :, pl.ds(begin, shared)], late_from.at[d, :, pl.ds(low, shared)],
                    along_sems, (d, g, 0), peer,
                )
            )
            if low + shared < high:
                rows = pl.ds(low + shared, high - low - shared)
                copies.append(
                    remote(own_ref.at[x, :, rows], late_from.at[d, :, rows], along_sems, (d, g, 1), peer)
                )
        return copies

    def along_x(g):
        low, _, begin, end = groups[g]
        core_copy(g).wait()

        def core_add(i, carry):
            j, s = i // count, i % count
            mine = own_ref[j, s, low : low + end - begin].astype(f32)
            late_got[j, s, begin:end] = (mine + late_got[j, s, begin:end].astype(f32)).astype(bf16)
            return carry

        lax.fori_loop(0, along * count, core_add, 0)
        for copy in x_copies(g):
            copy.start()

    def first_late(i, g):
        low, high, _, _ = groups[g]
        return remote(
            late_from.at[0, turned([0] + first[i]), pl.ds(low, high - low)],
            got_first.at[i, rows_of(parts[1 + g])], first_late_sems, (i, g), head_peers[0],
        )

    def over_heads(g):
        low, high, begin, end = groups[g]
        middle = low + end - begin
        for copy in x_copies(g):
            copy.wait()

        def x_add(s, carry):
            total = late_got[x_at, s, begin:end].astype(f32)
            for d in range(along - 1):
                total = total + late_from[d, s, low:middle].astype(f32)
            late_from[0, s, low:middle] = total.astype(bf16)
            if middle < high:
                total = own_ref[x_at, s, middle:high].astype(f32)
                for d in range(along - 1):
                    total = total + late_from[d, s, middle:high].astype(f32)
                late_from[0, s, middle:high] = total.astype(bf16)
            return carry

        lax.fori_loop(0, count, x_add, 0)
        for i in range(len(first)):
            first_late(i, g).start()

    def late_step(i, g):
        low, high, _, _ = groups[g]
        first_late(i, g).wait()
        add_rows(
            got_first.at[i, rows_of(parts[1 + g])],
            late_from.at[0, turned(first[i]), pl.ds(low, high - low)],
            high - low,
        )
        settle(i, 1 + g)

    mine = lambda ref, size: ref[:, pl.ds(pl.multiple_of(core * size, size), size)]
    theirs = lambda ref, size: ref[:, pl.ds(pl.multiple_of((1 - core) * size, size), size)]
    chain_copy = remote(joined_ref, chain_got, chain_sems, (0,), below)
    chain_copy.start()
    query_copy = remote(query_grad_ref.at[1], query_got, chain_sems, (1,), core_peer)
    query_copy.start()
    for i in range(len(first)):
        for n in range(len(sections)):
            first_early(i, n).start()

    @pl.loop(0, tokens // block)
    def _(t):
        at = pl.ds(pl.multiple_of(t * block, block), block)
        row = inputs_ref[at].astype(f32)
        scale = lax.rsqrt(jnp.mean(row * row, axis=-1, keepdims=True) + epsilon)
        normed[at] = (row * scale * gain_ref[...]).astype(bf16)

    fill_shards(own_ref, 0, matmul_tn(normed[...], query_grad_ref[0]), count)
    fill_shards(own_ref, share, key_up[...], count)
    fill_shards(own_ref, share + lift, value_up[...], count)
    query_copy.wait()
    fill_shards(sent_ref, 0, matmul_tn(normed[...], query_got[...]), count)
    core_copy(0).start()
    early_step(0)
    along_x(0)
    for i in range(1, len(first) // 2):
        early_step(i)

    chain_copy.wait()
    for side in (1, 0):
        for t in range(0, tokens, block):
            at = slice(t, t + block)
            latent_low[side, at] = (latent_grad_ref[side, at] + chain_got[side, at].astype(f32)).astype(bf16)
        if side == 1:
            latent_copy = remote(latent_low.at[1], latent_got, chain_sems, (2,), core_peer)
            latent_copy.start()
    latent_copy.wait()

    def back(t, gain_total):
        at = pl.ds(pl.multiple_of(t * block, block), block)
        row = inputs_ref[at].astype(f32)
        scale = lax.rsqrt(jnp.mean(row * row, axis=-1, keepdims=True) + epsilon)
        unit = row * scale
        grad = (
            matmul_nt(query_grad_ref[0, at], mine(query_ref, half))
            + matmul_nt(query_got[at], theirs(query_ref, half))
            + matmul_nt(latent_low[0, at], mine(latent_ref, latent))
            + matmul_nt(latent_got[at], theirs(latent_ref, latent))
        )
        scaled = grad * gain_ref[...]
        grad_ref[at] = resid_ref[at] + scale * (
            scaled - unit * jnp.mean(scaled * unit, axis=-1, keepdims=True)
        )
        return gain_total + jnp.sum(grad * unit, axis=0, keepdims=True)

    gain_total = lax.fori_loop(0, tokens // block, back, jnp.zeros((1, width), f32))
    other = other_gain_ref[...]
    low = groups[1][0]
    for target, at, latents, gain in (
        (own_ref, low, latent_low[0], jnp.where(core == 0, gain_total, other)),
        (sent_ref, groups[1][2], latent_got[...], jnp.where(core == 0, other, gain_total)),
    ):
        fill_folded(target, at, matmul_tn(normed[...], latents), count)
        fill_gains(target, at + fold, gain, count)
    core_copy(1).start()
    over_heads(0)
    along_x(1)
    for i in range(max(1, len(first) // 2), final):
        early_step(i)
    over_heads(1)
    for i in range(final):
        for g in range(len(groups)):
            late_step(i, g)

    def spread(which):
        rows = rows_of(parts[which])
        out_ref[row_at, rows] = got_first[final, rows]
        copies = [remote(out_ref.at[row_at, rows], out_ref.at[row_at, rows], out_sems, (which, 0), core_peer)]
        for d, peer in enumerate(x_peers):
            copies.append(
                remote(out_ref.at[row_at, rows], out_ref.at[row_at, rows], out_sems, (which, 1 + d), peer)
            )
        for copy in copies:
            copy.start()
        return copies

    def pass_on(which, copies):
        rows = rows_of(parts[which])
        more = []
        for d in range(along - 1):
            copies[1 + d].wait_recv()
            source = ((x_at + along - 1 - d) % along) * 2 + core
            more.append(
                remote(
                    out_ref.at[source, rows], out_ref.at[source, rows], out_sems, (which, along + d), core_peer
                )
            )
            more[-1].start()
        return more

    early_step(final)
    spreads = [spread(0)]
    for g in range(len(groups)):
        late_step(final, g)
        spreads.append(spread(1 + g))
    passes = [pass_on(which, copies) for which, copies in enumerate(spreads)]
    for copies, more in zip(spreads, passes):
        copies[0].wait()
        for copy in copies[1:]:
            copy.wait_send()
        for copy in more:
            copy.wait()
    for copy in pending:
        copy.wait_send()


def finish(early, shares, count, late_args):
    inputs, _, query_grads, latent_grads = late_args[:4]
    tokens, width = inputs.shape
    latent = latent_grads.shape[2]
    piece = early[0].shape[1]
    along = width // piece // 2
    share = width // count
    fold, lift = share // 2, latent // count
    bits = count.bit_length() - 1
    groups = [
        (0, share + 2 * lift, 0, share),
        (share + 2 * lift, share + 2 * lift + fold + 16, share, share + fold + 16),
    ]
    late_rows, shared_rows = groups[1][1], groups[1][3]
    sections = []
    row = 0
    for which, of_one in enumerate(shares):
        start = 0
        for size in of_one:
            sections.append((which, start, size, row))
            start += size * count
            row += size
    total = row + late_rows
    vmem = pl.BlockSpec(memory_space=pltpu.VMEM)
    dma = pltpu.SemaphoreType.DMA

    def body(*refs):
        refs = list(refs)
        take = lambda k: [refs.pop(0) for _ in range(k)]
        given = [take(len(early))] + take(len(late_args)) + take(2)
        given += take(6) + [take(bits - 1)] + take(4) + take(5) + [take(bits - 1)] + take(1)
        finish_kernel(sections, groups, (row, share, fold, lift), given)

    return pl.pallas_call(
        body,
        out_shape=[
            jax.ShapeDtypeStruct((2 * along, total, piece), bf16),
            jax.ShapeDtypeStruct((tokens, width), f32),
        ],
        in_specs=[vmem] * (len(early) + len(late_args)),
        out_specs=[vmem] * 2,
        scratch_shapes=[
            pltpu.VMEM((tokens, width), bf16),
            pltpu.VMEM((along, count, late_rows, piece), bf16),
            pltpu.VMEM((along, count, shared_rows, piece), bf16),
            pltpu.VMEM((along, count, shared_rows, piece), bf16),
            pltpu.VMEM((along - 1, count, late_rows, piece), bf16),
            pltpu.VMEM((count // 2, total, piece), bf16),
        ]
        + [pltpu.VMEM((count >> (bit + 1), total, piece), bf16) for bit in range(1, bits)]
        + [
            pltpu.VMEM((2, tokens, latent), bf16),
            pltpu.VMEM(query_grads.shape[1:], bf16),
            pltpu.VMEM((2, tokens, latent), bf16),
            pltpu.VMEM((tokens, latent), bf16),
            dma((2, 3)),
            dma((2, 2)),
            dma((2, along - 1, 2, 2)),
            dma((2, count // 2, len(sections))),
            dma((2, count // 2, 2)),
        ]
        + [dma((2, count >> (bit + 1), 3)) for bit in range(1, bits)]
        + [dma((2, 3, 2 * along))],
        compiler_params=pltpu.CompilerParams(
            collective_id=0, has_side_effects=True, vmem_limit_bytes=60 << 20
        ),
        name="finish",
    )(*early, *late_args)


def lay_out_kernel(
    rows, latent, full_ref, grad_in, gate_ref, up_ref, output_ref, down_ref, query_ref, latent_ref, key_ref, value_ref,
    gains_ref, grad_out, sem,
):
    copy = pltpu.make_async_copy(grad_in, grad_out, sem)
    copy.start()
    pieces, _, piece = full_ref.shape
    at = 0
    for ref, size in zip((gate_ref, up_ref, output_ref, down_ref), rows):
        for j in range(pieces):
            ref[:, j * piece : (j + 1) * piece] = full_ref[j, at : at + size].astype(f32)
        at += size
    share = query_ref.shape[0]
    fold = share // 2
    lift = key_ref.shape[1]
    half = key_ref.shape[2]
    lane = gains_ref.shape[1]
    for j in range(pieces):
        x, core = divmod(j, 2)
        row = at
        query_ref[:, core * half + x * piece : core * half + (x + 1) * piece] = full_ref[
            j, row : row + share
        ].astype(f32)
        row += share
        for ref in (key_ref, value_ref):
            ref[core, :, x * piece : (x + 1) * piece] = full_ref[j, row : row + lift].astype(f32)
            row += lift
        side, column = divmod(x * piece, latent)
        column += core * latent
        latent_ref[side * fold : (side + 1) * fold, column : column + piece] = full_ref[
            j, row : row + fold
        ].astype(f32)
        row += fold
        if x == 0:
            gains_ref[core : core + 1] = full_ref[j, row : row + 16, :lane].astype(f32)[:1]
    copy.wait()


def lay_out(full, grad, rows, share, latent, half, count, width):
    shape = jax.ShapeDtypeStruct
    gate, up, output, down = rows
    lift = latent // count
    vmem = pl.BlockSpec(memory_space=pltpu.VMEM)
    outs = [
        shape((gate, width), f32),
        shape((up, width), f32),
        shape((output, width), f32),
        shape((down, width), f32),
        shape((share, width), f32),
        shape((share, 2 * latent), f32),
        shape((2, lift, half), f32),
        shape((2, lift, half), f32),
        shape((2, max(share, 128)), f32),
        shape(grad.shape, f32),
    ]
    anywhere = pl.BlockSpec(memory_space=pl.ANY)
    return pl.pallas_call(
        functools.partial(lay_out_kernel, rows, latent),
        out_shape=outs,
        in_specs=[vmem] * 2,
        out_specs=[vmem] * (len(outs) - 1) + [anywhere],
        scratch_shapes=[pltpu.SemaphoreType.DMA],
        compiler_params=pltpu.CompilerParams(vmem_limit_bytes=48 << 20),
        name="lay_out",
    )(full, grad)


def shards(
    hidden_in,
    doc_ids,
    cotangent,
    attn_gain,
    query_weight,
    latent_weight,
    key_lift_weight,
    value_lift_weight,
    output_weight,
    ffn_gain,
    gate_weight,
    up_weight,
    down_weight,
):
    rows, tokens, width = hidden_in.shape
    peers = lax.axis_size("heads")
    place = lax.axis_index("heads")
    core = lax.axis_index("rows") & 1
    groups, latent_size, group_width = key_lift_weight.shape
    count = rows * tokens
    steps = peers // 2
    pieces = lax.axis_size("rows")
    share = width // peers
    side = place & 1
    level = place // 2
    swap = lambda a: flip(a, "rows", 0)
    mine = lambda a, axis: lax.dynamic_slice_in_dim(a, core * (a.shape[axis] // 2), a.shape[axis] // 2, axis)
    theirs = lambda a, axis: lax.dynamic_slice_in_dim(
        a, (1 - core) * (a.shape[axis] // 2), a.shape[axis] // 2, axis
    )

    own_base = place * tokens
    own_docs = lax.dynamic_slice_in_dim(doc_ids, own_base, tokens, 1)
    position = own_base + jnp.arange(tokens, dtype=jnp.int32)
    before = (doc_ids[:, None, :] == own_docs[:, :, None]) & (
        jnp.arange(doc_ids.shape[1], dtype=jnp.int32)[None, None, :] <= position[None, :, None]
    )
    own_start = position[None, :] + 1 - jnp.sum(before.astype(jnp.int32), axis=-1)
    start = jnp.concatenate([own_start, swap(own_start)], axis=0)
    lo = start[:, 0]
    start = start[:, None, :]

    inputs = hidden_in.reshape(count, width).astype(f32)
    inverse_one = rms_inverse(inputs)
    normed_one = (inputs * inverse_one * attn_gain).astype(bf16)
    latent_mine = matmul(normed_one, mine(latent_weight, 1)).astype(bf16)
    latent_sent = matmul(normed_one, theirs(latent_weight, 1)).astype(bf16)
    latent_got = swap(latent_sent)
    own_seg = jnp.concatenate([latent_mine, latent_got], axis=0).reshape(2 * rows, tokens, latent_size)
    query_mine = matmul(normed_one, mine(query_weight, 1)).astype(bf16)
    query_sent = matmul(normed_one, theirs(query_weight, 1)).astype(bf16)
    queries = jnp.concatenate([query_mine, swap(query_sent)], axis=0).reshape(2 * rows, tokens, group_width)

    key_mine = lax.dynamic_index_in_dim(key_lift_weight, core, 0, keepdims=False)
    value_mine = lax.dynamic_index_in_dim(value_lift_weight, core, 0, keepdims=False)
    key_lift = quad_lift(key_mine)
    value_lift = quad_lift(value_mine)
    key_lift_t = head_lift(key_mine)
    value_lift_t = head_lift(value_mine)

    up_chain = [(i, i + 2) for i in range(peers - 2)]
    down_chain = [(i + 2, i) for i in range(peers - 2)]
    segs = []
    bases = []
    moving = own_seg
    for k in range(steps):
        if k > 0:
            moving = lax.ppermute(moving, "heads", up_chain)
            moving, crossed = lax.optimization_barrier((moving, segs[-1][1]))
            segs[-1] = (segs[-1][0], crossed)
        segs.append((moving, flip(moving, "heads", 0)))
        base = ((level - k) * 2 + side) * tokens
        other = ((level - k) * 2 + 1 - side) * tokens
        there = level >= k
        bases.append(
            (jnp.where(there, base, -1), jnp.where(there & (other < own_base), other, -1))
        )

    def pick(items):
        return (
            [segs[k][j] for k, j in items],
            jnp.stack([bases[k][j] for k, j in items] + [own_base]).astype(jnp.int32),
        )

    parts = [p for p in (range(0, 2), range(2, steps - 1), range(steps - 1, steps)) if len(p) > 0]
    state = expanded = None
    for i, ks in enumerate(parts):
        seg_list, base_list = pick([(k, j) for k in ks for j in range(2)])
        made = attend_part(
            queries, start, key_lift, value_lift_t, lo, seg_list, base_list, expanded, state, i == len(parts) - 1
        )
        state = made[:3]
        if i == 0:
            expanded = made[3]
    head_out, lse, head_mix = state
    mixed_mine = head_out[:rows].reshape(count, group_width)
    mixed_got = swap(head_out[rows:]).reshape(count, group_width)
    keep = (own_docs != 0).astype(f32).reshape(count, 1)
    hidden_out, grad_resid, grad_mixed_mine, grad_mixed_sent, ffn_gain_part, down_grad, feed_grads = feed(
        core, hidden_in.reshape(count, width), mixed_mine, mixed_got, output_weight, ffn_gain,
        cotangent.reshape(count, width), keep, (gate_weight, up_weight, down_weight), pieces,
    )
    head_grads = [a.reshape(rows, tokens, group_width) for a in (grad_mixed_mine, swap(grad_mixed_sent))]
    early_down = lax.psum_scatter(down_grad, "rows", scatter_dimension=0, tiled=True)[0]
    early_feed = lax.psum_scatter(feed_grads, "rows", scatter_dimension=0, tiled=True)[0]

    calls = [[(k, 0), (k, 1)] for k in range(steps - 1, 0, -1)]
    calls[-1].append((0, 1))
    calls.append([(0, 0)])
    state = kept = None
    pieces_in = []
    waiting = []
    passing = None
    now = queries

    def join(parts):
        total = parts[0].astype(f32) + parts[1].astype(f32)
        if passing is not None:
            total = total + passing.astype(f32)
        return total.astype(bf16)

    for i, items in enumerate(calls):
        if len(waiting) == 2:
            now, joined = lax.optimization_barrier((queries, join(waiting.pop(0))))
            passing = lax.ppermute(joined, "heads", down_chain)
        seg_list, base_list = pick(items)
        made = attend_back_part(
            now, head_grads, lse, head_mix, start, expanded, value_lift, key_lift_t, lo,
            seg_list, base_list, kept, state, len(items) == 1,
        )
        state = made[len(items) : len(items) + 2]
        if i == 0:
            *kept, value_part = made[len(items) + 2 :]
        k = items[0][0]
        if k == 0:
            pieces_in.append(made[0])
            continue
        waiting.append((made[0], flip(made[1], "heads", 0)))
        if k == 1:
            pieces_in.append(flip(made[2], "heads", 0))
    joined = join(waiting.pop())
    query_grads, key_part = made[1:]
    latent_grads = sum(p.astype(f32) for p in pieces_in)

    ff_share = gate_weight.shape[1] // peers
    full, hidden_grad = finish(
        (early_feed, early_down),
        ((ff_share, ff_share, share), (ff_share,)),
        peers,
        (
            hidden_in.reshape(count, width), attn_gain.reshape(1, width),
            query_grads.reshape(2, count, group_width), latent_grads.reshape(2, count, latent_size),
            joined.reshape(2, count, latent_size),
            query_weight, latent_weight, grad_resid, ffn_gain_part, key_part, value_part,
        ),
    )
    (
        gate_share, up_share, output_share, down_share, query_share, latent_share, key_share, value_share, gains,
        hidden_grad,
    ) = lay_out(full, hidden_grad, (ff_share, ff_share, share, ff_share), share, latent_size, group_width, peers, width)
    gains = lax.dynamic_slice_in_dim(gains, (place * share) % gains.shape[1], share, 1)
    return (
        hidden_out.reshape(rows, tokens, width),
        hidden_grad.reshape(rows, tokens, width),
        gains[0],
        query_share,
        latent_share,
        key_share,
        value_share,
        output_share,
        gains[1],
        gate_share.T,
        up_share.T,
        down_share,
    )


def solution(mesh):
    placed = (
        P("rows", "heads", None),
        P("rows", None),
        P("rows", "heads", None),
        P(),
        P(),
        P(),
        P(),
        P(),
        P(),
        P(),
        P(),
        P(),
        P(),
    )
    return jax.shard_map(
        shards,
        mesh=mesh,
        in_specs=placed,
        out_specs=(
            P("rows", "heads", None),
            P("rows", "heads", None),
            P("heads"),
            P("heads", None),
            P("heads", None),
            P(None, "heads", None),
            P(None, "heads", None),
            P("heads", None),
            P("heads"),
            P(None, "heads"),
            P(None, "heads"),
            P("heads", None),
        ),
        check_vma=False,
    )
```

```python
import functools
import math

import jax
import jax.numpy as jnp
from jax import lax
from jax.experimental import pallas as pl
from jax.experimental.pallas import tpu as pltpu
from jax.sharding import PartitionSpec as P

HEAD_WIDTH = 64
epsilon = 1e-05
blocked = -1e30
LOG2E = math.log2(math.e)
LN2 = math.log(2.0)
QUAD = 4
f32 = jnp.float32
bf16 = jnp.bfloat16


def matmul(left, right):
    return jnp.dot(left, right, preferred_element_type=f32)


def matmul_nt(left, right):
    return lax.dot_general(
        left, right, (((left.ndim - 1,), (right.ndim - 1,)), ((), ())), preferred_element_type=f32
    )


def matmul_tn(left, right):
    return lax.dot_general(left, right, (((0,), (0,)), ((), ())), preferred_element_type=f32)


def rms_inverse(value_matrix):
    return lax.rsqrt(jnp.mean(value_matrix * value_matrix, axis=-1, keepdims=True) + epsilon)


def expand_heads(source, weights, factor, out_ref):
    tokens = source.shape[0]
    quads, wide, deep = weights.shape
    latent = wide // QUAD
    for quad in range(quads):
        product = matmul_nt(weights[quad], source[:, quad * deep : (quad + 1) * deep])
        if factor != 1.0:
            product = product * factor
        product = product.astype(bf16)
        for h in range(QUAD):
            at = (quad * QUAD + h) * tokens
            out_ref[:, at : at + tokens] = product[h * latent : (h + 1) * latent]


def lift_heads(source, weights, tokens):
    parts = [
        matmul(weights[h], source[:, h * tokens : (h + 1) * tokens]) for h in range(weights.shape[0])
    ]
    return jnp.concatenate(parts, axis=0)


def lift_grad(left, right, tokens, out_ref):
    latent = left.shape[0]
    deep = QUAD * HEAD_WIDTH
    head = lax.broadcasted_iota(jnp.int32, (latent, deep), 1) // HEAD_WIDTH
    for quad in range(right.shape[1] // deep):
        columns = slice(quad * deep, (quad + 1) * deep)
        found = None
        for h in range(QUAD):
            at = (quad * QUAD + h) * tokens
            part = matmul(left[:, at : at + tokens], right[:, columns])
            found = part if h == 0 else jnp.where(head == h, part, found)
        out_ref[:, columns] += found


def seg_mask(base, own_base, start):
    tokens = start.shape[-1]
    key_at = lax.broadcasted_iota(jnp.int32, (tokens, tokens), 0)
    query_at = lax.broadcasted_iota(jnp.int32, (tokens, tokens), 1)
    return (key_at >= start - base) & (key_at <= query_at + (own_base - base))


def attend_kernel(count, first, last, lo, bases, *refs):
    refs = list(refs)
    take = lambda k: [refs.pop(0) for _ in range(k)]
    (start_ref,) = take(1)
    if first:
        query_ref, key_lift_ref = take(2)
    else:
        expanded_ref, top_in, total_in, mix_in = take(4)
    seg_refs = take(count)
    if last:
        (value_lift_ref,) = take(1)
        out_ref, lse_ref, mix_ref = take(3)
    else:
        top_out, total_out, mix_out = take(3)
    if first:
        (expanded_ref,) = take(1)
    top, total, mix, segs = take(4)
    expanded = expanded_ref.at[0]
    tokens = start_ref.shape[2]
    heads = expanded.shape[1] // tokens
    row = pl.program_id(0)
    touched = lambda i: (bases[i] >= 0) & (bases[i] + tokens - 1 >= lo[row])
    if first:
        expand_heads(query_ref[0], key_lift_ref, HEAD_WIDTH ** (-0.5) * LOG2E, expanded)
        top[...] = jnp.full_like(top, blocked)
        total[...] = jnp.zeros_like(total)
        mix[...] = jnp.zeros_like(mix)
    else:
        top[...] = top_in[0]
        total[...] = total_in[0]
        mix[...] = mix_in[0].astype(f32)
    for i in range(count):
        segs[i] = seg_refs[i][0]

    @pl.loop(0, count)
    def _(i):
        @pl.when(touched(i))
        def _():
            latent = segs[i]
            latent_t = latent.T
            allow = seg_mask(bases[i], bases[count], start_ref[0])
            for h in range(heads):
                at = slice(h * tokens, (h + 1) * tokens)
                score = jnp.where(allow, matmul(latent, expanded[:, at]), blocked)
                old = top[:, at]
                new = jnp.maximum(old, jnp.max(score, axis=0, keepdims=True))
                probs = jnp.exp2(score - new)
                fade = jnp.exp2(old - new)
                top[:, at] = new
                total[:, at] = total[:, at] * fade + jnp.sum(probs, axis=0, keepdims=True)
                mix[:, at] = mix[:, at] * fade + matmul(latent_t, probs.astype(bf16))

    if not last:
        top_out[0] = top[...]
        total_out[0] = total[...]
        mix_out[0] = mix[...].astype(bf16)
        return
    lse_ref[0] = top[...] + jnp.log2(total[...])
    mix_ref[0] = (mix[...] * (1.0 / total[...])).astype(bf16)
    out_ref[0] = lift_heads(mix_ref[0], value_lift_ref, tokens).T.astype(bf16)


def whole(array):
    return pl.BlockSpec(array.shape, lambda *_: (0,) * len(array.shape))


def by_row(shape):
    return pl.BlockSpec((1,) + tuple(shape[1:]), lambda r, *_: (r,) + (0,) * (len(shape) - 1))


def attend_part(queries, start, key_lift, value_lift_t, lo, segs, bases, expanded, state, last):
    rows, tokens, width = queries.shape
    heads = width // HEAD_WIDTH
    latent = segs[0].shape[-1]
    shape = jax.ShapeDtypeStruct
    stat = shape((rows, 1, heads * tokens), f32)
    flat = shape((rows, latent, heads * tokens), bf16)
    if state is None:
        args = [start, queries, key_lift, *segs]
        specs = [by_row(start.shape), by_row(queries.shape), whole(key_lift)]
    else:
        args = [start, expanded, *state, *segs]
        specs = [by_row(a.shape) for a in args[:5]]
    specs += [by_row(s.shape) for s in segs]
    if last:
        args.append(value_lift_t)
        specs.append(whole(value_lift_t))
        outs = [shape(queries.shape, bf16), stat, flat]
    else:
        outs = [stat, stat, flat]
    if state is None:
        outs.append(flat)
    blocks = rows * heads * len(segs)
    return pl.pallas_call(
        functools.partial(attend_kernel, len(segs), state is None, last),
        out_shape=outs,
        grid_spec=pltpu.PrefetchScalarGridSpec(
            num_scalar_prefetch=2,
            grid=(rows,),
            in_specs=specs,
            out_specs=[by_row(o.shape) for o in outs],
            scratch_shapes=[
                pltpu.VMEM((1, heads * tokens), f32),
                pltpu.VMEM((1, heads * tokens), f32),
                pltpu.VMEM((latent, heads * tokens), f32),
                pltpu.VMEM((len(segs), tokens, latent), bf16),
            ],
        ),
        compiler_params=pltpu.CompilerParams(
            dimension_semantics=("arbitrary",), vmem_limit_bytes=48 << 20
        ),
        cost_estimate=pl.CostEstimate(
            flops=blocks * tokens * tokens * latent * 64,
            bytes_accessed=rows * heads * latent * tokens * 64,
            transcendentals=blocks * tokens * tokens,
        ),
        name="attend",
    )(lo, bases, *args)


def attend_back_kernel(count, first, last, lo, bases, *refs):
    refs = list(refs)
    take = lambda k: [refs.pop(0) for _ in range(k)]
    query_ref, lse_ref, start_ref, expanded_ref, key_lift_t_ref = take(5)
    seg_refs = take(count)
    if first:
        grad_mine, grad_got, mix_ref, value_lift_ref = take(4)
    else:
        expanded_grad_ref, delta_ref, query_back_in, key_up_in = take(4)
    grad_refs = take(count)
    query_back_ref, key_up_ref = take(2)
    if first:
        expanded_grad_ref, delta_ref, value_up_ref = take(3)
    back, query_back, segs, seg_grads = take(4)
    expanded, expanded_grad = expanded_ref.at[0], expanded_grad_ref.at[0]
    tokens = query_ref.shape[1]
    heads = expanded.shape[1] // tokens
    row = pl.program_id(0)
    scale = HEAD_WIDTH ** (-0.5)
    touched = lambda i: (bases[i] >= 0) & (bases[i] + tokens - 1 >= lo[row])
    any_touched = functools.reduce(jnp.logical_or, [touched(i) for i in range(count)])

    @pl.when(row == 0)
    def _():
        key_up_ref[...] = jnp.zeros_like(key_up_ref) if first else key_up_in[...]
        if first:
            value_up_ref[...] = jnp.zeros_like(value_up_ref)

    query_back[...] = jnp.zeros_like(query_back) if first else query_back_in[0]
    seg_grads[...] = jnp.zeros_like(seg_grads)
    if first:
        grads = jnp.where(row < pl.num_programs(0) // 2, grad_mine[0], grad_got[0])
        expand_heads(grads, value_lift_ref, 1.0, expanded_grad)
        delta_ref[0] = jnp.sum(mix_ref[0].astype(f32) * expanded_grad[...].astype(f32), axis=0, keepdims=True)
        lift_grad(mix_ref[0], grads, tokens, value_up_ref)

    @pl.when(any_touched)
    def _():
        back[...] = jnp.zeros_like(back)
        for i in range(count):
            segs[i] = seg_refs[i][0]

    @pl.loop(0, count)
    def _(i):
        @pl.when(touched(i))
        def _():
            latent = segs[i]
            allow = seg_mask(bases[i], bases[count], start_ref[0])
            allow = jnp.concatenate([allow] * heads, axis=1)
            score = matmul(latent, expanded[...])
            probs = jnp.where(allow, jnp.exp2(score - lse_ref[0]), 0.0)
            dprobs = matmul(latent, expanded_grad[...])
            dscore = (probs * (dprobs - delta_ref[0])).astype(bf16)
            by_key = matmul_nt(dscore, expanded[...])
            by_value = matmul_nt(probs.astype(bf16), expanded_grad[...])
            seg_grads[i] = (by_key * LN2 + by_value).astype(bf16)
            back[...] += matmul(latent.T, dscore)

    for i in range(count):
        grad_refs[i][0] = seg_grads[i]

    @pl.when(any_touched)
    def _():
        part = (back[...] * scale).astype(bf16)
        query_back[...] += lift_heads(part, key_lift_t_ref, tokens)
        lift_grad(part, query_ref[0], tokens, key_up_ref)

    if last:
        query_back_ref[0] = query_back[...].T.astype(bf16)
    else:
        query_back_ref[0] = query_back[...]


def attend_back_part(queries, grads, lse, mix, start, expanded, value_lift, key_lift_t, lo, segs, bases, kept, state, last):
    rows, tokens, width = queries.shape
    heads = width // HEAD_WIDTH
    latent = segs[0].shape[-1]
    shape = jax.ShapeDtypeStruct
    back_shape = shape((rows, width, tokens), f32)
    up_shape = shape((latent, width), f32)
    first = state is None
    args = [queries, lse, start, expanded, key_lift_t, *segs]
    specs = [by_row(a.shape) for a in args[:4]] + [whole(key_lift_t)]
    specs += [by_row(s.shape) for s in segs]
    if first:
        args += [*grads, mix, value_lift]
        half = (1, tokens, width)
        specs.append(pl.BlockSpec(half, lambda r, *_: (jnp.minimum(r, rows // 2 - 1), 0, 0)))
        specs.append(pl.BlockSpec(half, lambda r, *_: (jnp.maximum(r - rows // 2, 0), 0, 0)))
        specs += [by_row(mix.shape), whole(value_lift)]
    else:
        args += [*kept, *state]
        specs += [by_row(kept[0].shape), by_row(kept[1].shape), by_row(back_shape.shape), whole(up_shape)]
    outs = [shape(s.shape, bf16) for s in segs]
    outs += [shape(queries.shape, bf16) if last else back_shape, up_shape]
    out_specs = [by_row(o.shape) for o in outs[:-1]] + [whole(up_shape)]
    if first:
        outs += [shape(expanded.shape, bf16), shape(lse.shape, f32), up_shape]
        out_specs += [by_row(expanded.shape), by_row(lse.shape), whole(up_shape)]
    blocks = rows * heads * len(segs)
    return pl.pallas_call(
        functools.partial(attend_back_kernel, len(segs), first, last),
        out_shape=outs,
        grid_spec=pltpu.PrefetchScalarGridSpec(
            num_scalar_prefetch=2,
            grid=(rows,),
            in_specs=specs,
            out_specs=out_specs,
            scratch_shapes=[
                pltpu.VMEM((latent, heads * tokens), f32),
                pltpu.VMEM((width, tokens), f32),
                pltpu.VMEM((len(segs), tokens, latent), bf16),
                pltpu.VMEM((len(segs), tokens, latent), bf16),
            ],
        ),
        compiler_params=pltpu.CompilerParams(
            dimension_semantics=("arbitrary",), vmem_limit_bytes=48 << 20
        ),
        cost_estimate=pl.CostEstimate(
            flops=blocks * tokens * tokens * latent,
            bytes_accessed=rows * heads * latent * tokens,
            transcendentals=0,
        ),
        name="attend_back",
    )(lo, bases, *args)


def quad_lift(lift):
    latent, width = lift.shape
    deep = QUAD * HEAD_WIDTH
    quads = width // deep
    tall = jnp.tile(lift.reshape(latent, quads, deep).transpose(1, 0, 2), (1, QUAD, 1))
    row_head = lax.broadcasted_iota(jnp.int32, tall.shape, 1) // latent
    column_head = lax.broadcasted_iota(jnp.int32, tall.shape, 2) // HEAD_WIDTH
    return jnp.where(row_head == column_head, tall, jnp.zeros_like(tall))


def head_lift(lift):
    latent, width = lift.shape
    return lift.T.reshape(width // HEAD_WIDTH, HEAD_WIDTH, latent)


def put_pieces(ref, value, at=0):
    pieces, _, piece = ref.shape
    for j in range(pieces):
        ref[j, pl.ds(at, value.shape[0])] = value[:, j * piece : (j + 1) * piece].astype(bf16)


def feed_kernel(core_ref, *refs):
    (
        inputs_ref, mine_ref, got_ref, output_ref, gain_ref, cotangent_ref, keep_ref,
        gate_ref, up_ref, down_ref,
        hidden_out_ref, resid_out, normed_out, back_out, active_ref, slope_ref, down_grad_ref,
        result, hidden, resid, normed, back, sems,
    ) = refs
    step = pl.program_id(0)
    leaving = [
        pltpu.make_async_copy(source, target, sems.at[i])
        for i, (source, target) in enumerate(((resid, resid_out), (normed, normed_out), (back, back_out)))
    ]
    count = inputs_ref.shape[0]
    block = min(256, count)
    core = core_ref[0]

    @pl.when(step == 0)
    def _():
        for t in range(0, count, block):
            at = slice(t, t + block)
            row = inputs_ref[at].astype(f32) + (
                matmul(mine_ref[at], output_ref[core]) + matmul(got_ref[at], output_ref[1 - core])
            )
            resid[at] = row
            scale = lax.rsqrt(jnp.mean(row * row, axis=-1, keepdims=True) + epsilon)
            normed[at] = (row * scale * gain_ref[...]).astype(bf16)
            back[at] = (cotangent_ref[at].astype(f32) * keep_ref[at]).astype(bf16)
        for copy in leaving:
            copy.start()
        result[...] = jnp.zeros_like(result)

    part = count // 4
    for t in range(0, count, part):
        at = slice(t, t + part)
        gate = matmul(normed[at], gate_ref[...])
        up = matmul(normed[at], up_ref[...])
        sigmoid = 1.0 / (1.0 + jnp.exp(-gate))
        active = gate * sigmoid
        hidden[at] = (active * up).astype(bf16)
        active_ref[at] = active.astype(bf16)
        slope_ref[at] = (up * (sigmoid * (1.0 + gate * (1.0 - sigmoid)))).astype(bf16)
    put_pieces(down_grad_ref, matmul_tn(hidden[...], back[...]))
    result[...] += matmul(hidden[...], down_ref[...])

    @pl.when(step == pl.num_programs(0) - 1)
    def _():
        hidden_out_ref[...] = (resid[...] + result[...]).astype(bf16)
        for copy in leaving:
            copy.wait()


def feed_back_kernel(core_ref, *refs):
    (
        mine_in, got_in, output_in, resid_in, gain_ref, normed, back,
        active_ref, slope_ref, gate_ref, up_ref, down_ref,
        grad_resid_out, head_mine_out, head_sent_out, gain_grad_ref, grads_ref,
        grad_two, both, low, staged, staged_out, mine_ref, got_ref, output_ref, resid_ref, head_mine_ref, head_sent_ref,
        sems, out_sem, in_sems, leave_sems,
    ) = refs
    step = pl.program_id(0)
    steps = pl.num_programs(0)
    count, width = resid_ref.shape
    coming = [
        pltpu.make_async_copy(source, target, in_sems.at[i])
        for i, (source, target) in enumerate(
            ((mine_in, mine_ref), (got_in, got_ref), (output_in, output_ref), (resid_in, resid_ref))
        )
    ]
    chunk = down_ref.shape[0]
    ff = (grads_ref.shape[1] - width) // 2
    block = min(256, count)
    core = core_ref[0]
    slot = step % 2

    def leave(at, kind, place):
        return pltpu.make_async_copy(
            staged.at[at, kind],
            grads_ref.at[:, pl.ds(pl.multiple_of(kind * ff + place * chunk, chunk), chunk)],
            sems.at[at, kind],
        )

    @pl.when(step >= 2)
    def _():
        for kind in range(2):
            leave(slot, kind, step - 2).wait()

    @pl.when(step == 0)
    def _():
        for copy in coming:
            copy.start()
        grad_two[...] = jnp.zeros_like(grad_two)

    part = count // 4
    for t in range(0, count, part):
        at = slice(t, t + part)
        grad_act = matmul_nt(back[at], down_ref[...])
        both[at, :chunk] = (grad_act * slope_ref[at].astype(f32)).astype(bf16)
        both[at, chunk:] = (grad_act * active_ref[at].astype(f32)).astype(bf16)
    for kind in range(2):
        put_pieces(staged.at[slot, kind], matmul_tn(both[:, kind * chunk : (kind + 1) * chunk], normed[...]))
        leave(slot, kind, step).start()
    weights = jnp.concatenate([gate_ref[...], up_ref[...]], axis=1)
    for t in range(0, count, part):
        at = slice(t, t + part)
        grad_two[at] += matmul_nt(both[at], weights)

    @pl.when(step == steps - 1)
    def _():
        for copy in coming:
            copy.wait()
        gain_total = jnp.zeros((1, width), f32)
        leaving = []
        for t in range(0, count, block):
            at = slice(t, t + block)
            row = resid_ref[at]
            scale = lax.rsqrt(jnp.mean(row * row, axis=-1, keepdims=True) + epsilon)
            unit = row * scale
            grad = grad_two[at]
            gain_total += jnp.sum(grad * unit, axis=0, keepdims=True)
            scaled = grad * gain_ref[...]
            grad = back[at].astype(f32) + scale * (
                scaled - unit * jnp.mean(scaled * unit, axis=-1, keepdims=True)
            )
            grad_two[at] = grad
            low[at] = grad.astype(bf16)
            head_mine_ref[at] = matmul_nt(low[at], output_ref[core]).astype(bf16)
            head_sent_ref[at] = matmul_nt(low[at], output_ref[1 - core]).astype(bf16)
            for i, (source, target) in enumerate(
                ((grad_two, grad_resid_out), (head_mine_ref, head_mine_out), (head_sent_ref, head_sent_out))
            ):
                rows = pl.ds(t, block)
                copy = pltpu.make_async_copy(source.at[rows], target.at[rows], leave_sems.at[t // block, i])
                copy.start()
                leaving.append(copy)
        gain_grad_ref[...] = gain_total
        half = mine_ref.shape[1]
        put_pieces(staged_out, matmul_tn(mine_ref[...], low[...]), core * half)
        put_pieces(staged_out, matmul_tn(got_ref[...], low[...]), (1 - core) * half)
        last = pltpu.make_async_copy(staged_out, grads_ref.at[:, pl.ds(2 * ff, width)], out_sem)
        last.start()
        for kind in range(2):
            leave(1 - slot, kind, step - 1).wait()
            leave(slot, kind, step).wait()
        last.wait()
        for copy in leaving:
            copy.wait()


def once(array):
    return pl.BlockSpec(array.shape, lambda *_: (0,) * len(array.shape), pipeline_mode=pl.Buffered(1))


def feed(core, inputs, mixed_mine, mixed_got, output_weight, gain, cotangent, keep, weights, pieces):
    count, width = inputs.shape
    gate_weight, up_weight, down_weight = weights
    ff = gate_weight.shape[1]
    chunk = 256
    piece = width // pieces
    output_weight = output_weight.reshape(2, -1, width)
    gain = gain.reshape(1, width)
    by_rows = pl.BlockSpec((chunk, width), lambda c, *_: (c, 0))
    by_columns = pl.BlockSpec((width, chunk), lambda c, *_: (0, c))
    kept_columns = pl.BlockSpec((count, chunk), lambda c, *_: (0, c))
    shape = jax.ShapeDtypeStruct
    params = pltpu.CompilerParams(dimension_semantics=("arbitrary",), vmem_limit_bytes=60 << 20)
    full_bf, full_f = shape((count, width), bf16), shape((count, width), f32)
    kept = shape((count, ff), bf16)
    firsts = [inputs, mixed_mine, mixed_got, output_weight, gain, cotangent, keep]
    outs = [full_bf, full_f, full_bf, full_bf, kept, kept, shape((pieces, ff, piece), bf16)]
    hidden_out, resid, normed, back, active, slope, down_grad = pl.pallas_call(
        feed_kernel,
        out_shape=outs,
        grid_spec=pltpu.PrefetchScalarGridSpec(
            num_scalar_prefetch=1,
            grid=(ff // chunk,),
            in_specs=[once(a) for a in firsts] + [by_columns, by_columns, by_rows],
            out_specs=[once(outs[0])]
            + [pl.BlockSpec(memory_space=pl.ANY)] * 3
            + [kept_columns, kept_columns, pl.BlockSpec((pieces, chunk, piece), lambda c, *_: (0, c, 0))],
            scratch_shapes=[
                pltpu.VMEM((count, width), f32),
                pltpu.VMEM((count, chunk), bf16),
                pltpu.VMEM((count, width), f32),
                pltpu.VMEM((count, width), bf16),
                pltpu.VMEM((count, width), bf16),
                pltpu.SemaphoreType.DMA((3,)),
            ],
        ),
        compiler_params=params,
        cost_estimate=pl.CostEstimate(
            flops=count * width * (ff * 8 + width * 2),
            bytes_accessed=width * ff * 8 + count * width * 16 + count * ff * 4,
            transcendentals=count * ff,
        ),
        name="feed",
    )(core.reshape(1), *firsts, *weights)
    firsts = [mixed_mine, mixed_got, output_weight, resid, gain, normed, back]
    anywhere = pl.BlockSpec(memory_space=pl.ANY)
    outs = [
        full_f,
        shape(mixed_mine.shape, bf16),
        shape(mixed_mine.shape, bf16),
        shape((1, width), f32),
        shape((pieces, 2 * ff + width, piece), bf16),
    ]
    grad_resid, head_mine, head_sent, gain_grad, grads = pl.pallas_call(
        feed_back_kernel,
        out_shape=outs,
        grid_spec=pltpu.PrefetchScalarGridSpec(
            num_scalar_prefetch=1,
            grid=(ff // chunk,),
            in_specs=[anywhere] * 4
            + [once(a) for a in firsts[4:]]
            + [kept_columns, kept_columns, by_columns, by_columns, by_rows],
            out_specs=[anywhere] * 3 + [once(outs[3]), anywhere],
            scratch_shapes=[
                pltpu.VMEM((count, width), f32),
                pltpu.VMEM((count, 2 * chunk), bf16),
                pltpu.VMEM((count, width), bf16),
                pltpu.VMEM((2, 2, pieces, chunk, piece), bf16),
                pltpu.VMEM((pieces, width, piece), bf16),
                pltpu.VMEM(mixed_mine.shape, bf16),
                pltpu.VMEM(mixed_mine.shape, bf16),
                pltpu.VMEM(output_weight.shape, bf16),
                pltpu.VMEM((count, width), f32),
                pltpu.VMEM(mixed_mine.shape, bf16),
                pltpu.VMEM(mixed_mine.shape, bf16),
                pltpu.SemaphoreType.DMA((2, 2)),
                pltpu.SemaphoreType.DMA,
                pltpu.SemaphoreType.DMA((4,)),
                pltpu.SemaphoreType.DMA((max(1, count // 256), 3)),
            ],
        ),
        compiler_params=params,
        cost_estimate=pl.CostEstimate(
            flops=count * width * (ff * 10 + width * 4),
            bytes_accessed=width * ff * 10 + count * width * 20 + count * ff * 4,
            transcendentals=0,
        ),
        name="feed_back",
    )(core.reshape(1), *firsts, active, slope, *weights)
    return hidden_out, grad_resid, head_mine, head_sent, gain_grad, down_grad, grads


def flip(array, axis, bit):
    size = lax.axis_size(axis)
    return lax.ppermute(array, axis, [(i, i ^ (1 << bit)) for i in range(size)])


def fill_shards(target, at, grad, count):
    along, piece = target.shape[0], target.shape[3]
    size = grad.shape[0] // count
    for s in range(count):
        for j in range(along):
            target[j, s, at : at + size] = grad[s * size : (s + 1) * size, j * piece : (j + 1) * piece].astype(bf16)


def fill_folded(target, at, grad, count):
    along, piece = target.shape[0], target.shape[3]
    size = grad.shape[0] // count
    latent = grad.shape[1]
    fold = size // 2
    for s in range(count):
        for j in range(along):
            side, column = divmod(j * piece, latent)
            first = s * size + side * fold
            target[j, s, at : at + fold] = grad[first : first + fold, column : column + piece].astype(bf16)


def fill_gains(target, at, gain, count):
    along, piece = target.shape[0], target.shape[3]
    share = gain.shape[1] // count
    lane = max(share, 128)
    for s in range(count):
        begin = s * share // lane * lane
        kept = jnp.broadcast_to(gain[:, begin : begin + lane], (16, lane)).astype(bf16)
        target[0, s, at : at + 16, :lane] = kept
        if piece > lane:
            target[0, s, at : at + 16, lane:] = jnp.zeros((16, piece - lane), bf16)
        for j in range(1, along):
            target[j, s, at : at + 16] = jnp.zeros((16, piece), bf16)


def finish_kernel(sections, groups, sizes, refs, loads, grad_copy):
    (
        early_refs, inputs_ref, gain_ref, query_grad_ref, latent_grad_ref, joined_ref,
        query_ref, latent_ref, resid_ref, other_gain_ref, key_up, value_up,
        out_ref, grad_ref,
        normed, own_ref, sent_ref, late_got, late_from, got_first, got_next,
        chain_got, query_got, latent_low, latent_got,
        chain_sems, core_sems, along_sems, first_sems, first_late_sems, next_sems, out_sems,
    ) = refs
    along, count, late_rows, piece = own_ref.shape
    early_rows, share, fold, lift = sizes
    early_loads, late_loads = loads

    def here(*which):
        for i in which:
            late_loads[i].wait()

    for copy in [late_loads[4], late_loads[2], *early_loads, late_loads[0], late_loads[1]]:
        copy.start()
    for i in (9, 10, 3, 5, 6, 7, 8):
        late_loads[i].start()
    bits = count.bit_length() - 1
    row_at = lax.axis_index("rows")
    place = lax.axis_index("heads")
    core = row_at % 2
    x_at = row_at // 2
    mesh = pl.DeviceIdType.MESH
    tokens, width = inputs_ref.shape
    latent = latent_low.shape[2]
    half = query_got.shape[1]
    block = min(256, tokens)
    parts = [slice(0, early_rows)] + [slice(early_rows + g[0], early_rows + g[1]) for g in groups]

    def turned(which):
        at = place
        for bit in which:
            at = at + (1 << bit) * (1 - 2 * ((place // (1 << bit)) % 2))
        return at

    core_peer = (row_at + 1 - 2 * core, place)
    x_others = [(x_at + d) % along for d in range(1, along)]
    x_peers = [(x * 2 + core, place) for x in x_others]
    head_peers = [(row_at, turned([bit])) for bit in range(bits)]
    above = (row_at, (place + 2) % count)
    below = (row_at, (place + count - 2) % count)
    barrier = pltpu.get_barrier_semaphore()
    everyone = [core_peer, above, below] + x_peers + head_peers
    for peer in everyone:
        pl.semaphore_signal(barrier, inc=1, device_id=peer, device_id_type=mesh)
    pl.semaphore_wait(barrier, len(everyone))

    def remote(source, target, sems, index, peer):
        return pltpu.make_async_remote_copy(
            src_ref=source, dst_ref=target, send_sem=sems.at[(0,) + index], recv_sem=sems.at[(1,) + index],
            device_id=peer, device_id_type=mesh,
        )

    def orders(bit):
        rest = list(range(bit + 1, bits))
        return [
            [b for i, b in enumerate(rest) if not (mask >> (len(rest) - 1 - i)) & 1]
            for mask in range(1 << len(rest))
        ]

    def add_rows(target, other, size):
        step = size if size <= 600 else size // 2

        def one(i, carry):
            at = pl.ds(pl.multiple_of(i * step, 16), step)
            target[at] = (target[at].astype(f32) + other[at].astype(f32)).astype(bf16)
            return carry

        lax.fori_loop(0, size // step, one, 0)

    def rows_of(part):
        return pl.ds(part.start, part.stop - part.start)

    first = orders(0)
    final = len(first) - 1
    pending = []

    def early_rows_of(n, shard):
        which, start, size, _ = sections[n]
        return early_refs[which].at[pl.ds(pl.multiple_of(start + shard * size, 16), size)]

    def first_early(i, n):
        _, _, size, row = sections[n]
        return remote(
            early_rows_of(n, turned([0] + first[i])), got_first.at[i, pl.ds(row, size)],
            first_sems, (i, n), head_peers[0],
        )

    def next_copy(bit, j, i, which):
        rows = rows_of(parts[which])
        return remote(
            got_first.at[i, rows], got_next[bit - 1].at[j, rows], next_sems[bit - 1], (j, which), head_peers[bit]
        )

    def settle(i, which):
        rest = first[i]
        level = rest[0] if rest else bits
        rows = rows_of(parts[which])
        for bit in range(1, level):
            j = orders(bit).index(rest)
            next_copy(bit, j, i, which).wait_recv()
            add_rows(got_first.at[i, rows], got_next[bit - 1].at[j, rows], rows.size)
        if rest:
            copy = next_copy(level, orders(level).index(rest[1:]), i, which)
            copy.start()
            pending.append(copy)

    def early_step(i):
        for n, (_, _, size, row) in enumerate(sections):
            first_early(i, n).wait()
            add_rows(got_first.at[i, pl.ds(row, size)], early_rows_of(n, turned(first[i])), size)
        settle(i, 0)

    def core_copy(g):
        _, _, begin, end = groups[g]
        rows = pl.ds(begin, end - begin)
        return remote(sent_ref.at[:, :, rows], late_got.at[:, :, rows], core_sems, (g,), core_peer)

    def x_copies(g):
        low, high, begin, end = groups[g]
        shared = end - begin
        copies = []
        for d, (x, peer) in enumerate(zip(x_others, x_peers)):
            copies.append(
                remote(
                    late_got.at[x, :, pl.ds(begin, shared)], late_from.at[d, :, pl.ds(low, shared)],
                    along_sems, (d, g, 0), peer,
                )
            )
            if low + shared < high:
                rows = pl.ds(low + shared, high - low - shared)
                copies.append(
                    remote(own_ref.at[x, :, rows], late_from.at[d, :, rows], along_sems, (d, g, 1), peer)
                )
        return copies

    def along_x(g):
        low, _, begin, end = groups[g]
        core_copy(g).wait()

        def core_add(i, carry):
            j, s = i // count, i % count
            mine = own_ref[j, s, low : low + end - begin].astype(f32)
            late_got[j, s, begin:end] = (mine + late_got[j, s, begin:end].astype(f32)).astype(bf16)
            return carry

        lax.fori_loop(0, along * count, core_add, 0)
        for copy in x_copies(g):
            copy.start()

    def first_late(i, g):
        low, high, _, _ = groups[g]
        return remote(
            late_from.at[0, turned([0] + first[i]), pl.ds(low, high - low)],
            got_first.at[i, rows_of(parts[1 + g])], first_late_sems, (i, g), head_peers[0],
        )

    def over_heads(g):
        low, high, begin, end = groups[g]
        middle = low + end - begin
        for copy in x_copies(g):
            copy.wait()

        def x_add(s, carry):
            total = late_got[x_at, s, begin:end].astype(f32)
            for d in range(along - 1):
                total = total + late_from[d, s, low:middle].astype(f32)
            late_from[0, s, low:middle] = total.astype(bf16)
            if middle < high:
                total = own_ref[x_at, s, middle:high].astype(f32)
                for d in range(along - 1):
                    total = total + late_from[d, s, middle:high].astype(f32)
                late_from[0, s, middle:high] = total.astype(bf16)
            return carry

        lax.fori_loop(0, count, x_add, 0)
        for i in range(len(first)):
            first_late(i, g).start()

    def late_step(i, g):
        low, high, _, _ = groups[g]
        first_late(i, g).wait()
        add_rows(
            got_first.at[i, rows_of(parts[1 + g])],
            late_from.at[0, turned(first[i]), pl.ds(low, high - low)],
            high - low,
        )
        settle(i, 1 + g)

    mine = lambda ref, size: ref[:, pl.ds(pl.multiple_of(core * size, size), size)]
    theirs = lambda ref, size: ref[:, pl.ds(pl.multiple_of((1 - core) * size, size), size)]
    here(4, 2)
    chain_copy = remote(joined_ref, chain_got, chain_sems, (0,), below)
    chain_copy.start()
    query_copy = remote(query_grad_ref.at[1], query_got, chain_sems, (1,), core_peer)
    query_copy.start()
    for copy in early_loads:
        copy.wait()
    for i in range(len(first)):
        for n in range(len(sections)):
            first_early(i, n).start()

    here(0, 1)

    @pl.loop(0, tokens // block)
    def _(t):
        at = pl.ds(pl.multiple_of(t * block, block), block)
        row = inputs_ref[at].astype(f32)
        scale = lax.rsqrt(jnp.mean(row * row, axis=-1, keepdims=True) + epsilon)
        normed[at] = (row * scale * gain_ref[...]).astype(bf16)

    fill_shards(own_ref, 0, matmul_tn(normed[...], query_grad_ref[0]), count)
    here(9, 10)
    fill_shards(own_ref, share, key_up[...], count)
    fill_shards(own_ref, share + lift, value_up[...], count)
    query_copy.wait()
    fill_shards(sent_ref, 0, matmul_tn(normed[...], query_got[...]), count)
    core_copy(0).start()
    early_step(0)
    along_x(0)
    for i in range(1, len(first) // 2):
        early_step(i)

    here(3)
    chain_copy.wait()
    for side in (1, 0):
        for t in range(0, tokens, block):
            at = slice(t, t + block)
            latent_low[side, at] = (latent_grad_ref[side, at] + chain_got[side, at].astype(f32)).astype(bf16)
        if side == 1:
            latent_copy = remote(latent_low.at[1], latent_got, chain_sems, (2,), core_peer)
            latent_copy.start()
    latent_copy.wait()

    def back(t, gain_total):
        at = pl.ds(pl.multiple_of(t * block, block), block)
        row = inputs_ref[at].astype(f32)
        scale = lax.rsqrt(jnp.mean(row * row, axis=-1, keepdims=True) + epsilon)
        unit = row * scale
        grad = (
            matmul_nt(query_grad_ref[0, at], mine(query_ref, half))
            + matmul_nt(query_got[at], theirs(query_ref, half))
            + matmul_nt(latent_low[0, at], mine(latent_ref, latent))
            + matmul_nt(latent_got[at], theirs(latent_ref, latent))
        )
        scaled = grad * gain_ref[...]
        grad_ref[at] = resid_ref[at] + scale * (
            scaled - unit * jnp.mean(scaled * unit, axis=-1, keepdims=True)
        )
        return gain_total + jnp.sum(grad * unit, axis=0, keepdims=True)

    here(5, 6, 7, 8)
    gain_total = lax.fori_loop(0, tokens // block, back, jnp.zeros((1, width), f32))
    grad_copy.start()
    other = other_gain_ref[...]
    low = groups[1][0]
    for target, at, latents, gain in (
        (own_ref, low, latent_low[0], jnp.where(core == 0, gain_total, other)),
        (sent_ref, groups[1][2], latent_got[...], jnp.where(core == 0, other, gain_total)),
    ):
        fill_folded(target, at, matmul_tn(normed[...], latents), count)
        fill_gains(target, at + fold, gain, count)
    core_copy(1).start()
    over_heads(0)
    along_x(1)
    for i in range(max(1, len(first) // 2), final):
        early_step(i)
    over_heads(1)
    for i in range(final):
        for g in range(len(groups)):
            late_step(i, g)

    def spread(which):
        rows = rows_of(parts[which])
        out_ref[row_at, rows] = got_first[final, rows]
        copies = [remote(out_ref.at[row_at, rows], out_ref.at[row_at, rows], out_sems, (which, 0), core_peer)]
        for d, peer in enumerate(x_peers):
            copies.append(
                remote(out_ref.at[row_at, rows], out_ref.at[row_at, rows], out_sems, (which, 1 + d), peer)
            )
        for copy in copies:
            copy.start()
        return copies

    def pass_on(which, copies):
        rows = rows_of(parts[which])
        more = []
        for d in range(along - 1):
            copies[1 + d].wait_recv()
            source = ((x_at + along - 1 - d) % along) * 2 + core
            more.append(
                remote(
                    out_ref.at[source, rows], out_ref.at[source, rows], out_sems, (which, along + d), core_peer
                )
            )
            more[-1].start()
        return more

    early_step(final)
    spreads = [spread(0)]
    for g in range(len(groups)):
        late_step(final, g)
        spreads.append(spread(1 + g))
    passes = [pass_on(which, copies) for which, copies in enumerate(spreads)]
    for copies, more in zip(spreads, passes):
        copies[0].wait()
        for copy in copies[1:]:
            copy.wait_send()
        for copy in more:
            copy.wait()
    for copy in pending:
        copy.wait_send()
    grad_copy.wait()


def finish(early, shares, count, late_args):
    inputs, _, query_grads, latent_grads = late_args[:4]
    tokens, width = inputs.shape
    latent = latent_grads.shape[2]
    piece = early[0].shape[1]
    along = width // piece // 2
    share = width // count
    fold, lift = share // 2, latent // count
    bits = count.bit_length() - 1
    groups = [
        (0, share + 2 * lift, 0, share),
        (share + 2 * lift, share + 2 * lift + fold + 16, share, share + fold + 16),
    ]
    late_rows, shared_rows = groups[1][1], groups[1][3]
    sections = []
    row = 0
    for which, of_one in enumerate(shares):
        start = 0
        for size in of_one:
            sections.append((which, start, size, row))
            start += size * count
            row += size
    total = row + late_rows
    vmem = pl.BlockSpec(memory_space=pltpu.VMEM)
    dma = pltpu.SemaphoreType.DMA
    anywhere = pl.BlockSpec(memory_space=pl.ANY)

    def body(*refs):
        refs = list(refs)
        take = lambda k: [refs.pop(0) for _ in range(k)]
        early_in, late_in = take(len(early)), take(len(late_args))
        out_ref, grad_out = take(2)
        early_here, late_here = take(len(early)), take(len(late_args))
        grad_here, load_sems, grad_sem = take(3)
        loads = [
            pltpu.make_async_copy(source, target, load_sems.at[i])
            for i, (source, target) in enumerate(zip(early_in + late_in, early_here + late_here))
        ]
        given = [early_here] + late_here + [out_ref, grad_here]
        given += take(6) + [take(bits - 1)] + take(4) + take(5) + [take(bits - 1)] + take(1)
        finish_kernel(
            sections, groups, (row, share, fold, lift), given, (loads[: len(early)], loads[len(early) :]),
            pltpu.make_async_copy(grad_here, grad_out, grad_sem),
        )

    return pl.pallas_call(
        body,
        out_shape=[
            jax.ShapeDtypeStruct((2 * along, total, piece), bf16),
            jax.ShapeDtypeStruct((tokens, width), f32),
        ],
        in_specs=[anywhere] * (len(early) + len(late_args)),
        out_specs=[vmem, anywhere],
        scratch_shapes=[pltpu.VMEM(a.shape, a.dtype) for a in (*early, *late_args)]
        + [
            pltpu.VMEM((tokens, width), f32),
            dma((len(early) + len(late_args),)),
            dma,
            pltpu.VMEM((tokens, width), bf16),
            pltpu.VMEM((along, count, late_rows, piece), bf16),
            pltpu.VMEM((along, count, shared_rows, piece), bf16),
            pltpu.VMEM((along, count, shared_rows, piece), bf16),
            pltpu.VMEM((along - 1, count, late_rows, piece), bf16),
            pltpu.VMEM((count // 2, total, piece), bf16),
        ]
        + [pltpu.VMEM((count >> (bit + 1), total, piece), bf16) for bit in range(1, bits)]
        + [
            pltpu.VMEM((2, tokens, latent), bf16),
            pltpu.VMEM(query_grads.shape[1:], bf16),
            pltpu.VMEM((2, tokens, latent), bf16),
            pltpu.VMEM((tokens, latent), bf16),
            dma((2, 3)),
            dma((2, 2)),
            dma((2, along - 1, 2, 2)),
            dma((2, count // 2, len(sections))),
            dma((2, count // 2, 2)),
        ]
        + [dma((2, count >> (bit + 1), 3)) for bit in range(1, bits)]
        + [dma((2, 3, 2 * along))],
        compiler_params=pltpu.CompilerParams(
            collective_id=0, has_side_effects=True, vmem_limit_bytes=60 << 20
        ),
        name="finish",
    )(*early, *late_args)


def lay_out_kernel(
    rows, latent, full_ref, grad_in, gate_ref, up_ref, output_ref, down_ref, query_ref, latent_ref, key_ref, value_ref,
    gains_ref, grad_out, sem,
):
    copy = pltpu.make_async_copy(grad_in, grad_out, sem)
    copy.start()
    pieces, _, piece = full_ref.shape
    at = 0
    for ref, size in zip((gate_ref, up_ref, output_ref, down_ref), rows):
        for j in range(pieces):
            ref[:, j * piece : (j + 1) * piece] = full_ref[j, at : at + size].astype(f32)
        at += size
    share = query_ref.shape[0]
    fold = share // 2
    lift = key_ref.shape[1]
    half = key_ref.shape[2]
    lane = gains_ref.shape[1]
    for j in range(pieces):
        x, core = divmod(j, 2)
        row = at
        query_ref[:, core * half + x * piece : core * half + (x + 1) * piece] = full_ref[
            j, row : row + share
        ].astype(f32)
        row += share
        for ref in (key_ref, value_ref):
            ref[core, :, x * piece : (x + 1) * piece] = full_ref[j, row : row + lift].astype(f32)
            row += lift
        side, column = divmod(x * piece, latent)
        column += core * latent
        latent_ref[side * fold : (side + 1) * fold, column : column + piece] = full_ref[
            j, row : row + fold
        ].astype(f32)
        row += fold
        if x == 0:
            gains_ref[core : core + 1] = full_ref[j, row : row + 16, :lane].astype(f32)[:1]
    copy.wait()


def lay_out(full, grad, rows, share, latent, half, count, width):
    shape = jax.ShapeDtypeStruct
    gate, up, output, down = rows
    lift = latent // count
    vmem = pl.BlockSpec(memory_space=pltpu.VMEM)
    outs = [
        shape((gate, width), f32),
        shape((up, width), f32),
        shape((output, width), f32),
        shape((down, width), f32),
        shape((share, width), f32),
        shape((share, 2 * latent), f32),
        shape((2, lift, half), f32),
        shape((2, lift, half), f32),
        shape((2, max(share, 128)), f32),
        shape(grad.shape, f32),
    ]
    anywhere = pl.BlockSpec(memory_space=pl.ANY)
    return pl.pallas_call(
        functools.partial(lay_out_kernel, rows, latent),
        out_shape=outs,
        in_specs=[vmem] * 2,
        out_specs=[vmem] * (len(outs) - 1) + [anywhere],
        scratch_shapes=[pltpu.SemaphoreType.DMA],
        compiler_params=pltpu.CompilerParams(vmem_limit_bytes=48 << 20),
        name="lay_out",
    )(full, grad)


def shards(
    hidden_in,
    doc_ids,
    cotangent,
    attn_gain,
    query_weight,
    latent_weight,
    key_lift_weight,
    value_lift_weight,
    output_weight,
    ffn_gain,
    gate_weight,
    up_weight,
    down_weight,
):
    rows, tokens, width = hidden_in.shape
    peers = lax.axis_size("heads")
    place = lax.axis_index("heads")
    core = lax.axis_index("rows") & 1
    groups, latent_size, group_width = key_lift_weight.shape
    count = rows * tokens
    steps = peers // 2
    pieces = lax.axis_size("rows")
    share = width // peers
    side = place & 1
    level = place // 2
    swap = lambda a: flip(a, "rows", 0)
    mine = lambda a, axis: lax.dynamic_slice_in_dim(a, core * (a.shape[axis] // 2), a.shape[axis] // 2, axis)
    theirs = lambda a, axis: lax.dynamic_slice_in_dim(
        a, (1 - core) * (a.shape[axis] // 2), a.shape[axis] // 2, axis
    )

    own_base = place * tokens
    own_docs = lax.dynamic_slice_in_dim(doc_ids, own_base, tokens, 1)
    position = own_base + jnp.arange(tokens, dtype=jnp.int32)
    before = (doc_ids[:, None, :] == own_docs[:, :, None]) & (
        jnp.arange(doc_ids.shape[1], dtype=jnp.int32)[None, None, :] <= position[None, :, None]
    )
    own_start = position[None, :] + 1 - jnp.sum(before.astype(jnp.int32), axis=-1)
    start = jnp.concatenate([own_start, swap(own_start)], axis=0)
    lo = start[:, 0]
    start = start[:, None, :]

    inputs = hidden_in.reshape(count, width).astype(f32)
    inverse_one = rms_inverse(inputs)
    normed_one = (inputs * inverse_one * attn_gain).astype(bf16)
    latent_mine = matmul(normed_one, mine(latent_weight, 1)).astype(bf16)
    latent_sent = matmul(normed_one, theirs(latent_weight, 1)).astype(bf16)
    latent_got = swap(latent_sent)
    own_seg = jnp.concatenate([latent_mine, latent_got], axis=0).reshape(2 * rows, tokens, latent_size)
    query_mine = matmul(normed_one, mine(query_weight, 1)).astype(bf16)
    query_sent = matmul(normed_one, theirs(query_weight, 1)).astype(bf16)
    queries = jnp.concatenate([query_mine, swap(query_sent)], axis=0).reshape(2 * rows, tokens, group_width)

    key_mine = lax.dynamic_index_in_dim(key_lift_weight, core, 0, keepdims=False)
    value_mine = lax.dynamic_index_in_dim(value_lift_weight, core, 0, keepdims=False)
    key_lift = quad_lift(key_mine)
    value_lift = quad_lift(value_mine)
    key_lift_t = head_lift(key_mine)
    value_lift_t = head_lift(value_mine)

    up_chain = [(i, i + 2) for i in range(peers - 2)]
    down_chain = [(i + 2, i) for i in range(peers - 2)]
    segs = []
    bases = []
    moving = own_seg
    for k in range(steps):
        if k > 0:
            moving = lax.ppermute(moving, "heads", up_chain)
            moving, crossed = lax.optimization_barrier((moving, segs[-1][1]))
            segs[-1] = (segs[-1][0], crossed)
        segs.append((moving, flip(moving, "heads", 0)))
        base = ((level - k) * 2 + side) * tokens
        other = ((level - k) * 2 + 1 - side) * tokens
        there = level >= k
        bases.append(
            (jnp.where(there, base, -1), jnp.where(there & (other < own_base), other, -1))
        )

    def pick(items):
        return (
            [segs[k][j] for k, j in items],
            jnp.stack([bases[k][j] for k, j in items] + [own_base]).astype(jnp.int32),
        )

    parts = [p for p in (range(0, 2), range(2, steps - 1), range(steps - 1, steps)) if len(p) > 0]
    state = expanded = None
    for i, ks in enumerate(parts):
        seg_list, base_list = pick([(k, j) for k in ks for j in range(2)])
        made = attend_part(
            queries, start, key_lift, value_lift_t, lo, seg_list, base_list, expanded, state, i == len(parts) - 1
        )
        state = made[:3]
        if i == 0:
            expanded = made[3]
    head_out, lse, head_mix = state
    mixed_mine = head_out[:rows].reshape(count, group_width)
    mixed_got = swap(head_out[rows:]).reshape(count, group_width)
    keep = (own_docs != 0).astype(f32).reshape(count, 1)
    hidden_out, grad_resid, grad_mixed_mine, grad_mixed_sent, ffn_gain_part, down_grad, feed_grads = feed(
        core, hidden_in.reshape(count, width), mixed_mine, mixed_got, output_weight, ffn_gain,
        cotangent.reshape(count, width), keep, (gate_weight, up_weight, down_weight), pieces,
    )
    head_grads = [a.reshape(rows, tokens, group_width) for a in (grad_mixed_mine, swap(grad_mixed_sent))]
    early_down = lax.psum_scatter(down_grad, "rows", scatter_dimension=0, tiled=True)[0]
    early_feed = lax.psum_scatter(feed_grads, "rows", scatter_dimension=0, tiled=True)[0]

    calls = [[(k, 0), (k, 1)] for k in range(steps - 1, 0, -1)]
    calls[-1].append((0, 1))
    calls.append([(0, 0)])
    state = kept = None
    pieces_in = []
    waiting = []
    passing = None
    now = queries

    def join(parts):
        total = parts[0].astype(f32) + parts[1].astype(f32)
        if passing is not None:
            total = total + passing.astype(f32)
        return total.astype(bf16)

    for i, items in enumerate(calls):
        if len(waiting) == 2:
            now, joined = lax.optimization_barrier((queries, join(waiting.pop(0))))
            passing = lax.ppermute(joined, "heads", down_chain)
        seg_list, base_list = pick(items)
        made = attend_back_part(
            now, head_grads, lse, head_mix, start, expanded, value_lift, key_lift_t, lo,
            seg_list, base_list, kept, state, len(items) == 1,
        )
        state = made[len(items) : len(items) + 2]
        if i == 0:
            *kept, value_part = made[len(items) + 2 :]
        k = items[0][0]
        if k == 0:
            pieces_in.append(made[0])
            continue
        waiting.append((made[0], flip(made[1], "heads", 0)))
        if k == 1:
            pieces_in.append(flip(made[2], "heads", 0))
    joined = join(waiting.pop())
    query_grads, key_part = made[1:]
    latent_grads = sum(p.astype(f32) for p in pieces_in)

    ff_share = gate_weight.shape[1] // peers
    full, hidden_grad = finish(
        (early_feed, early_down),
        ((ff_share, ff_share, share), (ff_share,)),
        peers,
        (
            hidden_in.reshape(count, width), attn_gain.reshape(1, width),
            query_grads.reshape(2, count, group_width), latent_grads.reshape(2, count, latent_size),
            joined.reshape(2, count, latent_size),
            query_weight, latent_weight, grad_resid, ffn_gain_part, key_part, value_part,
        ),
    )
    (
        gate_share, up_share, output_share, down_share, query_share, latent_share, key_share, value_share, gains,
        hidden_grad,
    ) = lay_out(full, hidden_grad, (ff_share, ff_share, share, ff_share), share, latent_size, group_width, peers, width)
    gains = lax.dynamic_slice_in_dim(gains, (place * share) % gains.shape[1], share, 1)
    return (
        hidden_out.reshape(rows, tokens, width),
        hidden_grad.reshape(rows, tokens, width),
        gains[0],
        query_share,
        latent_share,
        key_share,
        value_share,
        output_share,
        gains[1],
        gate_share.T,
        up_share.T,
        down_share,
    )


def solution(mesh):
    placed = (
        P("rows", "heads", None),
        P("rows", None),
        P("rows", "heads", None),
        P(),
        P(),
        P(),
        P(),
        P(),
        P(),
        P(),
        P(),
        P(),
        P(),
    )
    return jax.shard_map(
        shards,
        mesh=mesh,
        in_specs=placed,
        out_specs=(
            P("rows", "heads", None),
            P("rows", "heads", None),
            P("heads"),
            P("heads", None),
            P("heads", None),
            P(None, "heads", None),
            P(None, "heads", None),
            P("heads", None),
            P("heads"),
            P(None, "heads"),
            P(None, "heads"),
            P("heads", None),
        ),
        check_vma=False,
    )
```

```python
import functools
import math

import jax
import jax.numpy as jnp
from jax import lax
from jax.experimental import pallas as pl
from jax.experimental.pallas import tpu as pltpu
from jax.sharding import PartitionSpec as P

HEAD_WIDTH = 64
epsilon = 1e-05
blocked = -1e30
LOG2E = math.log2(math.e)
LN2 = math.log(2.0)
QUAD = 4
f32 = jnp.float32
bf16 = jnp.bfloat16


def matmul(left, right):
    return jnp.dot(left, right, preferred_element_type=f32)


def matmul_nt(left, right):
    return lax.dot_general(
        left, right, (((left.ndim - 1,), (right.ndim - 1,)), ((), ())), preferred_element_type=f32
    )


def matmul_tn(left, right):
    return lax.dot_general(left, right, (((0,), (0,)), ((), ())), preferred_element_type=f32)


def rms_inverse(value_matrix):
    return lax.rsqrt(jnp.mean(value_matrix * value_matrix, axis=-1, keepdims=True) + epsilon)


def expand_heads(source, weights, factor, out_ref):
    tokens = source.shape[0]
    quads, wide, deep = weights.shape
    latent = wide // QUAD
    for quad in range(quads):
        product = matmul_nt(weights[quad], source[:, quad * deep : (quad + 1) * deep])
        if factor != 1.0:
            product = product * factor
        product = product.astype(bf16)
        for h in range(QUAD):
            at = (quad * QUAD + h) * tokens
            out_ref[:, at : at + tokens] = product[h * latent : (h + 1) * latent]


def lift_heads(source, weights, tokens):
    parts = [
        matmul(weights[h], source[:, h * tokens : (h + 1) * tokens]) for h in range(weights.shape[0])
    ]
    return jnp.concatenate(parts, axis=0)


def lift_grad(left, right, tokens, out_ref):
    latent = left.shape[0]
    deep = QUAD * HEAD_WIDTH
    head = lax.broadcasted_iota(jnp.int32, (latent, deep), 1) // HEAD_WIDTH
    for quad in range(right.shape[1] // deep):
        columns = slice(quad * deep, (quad + 1) * deep)
        found = None
        for h in range(QUAD):
            at = (quad * QUAD + h) * tokens
            part = matmul(left[:, at : at + tokens], right[:, columns])
            found = part if h == 0 else jnp.where(head == h, part, found)
        out_ref[:, columns] += found


def seg_mask(base, own_base, start):
    tokens = start.shape[-1]
    key_at = lax.broadcasted_iota(jnp.int32, (tokens, tokens), 0)
    query_at = lax.broadcasted_iota(jnp.int32, (tokens, tokens), 1)
    return (key_at >= start - base) & (key_at <= query_at + (own_base - base))


def attend_kernel(count, first, last, lo, bases, *refs):
    refs = list(refs)
    take = lambda k: [refs.pop(0) for _ in range(k)]
    (start_ref,) = take(1)
    if first:
        query_ref, key_lift_ref = take(2)
    else:
        expanded_ref, top_in, total_in, mix_in = take(4)
    seg_refs = take(count)
    if last:
        (value_lift_ref,) = take(1)
        out_ref, lse_ref, mix_ref = take(3)
    else:
        top_out, total_out, mix_out = take(3)
    if first:
        (expanded_ref,) = take(1)
    top, total, mix, segs = take(4)
    expanded = expanded_ref.at[0]
    tokens = start_ref.shape[2]
    heads = expanded.shape[1] // tokens
    row = pl.program_id(0)
    touched = lambda i: (bases[i] >= 0) & (bases[i] + tokens - 1 >= lo[row])
    if first:
        expand_heads(query_ref[0], key_lift_ref, HEAD_WIDTH ** (-0.5) * LOG2E, expanded)
        top[...] = jnp.full_like(top, blocked)
        total[...] = jnp.zeros_like(total)
        mix[...] = jnp.zeros_like(mix)
    else:
        top[...] = top_in[0]
        total[...] = total_in[0]
        mix[...] = mix_in[0].astype(f32)
    for i in range(count):
        segs[i] = seg_refs[i][0]

    @pl.loop(0, count)
    def _(i):
        @pl.when(touched(i))
        def _():
            latent = segs[i]
            latent_t = latent.T
            allow = seg_mask(bases[i], bases[count], start_ref[0])
            for h in range(heads):
                at = slice(h * tokens, (h + 1) * tokens)
                score = jnp.where(allow, matmul(latent, expanded[:, at]), blocked)
                old = top[:, at]
                new = jnp.maximum(old, jnp.max(score, axis=0, keepdims=True))
                probs = jnp.exp2(score - new)
                fade = jnp.exp2(old - new)
                top[:, at] = new
                total[:, at] = total[:, at] * fade + jnp.sum(probs, axis=0, keepdims=True)
                mix[:, at] = mix[:, at] * fade + matmul(latent_t, probs.astype(bf16))

    if not last:
        top_out[0] = top[...]
        total_out[0] = total[...]
        mix_out[0] = mix[...].astype(bf16)
        return
    lse_ref[0] = top[...] + jnp.log2(total[...])
    mix_ref[0] = (mix[...] * (1.0 / total[...])).astype(bf16)
    out_ref[0] = lift_heads(mix_ref[0], value_lift_ref, tokens).T.astype(bf16)


def whole(array):
    return pl.BlockSpec(array.shape, lambda *_: (0,) * len(array.shape))


def by_row(shape):
    return pl.BlockSpec((1,) + tuple(shape[1:]), lambda r, *_: (r,) + (0,) * (len(shape) - 1))


def attend_part(queries, start, key_lift, value_lift_t, lo, segs, bases, expanded, state, last):
    rows, tokens, width = queries.shape
    heads = width // HEAD_WIDTH
    latent = segs[0].shape[-1]
    shape = jax.ShapeDtypeStruct
    stat = shape((rows, 1, heads * tokens), f32)
    flat = shape((rows, latent, heads * tokens), bf16)
    if state is None:
        args = [start, queries, key_lift, *segs]
        specs = [by_row(start.shape), by_row(queries.shape), whole(key_lift)]
    else:
        args = [start, expanded, *state, *segs]
        specs = [by_row(a.shape) for a in args[:5]]
    specs += [by_row(s.shape) for s in segs]
    if last:
        args.append(value_lift_t)
        specs.append(whole(value_lift_t))
        outs = [shape(queries.shape, bf16), stat, flat]
    else:
        outs = [stat, stat, flat]
    if state is None:
        outs.append(flat)
    blocks = rows * heads * len(segs)
    return pl.pallas_call(
        functools.partial(attend_kernel, len(segs), state is None, last),
        out_shape=outs,
        grid_spec=pltpu.PrefetchScalarGridSpec(
            num_scalar_prefetch=2,
            grid=(rows,),
            in_specs=specs,
            out_specs=[by_row(o.shape) for o in outs],
            scratch_shapes=[
                pltpu.VMEM((1, heads * tokens), f32),
                pltpu.VMEM((1, heads * tokens), f32),
                pltpu.VMEM((latent, heads * tokens), f32),
                pltpu.VMEM((len(segs), tokens, latent), bf16),
            ],
        ),
        compiler_params=pltpu.CompilerParams(
            dimension_semantics=("arbitrary",), vmem_limit_bytes=48 << 20
        ),
        cost_estimate=pl.CostEstimate(
            flops=blocks * tokens * tokens * latent * 64,
            bytes_accessed=rows * heads * latent * tokens * 64,
            transcendentals=blocks * tokens * tokens,
        ),
        name="attend",
    )(lo, bases, *args)


def attend_back_kernel(count, first, last, lo, bases, *refs):
    refs = list(refs)
    take = lambda k: [refs.pop(0) for _ in range(k)]
    query_ref, lse_ref, start_ref, expanded_ref, key_lift_t_ref = take(5)
    seg_refs = take(count)
    if first:
        grad_mine, grad_got, mix_ref, value_lift_ref = take(4)
    else:
        expanded_grad_ref, delta_ref, query_back_in, key_up_in = take(4)
    grad_refs = take(count)
    query_back_ref, key_up_ref = take(2)
    if first:
        expanded_grad_ref, delta_ref, value_up_ref = take(3)
    back, query_back, segs, seg_grads = take(4)
    expanded, expanded_grad = expanded_ref.at[0], expanded_grad_ref.at[0]
    tokens = query_ref.shape[1]
    heads = expanded.shape[1] // tokens
    row = pl.program_id(0)
    scale = HEAD_WIDTH ** (-0.5)
    touched = lambda i: (bases[i] >= 0) & (bases[i] + tokens - 1 >= lo[row])
    any_touched = functools.reduce(jnp.logical_or, [touched(i) for i in range(count)])

    @pl.when(row == 0)
    def _():
        key_up_ref[...] = jnp.zeros_like(key_up_ref) if first else key_up_in[...]
        if first:
            value_up_ref[...] = jnp.zeros_like(value_up_ref)

    query_back[...] = jnp.zeros_like(query_back) if first else query_back_in[0]
    seg_grads[...] = jnp.zeros_like(seg_grads)
    if first:
        grads = jnp.where(row < pl.num_programs(0) // 2, grad_mine[0], grad_got[0])
        expand_heads(grads, value_lift_ref, 1.0, expanded_grad)
        delta_ref[0] = jnp.sum(mix_ref[0].astype(f32) * expanded_grad[...].astype(f32), axis=0, keepdims=True)
        lift_grad(mix_ref[0], grads, tokens, value_up_ref)

    @pl.when(any_touched)
    def _():
        back[...] = jnp.zeros_like(back)
        for i in range(count):
            segs[i] = seg_refs[i][0]

    @pl.loop(0, count)
    def _(i):
        @pl.when(touched(i))
        def _():
            latent = segs[i]
            allow = seg_mask(bases[i], bases[count], start_ref[0])
            allow = jnp.concatenate([allow] * heads, axis=1)
            score = matmul(latent, expanded[...])
            probs = jnp.where(allow, jnp.exp2(score - lse_ref[0]), 0.0)
            dprobs = matmul(latent, expanded_grad[...])
            dscore = (probs * (dprobs - delta_ref[0])).astype(bf16)
            by_key = matmul_nt(dscore, expanded[...])
            by_value = matmul_nt(probs.astype(bf16), expanded_grad[...])
            seg_grads[i] = (by_key * LN2 + by_value).astype(bf16)
            back[...] += matmul(latent.T, dscore)

    for i in range(count):
        grad_refs[i][0] = seg_grads[i]

    @pl.when(any_touched)
    def _():
        part = (back[...] * scale).astype(bf16)
        query_back[...] += lift_heads(part, key_lift_t_ref, tokens)
        lift_grad(part, query_ref[0], tokens, key_up_ref)

    if last:
        query_back_ref[0] = query_back[...].T.astype(bf16)
    else:
        query_back_ref[0] = query_back[...]


def attend_back_part(queries, grads, lse, mix, start, expanded, value_lift, key_lift_t, lo, segs, bases, kept, state, last):
    rows, tokens, width = queries.shape
    heads = width // HEAD_WIDTH
    latent = segs[0].shape[-1]
    shape = jax.ShapeDtypeStruct
    back_shape = shape((rows, width, tokens), f32)
    up_shape = shape((latent, width), f32)
    first = state is None
    args = [queries, lse, start, expanded, key_lift_t, *segs]
    specs = [by_row(a.shape) for a in args[:4]] + [whole(key_lift_t)]
    specs += [by_row(s.shape) for s in segs]
    if first:
        args += [*grads, mix, value_lift]
        half = (1, tokens, width)
        specs.append(pl.BlockSpec(half, lambda r, *_: (jnp.minimum(r, rows // 2 - 1), 0, 0)))
        specs.append(pl.BlockSpec(half, lambda r, *_: (jnp.maximum(r - rows // 2, 0), 0, 0)))
        specs += [by_row(mix.shape), whole(value_lift)]
    else:
        args += [*kept, *state]
        specs += [by_row(kept[0].shape), by_row(kept[1].shape), by_row(back_shape.shape), whole(up_shape)]
    outs = [shape(s.shape, bf16) for s in segs]
    outs += [shape(queries.shape, bf16) if last else back_shape, up_shape]
    out_specs = [by_row(o.shape) for o in outs[:-1]] + [whole(up_shape)]
    if first:
        outs += [shape(expanded.shape, bf16), shape(lse.shape, f32), up_shape]
        out_specs += [by_row(expanded.shape), by_row(lse.shape), whole(up_shape)]
    blocks = rows * heads * len(segs)
    return pl.pallas_call(
        functools.partial(attend_back_kernel, len(segs), first, last),
        out_shape=outs,
        grid_spec=pltpu.PrefetchScalarGridSpec(
            num_scalar_prefetch=2,
            grid=(rows,),
            in_specs=specs,
            out_specs=out_specs,
            scratch_shapes=[
                pltpu.VMEM((latent, heads * tokens), f32),
                pltpu.VMEM((width, tokens), f32),
                pltpu.VMEM((len(segs), tokens, latent), bf16),
                pltpu.VMEM((len(segs), tokens, latent), bf16),
            ],
        ),
        compiler_params=pltpu.CompilerParams(
            dimension_semantics=("arbitrary",), vmem_limit_bytes=48 << 20
        ),
        cost_estimate=pl.CostEstimate(
            flops=blocks * tokens * tokens * latent,
            bytes_accessed=rows * heads * latent * tokens,
            transcendentals=0,
        ),
        name="attend_back",
    )(lo, bases, *args)


def quad_lift(lift):
    latent, width = lift.shape
    deep = QUAD * HEAD_WIDTH
    quads = width // deep
    tall = jnp.tile(lift.reshape(latent, quads, deep).transpose(1, 0, 2), (1, QUAD, 1))
    row_head = lax.broadcasted_iota(jnp.int32, tall.shape, 1) // latent
    column_head = lax.broadcasted_iota(jnp.int32, tall.shape, 2) // HEAD_WIDTH
    return jnp.where(row_head == column_head, tall, jnp.zeros_like(tall))


def head_lift(lift):
    latent, width = lift.shape
    return lift.T.reshape(width // HEAD_WIDTH, HEAD_WIDTH, latent)


def put_pieces(ref, value, at=0):
    pieces, _, piece = ref.shape
    for j in range(pieces):
        ref[j, pl.ds(at, value.shape[0])] = value[:, j * piece : (j + 1) * piece].astype(bf16)


def feed_kernel(core_ref, *refs):
    (
        inputs_ref, mine_ref, got_ref, output_ref, gain_ref, cotangent_ref, keep_ref,
        gate_ref, up_ref, down_ref,
        hidden_out_ref, resid_out, normed_out, back_out, active_ref, slope_ref, down_grad_ref,
        result, hidden, resid, normed, back, sems,
    ) = refs
    step = pl.program_id(0)
    leaving = [
        pltpu.make_async_copy(source, target, sems.at[i])
        for i, (source, target) in enumerate(((resid, resid_out), (normed, normed_out), (back, back_out)))
    ]
    count = inputs_ref.shape[0]
    block = min(256, count)
    core = core_ref[0]

    @pl.when(step == 0)
    def _():
        for t in range(0, count, block):
            at = slice(t, t + block)
            row = inputs_ref[at].astype(f32) + (
                matmul(mine_ref[at], output_ref[core]) + matmul(got_ref[at], output_ref[1 - core])
            )
            resid[at] = row
            scale = lax.rsqrt(jnp.mean(row * row, axis=-1, keepdims=True) + epsilon)
            normed[at] = (row * scale * gain_ref[...]).astype(bf16)
            back[at] = (cotangent_ref[at].astype(f32) * keep_ref[at]).astype(bf16)
        for copy in leaving:
            copy.start()
        result[...] = jnp.zeros_like(result)

    part = count // 4
    for t in range(0, count, part):
        at = slice(t, t + part)
        gate = matmul(normed[at], gate_ref[...])
        up = matmul(normed[at], up_ref[...])
        sigmoid = 1.0 / (1.0 + jnp.exp(-gate))
        active = gate * sigmoid
        hidden[at] = (active * up).astype(bf16)
        active_ref[at] = active.astype(bf16)
        slope_ref[at] = (up * (sigmoid * (1.0 + gate * (1.0 - sigmoid)))).astype(bf16)
    put_pieces(down_grad_ref, matmul_tn(hidden[...], back[...]))
    result[...] += matmul(hidden[...], down_ref[...])

    @pl.when(step == pl.num_programs(0) - 1)
    def _():
        hidden_out_ref[...] = (resid[...] + result[...]).astype(bf16)
        for copy in leaving:
            copy.wait()


def feed_back_kernel(core_ref, *refs):
    (
        mine_in, got_in, output_in, resid_in, gain_ref, normed, back,
        active_ref, slope_ref, gate_ref, up_ref, down_ref,
        grad_resid_out, head_mine_out, head_sent_out, gain_grad_ref, grads_ref,
        grad_two, both, low, staged, staged_out, mine_ref, got_ref, output_ref, resid_ref, head_mine_ref, head_sent_ref,
        sems, out_sem, in_sems, leave_sems,
    ) = refs
    step = pl.program_id(0)
    steps = pl.num_programs(0)
    count, width = resid_ref.shape
    coming = [
        pltpu.make_async_copy(source, target, in_sems.at[i])
        for i, (source, target) in enumerate(
            ((mine_in, mine_ref), (got_in, got_ref), (output_in, output_ref), (resid_in, resid_ref))
        )
    ]
    chunk = down_ref.shape[0]
    ff = (grads_ref.shape[1] - width) // 2
    block = min(256, count)
    core = core_ref[0]
    slot = step % 2

    def leave(at, kind, place):
        return pltpu.make_async_copy(
            staged.at[at, kind],
            grads_ref.at[:, pl.ds(pl.multiple_of(kind * ff + place * chunk, chunk), chunk)],
            sems.at[at, kind],
        )

    @pl.when(step >= 2)
    def _():
        for kind in range(2):
            leave(slot, kind, step - 2).wait()

    @pl.when(step == 0)
    def _():
        for copy in coming:
            copy.start()
        grad_two[...] = jnp.zeros_like(grad_two)

    part = count // 4
    for t in range(0, count, part):
        at = slice(t, t + part)
        grad_act = matmul_nt(back[at], down_ref[...])
        both[at, :chunk] = (grad_act * slope_ref[at].astype(f32)).astype(bf16)
        both[at, chunk:] = (grad_act * active_ref[at].astype(f32)).astype(bf16)
    for kind in range(2):
        put_pieces(staged.at[slot, kind], matmul_tn(both[:, kind * chunk : (kind + 1) * chunk], normed[...]))
        leave(slot, kind, step).start()
    weights = jnp.concatenate([gate_ref[...], up_ref[...]], axis=1)
    for t in range(0, count, part):
        at = slice(t, t + part)
        grad_two[at] += matmul_nt(both[at], weights)

    @pl.when(step == steps - 1)
    def _():
        for copy in coming:
            copy.wait()
        gain_total = jnp.zeros((1, width), f32)
        leaving = []
        for t in range(0, count, block):
            at = slice(t, t + block)
            row = resid_ref[at]
            scale = lax.rsqrt(jnp.mean(row * row, axis=-1, keepdims=True) + epsilon)
            unit = row * scale
            grad = grad_two[at]
            gain_total += jnp.sum(grad * unit, axis=0, keepdims=True)
            scaled = grad * gain_ref[...]
            grad = back[at].astype(f32) + scale * (
                scaled - unit * jnp.mean(scaled * unit, axis=-1, keepdims=True)
            )
            grad_two[at] = grad
            low[at] = grad.astype(bf16)
            head_mine_ref[at] = matmul_nt(low[at], output_ref[core]).astype(bf16)
            head_sent_ref[at] = matmul_nt(low[at], output_ref[1 - core]).astype(bf16)
            for i, (source, target) in enumerate(
                ((grad_two, grad_resid_out), (head_mine_ref, head_mine_out), (head_sent_ref, head_sent_out))
            ):
                rows = pl.ds(t, block)
                copy = pltpu.make_async_copy(source.at[rows], target.at[rows], leave_sems.at[t // block, i])
                copy.start()
                leaving.append(copy)
        gain_grad_ref[...] = gain_total
        half = mine_ref.shape[1]
        put_pieces(staged_out, matmul_tn(mine_ref[...], low[...]), core * half)
        put_pieces(staged_out, matmul_tn(got_ref[...], low[...]), (1 - core) * half)
        last = pltpu.make_async_copy(staged_out, grads_ref.at[:, pl.ds(2 * ff, width)], out_sem)
        last.start()
        for kind in range(2):
            leave(1 - slot, kind, step - 1).wait()
            leave(slot, kind, step).wait()
        last.wait()
        for copy in leaving:
            copy.wait()


def once(array):
    return pl.BlockSpec(array.shape, lambda *_: (0,) * len(array.shape), pipeline_mode=pl.Buffered(1))


def feed(core, inputs, mixed_mine, mixed_got, output_weight, gain, cotangent, keep, weights, pieces):
    count, width = inputs.shape
    gate_weight, up_weight, down_weight = weights
    ff = gate_weight.shape[1]
    chunk = 256
    piece = width // pieces
    output_weight = output_weight.reshape(2, -1, width)
    gain = gain.reshape(1, width)
    by_rows = pl.BlockSpec((chunk, width), lambda c, *_: (c, 0))
    by_columns = pl.BlockSpec((width, chunk), lambda c, *_: (0, c))
    kept_columns = pl.BlockSpec((count, chunk), lambda c, *_: (0, c))
    shape = jax.ShapeDtypeStruct
    params = pltpu.CompilerParams(dimension_semantics=("arbitrary",), vmem_limit_bytes=60 << 20)
    full_bf, full_f = shape((count, width), bf16), shape((count, width), f32)
    kept = shape((count, ff), bf16)
    firsts = [inputs, mixed_mine, mixed_got, output_weight, gain, cotangent, keep]
    outs = [full_bf, full_f, full_bf, full_bf, kept, kept, shape((pieces, ff, piece), bf16)]
    hidden_out, resid, normed, back, active, slope, down_grad = pl.pallas_call(
        feed_kernel,
        out_shape=outs,
        grid_spec=pltpu.PrefetchScalarGridSpec(
            num_scalar_prefetch=1,
            grid=(ff // chunk,),
            in_specs=[once(a) for a in firsts] + [by_columns, by_columns, by_rows],
            out_specs=[once(outs[0])]
            + [pl.BlockSpec(memory_space=pl.ANY)] * 3
            + [kept_columns, kept_columns, pl.BlockSpec((pieces, chunk, piece), lambda c, *_: (0, c, 0))],
            scratch_shapes=[
                pltpu.VMEM((count, width), f32),
                pltpu.VMEM((count, chunk), bf16),
                pltpu.VMEM((count, width), f32),
                pltpu.VMEM((count, width), bf16),
                pltpu.VMEM((count, width), bf16),
                pltpu.SemaphoreType.DMA((3,)),
            ],
        ),
        compiler_params=params,
        cost_estimate=pl.CostEstimate(
            flops=count * width * (ff * 8 + width * 2),
            bytes_accessed=width * ff * 8 + count * width * 16 + count * ff * 4,
            transcendentals=count * ff,
        ),
        name="feed",
    )(core.reshape(1), *firsts, *weights)
    firsts = [mixed_mine, mixed_got, output_weight, resid, gain, normed, back]
    anywhere = pl.BlockSpec(memory_space=pl.ANY)
    outs = [
        full_f,
        shape(mixed_mine.shape, bf16),
        shape(mixed_mine.shape, bf16),
        shape((1, width), f32),
        shape((pieces, 2 * ff + width, piece), bf16),
    ]
    grad_resid, head_mine, head_sent, gain_grad, grads = pl.pallas_call(
        feed_back_kernel,
        out_shape=outs,
        grid_spec=pltpu.PrefetchScalarGridSpec(
            num_scalar_prefetch=1,
            grid=(ff // chunk,),
            in_specs=[anywhere] * 4
            + [once(a) for a in firsts[4:]]
            + [kept_columns, kept_columns, by_columns, by_columns, by_rows],
            out_specs=[anywhere] * 3 + [once(outs[3]), anywhere],
            scratch_shapes=[
                pltpu.VMEM((count, width), f32),
                pltpu.VMEM((count, 2 * chunk), bf16),
                pltpu.VMEM((count, width), bf16),
                pltpu.VMEM((2, 2, pieces, chunk, piece), bf16),
                pltpu.VMEM((pieces, width, piece), bf16),
                pltpu.VMEM(mixed_mine.shape, bf16),
                pltpu.VMEM(mixed_mine.shape, bf16),
                pltpu.VMEM(output_weight.shape, bf16),
                pltpu.VMEM((count, width), f32),
                pltpu.VMEM(mixed_mine.shape, bf16),
                pltpu.VMEM(mixed_mine.shape, bf16),
                pltpu.SemaphoreType.DMA((2, 2)),
                pltpu.SemaphoreType.DMA,
                pltpu.SemaphoreType.DMA((4,)),
                pltpu.SemaphoreType.DMA((max(1, count // 256), 3)),
            ],
        ),
        compiler_params=params,
        cost_estimate=pl.CostEstimate(
            flops=count * width * (ff * 10 + width * 4),
            bytes_accessed=width * ff * 10 + count * width * 20 + count * ff * 4,
            transcendentals=0,
        ),
        name="feed_back",
    )(core.reshape(1), *firsts, active, slope, *weights)
    return hidden_out, grad_resid, head_mine, head_sent, gain_grad, down_grad, grads


def flip(array, axis, bit):
    size = lax.axis_size(axis)
    return lax.ppermute(array, axis, [(i, i ^ (1 << bit)) for i in range(size)])


def fill_shards(target, at, grad, count):
    along, piece = target.shape[0], target.shape[3]
    size = grad.shape[0] // count
    for s in range(count):
        for j in range(along):
            target[j, s, at : at + size] = grad[s * size : (s + 1) * size, j * piece : (j + 1) * piece].astype(bf16)


def fill_folded(target, at, grad, count):
    along, piece = target.shape[0], target.shape[3]
    size = grad.shape[0] // count
    latent = grad.shape[1]
    fold = size // 2
    for s in range(count):
        for j in range(along):
            side, column = divmod(j * piece, latent)
            first = s * size + side * fold
            target[j, s, at : at + fold] = grad[first : first + fold, column : column + piece].astype(bf16)


def fill_gains(target, at, gain, count):
    along, piece = target.shape[0], target.shape[3]
    share = gain.shape[1] // count
    lane = max(share, 128)
    for s in range(count):
        begin = s * share // lane * lane
        kept = jnp.broadcast_to(gain[:, begin : begin + lane], (16, lane)).astype(bf16)
        target[0, s, at : at + 16, :lane] = kept
        if piece > lane:
            target[0, s, at : at + 16, lane:] = jnp.zeros((16, piece - lane), bf16)
        for j in range(1, along):
            target[j, s, at : at + 16] = jnp.zeros((16, piece), bf16)


def finish_kernel(sections, groups, sizes, refs, loads, grad_copy):
    (
        early_refs, inputs_ref, gain_ref, query_grad_ref, latent_grad_ref, joined_ref,
        query_ref, latent_ref, resid_ref, other_gain_ref, key_up, value_up,
        out_ref, grad_ref,
        normed, own_ref, sent_ref, late_got, late_from, got_first, got_next,
        chain_got, query_got, latent_low, latent_got,
        chain_sems, core_sems, along_sems, first_sems, first_late_sems, next_sems, out_sems,
    ) = refs
    along, count, late_rows, piece = own_ref.shape
    early_rows, share, fold, lift = sizes
    early_loads, late_loads = loads

    def here(*which):
        for i in which:
            late_loads[i].wait()

    for copy in [late_loads[4], late_loads[2], *early_loads, late_loads[0], late_loads[1]]:
        copy.start()
    for i in (9, 10, 3, 5, 6, 7, 8):
        late_loads[i].start()
    bits = count.bit_length() - 1
    row_at = lax.axis_index("rows")
    place = lax.axis_index("heads")
    core = row_at % 2
    x_at = row_at // 2
    mesh = pl.DeviceIdType.MESH
    tokens, width = inputs_ref.shape
    latent = latent_low.shape[2]
    half = query_got.shape[1]
    block = min(256, tokens)
    parts = [slice(0, early_rows)] + [slice(early_rows + g[0], early_rows + g[1]) for g in groups]

    def turned(which):
        at = place
        for bit in which:
            at = at + (1 << bit) * (1 - 2 * ((place // (1 << bit)) % 2))
        return at

    core_peer = (row_at + 1 - 2 * core, place)
    x_others = [(x_at + d) % along for d in range(1, along)]
    x_peers = [(x * 2 + core, place) for x in x_others]
    head_peers = [(row_at, turned([bit])) for bit in range(bits)]
    above = (row_at, (place + 2) % count)
    below = (row_at, (place + count - 2) % count)
    barrier = pltpu.get_barrier_semaphore()
    everyone = [core_peer, above, below] + x_peers + head_peers
    for peer in everyone:
        pl.semaphore_signal(barrier, inc=1, device_id=peer, device_id_type=mesh)
    pl.semaphore_wait(barrier, len(everyone))

    def remote(source, target, sems, index, peer):
        return pltpu.make_async_remote_copy(
            src_ref=source, dst_ref=target, send_sem=sems.at[(0,) + index], recv_sem=sems.at[(1,) + index],
            device_id=peer, device_id_type=mesh,
        )

    def orders(bit):
        rest = list(range(bit + 1, bits))
        return [
            [b for i, b in enumerate(rest) if not (mask >> (len(rest) - 1 - i)) & 1]
            for mask in range(1 << len(rest))
        ]

    def add_rows(target, other, size):
        step = size if size <= 600 else size // 2

        def one(i, carry):
            at = pl.ds(pl.multiple_of(i * step, 16), step)
            target[at] = (target[at].astype(f32) + other[at].astype(f32)).astype(bf16)
            return carry

        lax.fori_loop(0, size // step, one, 0)

    def rows_of(part):
        return pl.ds(part.start, part.stop - part.start)

    first = orders(0)
    final = len(first) - 1
    pending = []

    def early_rows_of(n, shard):
        which, start, size, _ = sections[n]
        return early_refs[which].at[pl.ds(pl.multiple_of(start + shard * size, 16), size)]

    def first_early(i, n):
        _, _, size, row = sections[n]
        return remote(
            early_rows_of(n, turned([0] + first[i])), got_first.at[i, pl.ds(row, size)],
            first_sems, (i, n), head_peers[0],
        )

    def next_copy(bit, j, i, which):
        rows = rows_of(parts[which])
        return remote(
            got_first.at[i, rows], got_next[bit - 1].at[j, rows], next_sems[bit - 1], (j, which), head_peers[bit]
        )

    def settle(i, which):
        rest = first[i]
        level = rest[0] if rest else bits
        rows = rows_of(parts[which])
        for bit in range(1, level):
            j = orders(bit).index(rest)
            next_copy(bit, j, i, which).wait_recv()
            add_rows(got_first.at[i, rows], got_next[bit - 1].at[j, rows], rows.size)
        if rest:
            copy = next_copy(level, orders(level).index(rest[1:]), i, which)
            copy.start()
            pending.append(copy)

    def early_step(i):
        for n, (_, _, size, row) in enumerate(sections):
            first_early(i, n).wait()
            add_rows(got_first.at[i, pl.ds(row, size)], early_rows_of(n, turned(first[i])), size)
        settle(i, 0)

    def core_copy(g):
        _, _, begin, end = groups[g]
        rows = pl.ds(begin, end - begin)
        return remote(sent_ref.at[:, :, rows], late_got.at[:, :, rows], core_sems, (g,), core_peer)

    def x_copies(g):
        low, high, begin, end = groups[g]
        shared = end - begin
        copies = []
        for d, (x, peer) in enumerate(zip(x_others, x_peers)):
            copies.append(
                remote(
                    late_got.at[x, :, pl.ds(begin, shared)], late_from.at[d, :, pl.ds(low, shared)],
                    along_sems, (d, g, 0), peer,
                )
            )
            if low + shared < high:
                rows = pl.ds(low + shared, high - low - shared)
                copies.append(
                    remote(own_ref.at[x, :, rows], late_from.at[d, :, rows], along_sems, (d, g, 1), peer)
                )
        return copies

    def along_x(g):
        low, _, begin, end = groups[g]
        core_copy(g).wait()

        def core_add(i, carry):
            j, s = i // count, i % count
            mine = own_ref[j, s, low : low + end - begin].astype(f32)
            late_got[j, s, begin:end] = (mine + late_got[j, s, begin:end].astype(f32)).astype(bf16)
            return carry

        lax.fori_loop(0, along * count, core_add, 0)
        for copy in x_copies(g):
            copy.start()

    def first_late(i, g):
        low, high, _, _ = groups[g]
        return remote(
            late_from.at[0, turned([0] + first[i]), pl.ds(low, high - low)],
            got_first.at[i, rows_of(parts[1 + g])], first_late_sems, (i, g), head_peers[0],
        )

    def over_heads(g):
        low, high, begin, end = groups[g]
        middle = low + end - begin
        for copy in x_copies(g):
            copy.wait()

        def x_add(s, carry):
            total = late_got[x_at, s, begin:end].astype(f32)
            for d in range(along - 1):
                total = total + late_from[d, s, low:middle].astype(f32)
            late_from[0, s, low:middle] = total.astype(bf16)
            if middle < high:
                total = own_ref[x_at, s, middle:high].astype(f32)
                for d in range(along - 1):
                    total = total + late_from[d, s, middle:high].astype(f32)
                late_from[0, s, middle:high] = total.astype(bf16)
            return carry

        lax.fori_loop(0, count, x_add, 0)
        for i in range(len(first)):
            first_late(i, g).start()

    def late_step(i, g):
        low, high, _, _ = groups[g]
        first_late(i, g).wait()
        add_rows(
            got_first.at[i, rows_of(parts[1 + g])],
            late_from.at[0, turned(first[i]), pl.ds(low, high - low)],
            high - low,
        )
        settle(i, 1 + g)

    mine = lambda ref, size: ref[:, pl.ds(pl.multiple_of(core * size, size), size)]
    theirs = lambda ref, size: ref[:, pl.ds(pl.multiple_of((1 - core) * size, size), size)]
    here(4, 2)
    chain_copy = remote(joined_ref, chain_got, chain_sems, (0,), below)
    chain_copy.start()
    query_copy = remote(query_grad_ref.at[1], query_got, chain_sems, (1,), core_peer)
    query_copy.start()
    for copy in early_loads:
        copy.wait()
    for i in range(len(first)):
        for n in range(len(sections)):
            first_early(i, n).start()

    here(0, 1)

    @pl.loop(0, tokens // block)
    def _(t):
        at = pl.ds(pl.multiple_of(t * block, block), block)
        row = inputs_ref[at].astype(f32)
        scale = lax.rsqrt(jnp.mean(row * row, axis=-1, keepdims=True) + epsilon)
        normed[at] = (row * scale * gain_ref[...]).astype(bf16)

    fill_shards(own_ref, 0, matmul_tn(normed[...], query_grad_ref[0]), count)
    here(9, 10)
    fill_shards(own_ref, share, key_up[...], count)
    fill_shards(own_ref, share + lift, value_up[...], count)
    query_copy.wait()
    fill_shards(sent_ref, 0, matmul_tn(normed[...], query_got[...]), count)
    core_copy(0).start()
    early_step(0)
    along_x(0)
    for i in range(1, len(first) // 2):
        early_step(i)

    here(3)
    chain_copy.wait()
    for side in (1, 0):
        for t in range(0, tokens, block):
            at = slice(t, t + block)
            latent_low[side, at] = (latent_grad_ref[side, at] + chain_got[side, at].astype(f32)).astype(bf16)
        if side == 1:
            latent_copy = remote(latent_low.at[1], latent_got, chain_sems, (2,), core_peer)
            latent_copy.start()
    latent_copy.wait()

    def back(t, gain_total):
        at = pl.ds(pl.multiple_of(t * block, block), block)
        row = inputs_ref[at].astype(f32)
        scale = lax.rsqrt(jnp.mean(row * row, axis=-1, keepdims=True) + epsilon)
        unit = row * scale
        grad = (
            matmul_nt(query_grad_ref[0, at], mine(query_ref, half))
            + matmul_nt(query_got[at], theirs(query_ref, half))
            + matmul_nt(latent_low[0, at], mine(latent_ref, latent))
            + matmul_nt(latent_got[at], theirs(latent_ref, latent))
        )
        scaled = grad * gain_ref[...]
        grad_ref[at] = resid_ref[at] + scale * (
            scaled - unit * jnp.mean(scaled * unit, axis=-1, keepdims=True)
        )
        return gain_total + jnp.sum(grad * unit, axis=0, keepdims=True)

    here(5, 6, 7, 8)
    gain_total = lax.fori_loop(0, tokens // block, back, jnp.zeros((1, width), f32))
    grad_copy.start()
    other = other_gain_ref[...]
    low = groups[1][0]
    for target, at, latents, gain in (
        (own_ref, low, latent_low[0], jnp.where(core == 0, gain_total, other)),
        (sent_ref, groups[1][2], latent_got[...], jnp.where(core == 0, other, gain_total)),
    ):
        fill_folded(target, at, matmul_tn(normed[...], latents), count)
        fill_gains(target, at + fold, gain, count)
    core_copy(1).start()
    over_heads(0)
    along_x(1)
    for i in range(max(1, len(first) // 2), final):
        early_step(i)
    over_heads(1)
    for i in range(final):
        for g in range(len(groups)):
            late_step(i, g)

    def spread(which):
        rows = rows_of(parts[which])
        out_ref[row_at, rows] = got_first[final, rows]
        copies = [remote(out_ref.at[row_at, rows], out_ref.at[row_at, rows], out_sems, (which, 0), core_peer)]
        for d, peer in enumerate(x_peers):
            copies.append(
                remote(out_ref.at[row_at, rows], out_ref.at[row_at, rows], out_sems, (which, 1 + d), peer)
            )
        for copy in copies:
            copy.start()
        return copies

    def pass_on(which, copies):
        rows = rows_of(parts[which])
        more = []
        for d in range(along - 1):
            copies[1 + d].wait_recv()
            source = ((x_at + along - 1 - d) % along) * 2 + core
            more.append(
                remote(
                    out_ref.at[source, rows], out_ref.at[source, rows], out_sems, (which, along + d), core_peer
                )
            )
            more[-1].start()
        return more

    early_step(final)
    spreads = [spread(0)]
    for g in range(len(groups)):
        late_step(final, g)
        spreads.append(spread(1 + g))
    passes = [pass_on(which, copies) for which, copies in enumerate(spreads)]
    for copies, more in zip(spreads, passes):
        copies[0].wait()
        for copy in copies[1:]:
            copy.wait_send()
        for copy in more:
            copy.wait()
    for copy in pending:
        copy.wait_send()
    grad_copy.wait()


def finish(early, shares, count, late_args):
    inputs, _, query_grads, latent_grads = late_args[:4]
    tokens, width = inputs.shape
    latent = latent_grads.shape[2]
    piece = early[0].shape[1]
    along = width // piece // 2
    share = width // count
    fold, lift = share // 2, latent // count
    bits = count.bit_length() - 1
    groups = [
        (0, share + 2 * lift, 0, share),
        (share + 2 * lift, share + 2 * lift + fold + 16, share, share + fold + 16),
    ]
    late_rows, shared_rows = groups[1][1], groups[1][3]
    sections = []
    row = 0
    for which, of_one in enumerate(shares):
        start = 0
        for size in of_one:
            sections.append((which, start, size, row))
            start += size * count
            row += size
    total = row + late_rows
    vmem = pl.BlockSpec(memory_space=pltpu.VMEM)
    dma = pltpu.SemaphoreType.DMA
    anywhere = pl.BlockSpec(memory_space=pl.ANY)

    def body(*refs):
        refs = list(refs)
        take = lambda k: [refs.pop(0) for _ in range(k)]
        early_in, late_in = take(len(early)), take(len(late_args))
        out_ref, grad_out = take(2)
        early_here, late_here = take(len(early)), take(len(late_args))
        grad_here, load_sems, grad_sem = take(3)
        loads = [
            pltpu.make_async_copy(source, target, load_sems.at[i])
            for i, (source, target) in enumerate(zip(early_in + late_in, early_here + late_here))
        ]
        given = [early_here] + late_here + [out_ref, grad_here]
        given += take(6) + [take(bits - 1)] + take(4) + take(5) + [take(bits - 1)] + take(1)
        finish_kernel(
            sections, groups, (row, share, fold, lift), given, (loads[: len(early)], loads[len(early) :]),
            pltpu.make_async_copy(grad_here, grad_out, grad_sem),
        )

    return pl.pallas_call(
        body,
        out_shape=[
            jax.ShapeDtypeStruct((2 * along, total, piece), bf16),
            jax.ShapeDtypeStruct((tokens, width), f32),
        ],
        in_specs=[anywhere] * (len(early) + len(late_args)),
        out_specs=[vmem, anywhere],
        scratch_shapes=[pltpu.VMEM(a.shape, a.dtype) for a in (*early, *late_args)]
        + [
            pltpu.VMEM((tokens, width), f32),
            dma((len(early) + len(late_args),)),
            dma,
            pltpu.VMEM((tokens, width), bf16),
            pltpu.VMEM((along, count, late_rows, piece), bf16),
            pltpu.VMEM((along, count, shared_rows, piece), bf16),
            pltpu.VMEM((along, count, shared_rows, piece), bf16),
            pltpu.VMEM((along - 1, count, late_rows, piece), bf16),
            pltpu.VMEM((count // 2, total, piece), bf16),
        ]
        + [pltpu.VMEM((count >> (bit + 1), total, piece), bf16) for bit in range(1, bits)]
        + [
            pltpu.VMEM((2, tokens, latent), bf16),
            pltpu.VMEM(query_grads.shape[1:], bf16),
            pltpu.VMEM((2, tokens, latent), bf16),
            pltpu.VMEM((tokens, latent), bf16),
            dma((2, 3)),
            dma((2, 2)),
            dma((2, along - 1, 2, 2)),
            dma((2, count // 2, len(sections))),
            dma((2, count // 2, 2)),
        ]
        + [dma((2, count >> (bit + 1), 3)) for bit in range(1, bits)]
        + [dma((2, 3, 2 * along))],
        compiler_params=pltpu.CompilerParams(
            collective_id=0, has_side_effects=True, vmem_limit_bytes=60 << 20
        ),
        name="finish",
    )(*early, *late_args)


def lay_out_kernel(
    rows, latent, full_ref, grad_in, gate_ref, up_ref, output_ref, down_ref, query_ref, latent_ref, key_ref, value_ref,
    gains_ref, grad_out, held, sems,
):
    size = grad_in.shape[0] // 4
    rows_at = [pl.ds(i * size, size) for i in range(4)]
    coming = [pltpu.make_async_copy(grad_in.at[at], held.at[at], sems.at[0, i]) for i, at in enumerate(rows_at)]
    going = [pltpu.make_async_copy(held.at[at], grad_out.at[at], sems.at[1, i]) for i, at in enumerate(rows_at)]
    for copy in coming:
        copy.start()
    pieces, _, piece = full_ref.shape
    at = 0
    for ref, size in zip((gate_ref, up_ref, output_ref, down_ref), rows):
        for j in range(pieces):
            ref[:, j * piece : (j + 1) * piece] = full_ref[j, at : at + size].astype(f32)
        at += size
    for before, after in zip(coming, going):
        before.wait()
        after.start()
    share = query_ref.shape[0]
    fold = share // 2
    lift = key_ref.shape[1]
    half = key_ref.shape[2]
    lane = gains_ref.shape[1]
    for j in range(pieces):
        x, core = divmod(j, 2)
        row = at
        query_ref[:, core * half + x * piece : core * half + (x + 1) * piece] = full_ref[
            j, row : row + share
        ].astype(f32)
        row += share
        for ref in (key_ref, value_ref):
            ref[core, :, x * piece : (x + 1) * piece] = full_ref[j, row : row + lift].astype(f32)
            row += lift
        side, column = divmod(x * piece, latent)
        column += core * latent
        latent_ref[side * fold : (side + 1) * fold, column : column + piece] = full_ref[
            j, row : row + fold
        ].astype(f32)
        row += fold
        if x == 0:
            gains_ref[core : core + 1] = full_ref[j, row : row + 16, :lane].astype(f32)[:1]
    for copy in going:
        copy.wait()


def lay_out(full, grad, rows, share, latent, half, count, width):
    shape = jax.ShapeDtypeStruct
    gate, up, output, down = rows
    lift = latent // count
    vmem = pl.BlockSpec(memory_space=pltpu.VMEM)
    outs = [
        shape((gate, width), f32),
        shape((up, width), f32),
        shape((output, width), f32),
        shape((down, width), f32),
        shape((share, width), f32),
        shape((share, 2 * latent), f32),
        shape((2, lift, half), f32),
        shape((2, lift, half), f32),
        shape((2, max(share, 128)), f32),
        shape(grad.shape, f32),
    ]
    anywhere = pl.BlockSpec(memory_space=pl.ANY)
    return pl.pallas_call(
        functools.partial(lay_out_kernel, rows, latent),
        out_shape=outs,
        in_specs=[vmem, anywhere],
        out_specs=[vmem] * (len(outs) - 1) + [anywhere],
        scratch_shapes=[pltpu.VMEM(grad.shape, f32), pltpu.SemaphoreType.DMA((2, 4))],
        compiler_params=pltpu.CompilerParams(vmem_limit_bytes=48 << 20),
        name="lay_out",
    )(full, grad)


def shards(
    hidden_in,
    doc_ids,
    cotangent,
    attn_gain,
    query_weight,
    latent_weight,
    key_lift_weight,
    value_lift_weight,
    output_weight,
    ffn_gain,
    gate_weight,
    up_weight,
    down_weight,
):
    rows, tokens, width = hidden_in.shape
    peers = lax.axis_size("heads")
    place = lax.axis_index("heads")
    core = lax.axis_index("rows") & 1
    groups, latent_size, group_width = key_lift_weight.shape
    count = rows * tokens
    steps = peers // 2
    pieces = lax.axis_size("rows")
    share = width // peers
    side = place & 1
    level = place // 2
    swap = lambda a: flip(a, "rows", 0)
    mine = lambda a, axis: lax.dynamic_slice_in_dim(a, core * (a.shape[axis] // 2), a.shape[axis] // 2, axis)
    theirs = lambda a, axis: lax.dynamic_slice_in_dim(
        a, (1 - core) * (a.shape[axis] // 2), a.shape[axis] // 2, axis
    )

    own_base = place * tokens
    own_docs = lax.dynamic_slice_in_dim(doc_ids, own_base, tokens, 1)
    position = own_base + jnp.arange(tokens, dtype=jnp.int32)
    before = (doc_ids[:, None, :] == own_docs[:, :, None]) & (
        jnp.arange(doc_ids.shape[1], dtype=jnp.int32)[None, None, :] <= position[None, :, None]
    )
    own_start = position[None, :] + 1 - jnp.sum(before.astype(jnp.int32), axis=-1)
    start = jnp.concatenate([own_start, swap(own_start)], axis=0)
    lo = start[:, 0]
    start = start[:, None, :]

    inputs = hidden_in.reshape(count, width).astype(f32)
    inverse_one = rms_inverse(inputs)
    normed_one = (inputs * inverse_one * attn_gain).astype(bf16)
    latent_mine = matmul(normed_one, mine(latent_weight, 1)).astype(bf16)
    latent_sent = matmul(normed_one, theirs(latent_weight, 1)).astype(bf16)
    latent_got = swap(latent_sent)
    own_seg = jnp.concatenate([latent_mine, latent_got], axis=0).reshape(2 * rows, tokens, latent_size)
    query_mine = matmul(normed_one, mine(query_weight, 1)).astype(bf16)
    query_sent = matmul(normed_one, theirs(query_weight, 1)).astype(bf16)
    queries = jnp.concatenate([query_mine, swap(query_sent)], axis=0).reshape(2 * rows, tokens, group_width)

    key_mine = lax.dynamic_index_in_dim(key_lift_weight, core, 0, keepdims=False)
    value_mine = lax.dynamic_index_in_dim(value_lift_weight, core, 0, keepdims=False)
    key_lift = quad_lift(key_mine)
    value_lift = quad_lift(value_mine)
    key_lift_t = head_lift(key_mine)
    value_lift_t = head_lift(value_mine)

    up_chain = [(i, i + 2) for i in range(peers - 2)]
    down_chain = [(i + 2, i) for i in range(peers - 2)]
    segs = []
    bases = []
    moving = own_seg
    for k in range(steps):
        if k > 0:
            moving = lax.ppermute(moving, "heads", up_chain)
            moving, crossed = lax.optimization_barrier((moving, segs[-1][1]))
            segs[-1] = (segs[-1][0], crossed)
        segs.append((moving, flip(moving, "heads", 0)))
        base = ((level - k) * 2 + side) * tokens
        other = ((level - k) * 2 + 1 - side) * tokens
        there = level >= k
        bases.append(
            (jnp.where(there, base, -1), jnp.where(there & (other < own_base), other, -1))
        )

    def pick(items):
        return (
            [segs[k][j] for k, j in items],
            jnp.stack([bases[k][j] for k, j in items] + [own_base]).astype(jnp.int32),
        )

    parts = [p for p in (range(0, 2), range(2, steps - 1), range(steps - 1, steps)) if len(p) > 0]
    state = expanded = None
    for i, ks in enumerate(parts):
        seg_list, base_list = pick([(k, j) for k in ks for j in range(2)])
        made = attend_part(
            queries, start, key_lift, value_lift_t, lo, seg_list, base_list, expanded, state, i == len(parts) - 1
        )
        state = made[:3]
        if i == 0:
            expanded = made[3]
    head_out, lse, head_mix = state
    mixed_mine = head_out[:rows].reshape(count, group_width)
    mixed_got = swap(head_out[rows:]).reshape(count, group_width)
    keep = (own_docs != 0).astype(f32).reshape(count, 1)
    hidden_out, grad_resid, grad_mixed_mine, grad_mixed_sent, ffn_gain_part, down_grad, feed_grads = feed(
        core, hidden_in.reshape(count, width), mixed_mine, mixed_got, output_weight, ffn_gain,
        cotangent.reshape(count, width), keep, (gate_weight, up_weight, down_weight), pieces,
    )
    head_grads = [a.reshape(rows, tokens, group_width) for a in (grad_mixed_mine, swap(grad_mixed_sent))]
    early_down = lax.psum_scatter(down_grad, "rows", scatter_dimension=0, tiled=True)[0]
    early_feed = lax.psum_scatter(feed_grads, "rows", scatter_dimension=0, tiled=True)[0]

    calls = [[(k, 0), (k, 1)] for k in range(steps - 1, 0, -1)]
    calls[-1].append((0, 1))
    calls.append([(0, 0)])
    state = kept = None
    pieces_in = []
    waiting = []
    passing = None
    now = queries

    def join(parts):
        total = parts[0].astype(f32) + parts[1].astype(f32)
        if passing is not None:
            total = total + passing.astype(f32)
        return total.astype(bf16)

    for i, items in enumerate(calls):
        if len(waiting) == 2:
            now, joined = lax.optimization_barrier((queries, join(waiting.pop(0))))
            passing = lax.ppermute(joined, "heads", down_chain)
        seg_list, base_list = pick(items)
        made = attend_back_part(
            now, head_grads, lse, head_mix, start, expanded, value_lift, key_lift_t, lo,
            seg_list, base_list, kept, state, len(items) == 1,
        )
        state = made[len(items) : len(items) + 2]
        if i == 0:
            *kept, value_part = made[len(items) + 2 :]
        k = items[0][0]
        if k == 0:
            pieces_in.append(made[0])
            continue
        waiting.append((made[0], flip(made[1], "heads", 0)))
        if k == 1:
            pieces_in.append(flip(made[2], "heads", 0))
    joined = join(waiting.pop())
    query_grads, key_part = made[1:]
    latent_grads = sum(p.astype(f32) for p in pieces_in)

    ff_share = gate_weight.shape[1] // peers
    full, hidden_grad = finish(
        (early_feed, early_down),
        ((ff_share, ff_share, share), (ff_share,)),
        peers,
        (
            hidden_in.reshape(count, width), attn_gain.reshape(1, width),
            query_grads.reshape(2, count, group_width), latent_grads.reshape(2, count, latent_size),
            joined.reshape(2, count, latent_size),
            query_weight, latent_weight, grad_resid, ffn_gain_part, key_part, value_part,
        ),
    )
    (
        gate_share, up_share, output_share, down_share, query_share, latent_share, key_share, value_share, gains,
        hidden_grad,
    ) = lay_out(full, hidden_grad, (ff_share, ff_share, share, ff_share), share, latent_size, group_width, peers, width)
    gains = lax.dynamic_slice_in_dim(gains, (place * share) % gains.shape[1], share, 1)
    return (
        hidden_out.reshape(rows, tokens, width),
        hidden_grad.reshape(rows, tokens, width),
        gains[0],
        query_share,
        latent_share,
        key_share,
        value_share,
        output_share,
        gains[1],
        gate_share.T,
        up_share.T,
        down_share,
    )


def solution(mesh):
    placed = (
        P("rows", "heads", None),
        P("rows", None),
        P("rows", "heads", None),
        P(),
        P(),
        P(),
        P(),
        P(),
        P(),
        P(),
        P(),
        P(),
        P(),
    )
    return jax.shard_map(
        shards,
        mesh=mesh,
        in_specs=placed,
        out_specs=(
            P("rows", "heads", None),
            P("rows", "heads", None),
            P("heads"),
            P("heads", None),
            P("heads", None),
            P(None, "heads", None),
            P(None, "heads", None),
            P("heads", None),
            P("heads"),
            P(None, "heads"),
            P(None, "heads"),
            P("heads", None),
        ),
        check_vma=False,
    )
```
